32 devices in a mesh: data: 1 (over z), img: 4 (over y), seq: 8 (over x, core).
Axes of the slice: x: 4, y: 4, z: 1, core: 2. Of those that a mesh axis runs over, the one named last changes fastest.
The devices are a block of a 4x4x8 slice.
Arguments:
- x_in: bfloat16 [4, 32768, 384], P(('data', 'img'), 'seq')
- grad_y: bfloat16 [4, 32768, 384], P(('data', 'img'), 'seq')
- ln_gamma: float32 [384], replicated
- ln_beta: float32 [384], replicated
- w_qkv: bfloat16 [384, 1152], replicated
- w_out: bfloat16 [384, 384], replicated
- head_temp: float32 [8], replicated
Outputs:
- output 1: bfloat16 [4, 32768, 384], P(('data', 'img'), 'seq')
- output 2: bfloat16 [4, 32768, 384], P(('data', 'img'), 'seq')
- output 3: float32 [384, 1152], P(('data', 'seq'))
- output 4: float32 [384, 384], P(('data', 'seq'))
- output 5: float32 [384], P('data')
- output 6: float32 [384], P('data')
- output 7: float32 [8], P('data')
All inputs are finite; a program needn't handle non-finite values.
Results may differ from the reference program's by a relative error of at most 0.00309468.
Values are sent between devices in bfloat16 or wider.
A program may use at most 768 MiB of HBM per device.

```python
import jax
import jax.numpy as jnp
from jax import lax

IMAGES = 4
TOKENS = 32768
MODEL_DIM = 384
NUM_HEADS = 8
HEAD_DIM = 48
LN_EPS = 1e-6


def layer_norm(x_f32, ln_gamma, ln_beta):
    row_mean = jnp.mean(x_f32, axis=-1, keepdims=True)
    centered = x_f32 - row_mean
    row_var = jnp.mean(centered * centered, axis=-1, keepdims=True)
    return centered * lax.rsqrt(row_var + LN_EPS) * ln_gamma + ln_beta


def attn_probs(gram_mat, sum_qq, sum_kk, head_temp):
    scale_mat = head_temp[..., :, None, None] * lax.rsqrt(sum_qq)[..., :, None] * lax.rsqrt(sum_kk)[..., None, :]
    return jax.nn.softmax(gram_mat * scale_mat, axis=-1)


def setup_inputs(seed: int = 0, part: int = 0) -> dict:
    base_key = jax.random.key(seed)
    part_key = jax.random.fold_in(base_key, part)
    k_noise, k_region, k_grad = jax.random.split(part_key, 3)
    k_gamma, k_beta, k_wqkv, k_wout, k_temp = jax.random.split(jax.random.key(seed + 1), 5)
    region_id = (jnp.arange(TOKENS) * 8) // TOKENS
    region_vec = 1.5 * jax.random.normal(k_region, (IMAGES, 8, MODEL_DIM), jnp.float32)
    noise_val = jax.random.normal(k_noise, (IMAGES, TOKENS, MODEL_DIM), jnp.float32)
    x_in = (noise_val + region_vec[:, region_id, :]).astype(jnp.bfloat16)
    grad_y = jax.random.normal(k_grad, (IMAGES, TOKENS, MODEL_DIM), jnp.float32).astype(jnp.bfloat16)
    ln_gamma = 1.0 + 0.3 * jax.random.normal(k_gamma, (MODEL_DIM,), jnp.float32)
    ln_beta = 0.5 * jax.random.normal(k_beta, (MODEL_DIM,), jnp.float32)
    fan_scale = MODEL_DIM ** -0.5
    w_qkv = (fan_scale * jax.random.normal(k_wqkv, (MODEL_DIM, 3 * MODEL_DIM), jnp.float32)).astype(jnp.bfloat16)
    w_out = (fan_scale * jax.random.normal(k_wout, (MODEL_DIM, MODEL_DIM), jnp.float32)).astype(jnp.bfloat16)
    head_temp = jax.random.uniform(k_temp, (NUM_HEADS,), jnp.float32, 4.0, 8.0)
    return {'x_in': x_in, 'grad_y': grad_y, 'ln_gamma': ln_gamma, 'ln_beta': ln_beta, 'w_qkv': w_qkv, 'w_out': w_out, 'head_temp': head_temp}


def reference(x_in, grad_y, ln_gamma, ln_beta, w_qkv, w_out, head_temp):
    def image_step(acc_sums, img_pair):
        x_img, gy_img = img_pair
        x_f32 = x_img.astype(jnp.float32)
        u_f32, ln_pull = jax.vjp(layer_norm, x_f32, ln_gamma, ln_beta)
        u_act = u_f32.astype(jnp.bfloat16)
        qkv_all = jnp.dot(u_act, w_qkv, preferred_element_type=jnp.float32).astype(jnp.bfloat16)
        qkv_heads = qkv_all.reshape(TOKENS, 3, NUM_HEADS, HEAD_DIM).astype(jnp.float32)
        q_act = qkv_heads[:, 0]
        k_act = qkv_heads[:, 1]
        v_act = qkv_heads[:, 2]
        gram_mat = jnp.einsum('nhi,nhj->hij', q_act, k_act)
        sum_qq = jnp.sum(q_act * q_act, axis=0)
        sum_kk = jnp.sum(k_act * k_act, axis=0)
        attn_p, attn_pull = jax.vjp(attn_probs, gram_mat, sum_qq, sum_kk, head_temp)
        attn_pb = attn_p.astype(jnp.bfloat16).astype(jnp.float32)
        head_out = jnp.einsum('nhj,hij->nhi', v_act, attn_pb).astype(jnp.bfloat16).reshape(TOKENS, MODEL_DIM)
        proj_out = jnp.dot(head_out, w_out, preferred_element_type=jnp.float32)
        y_img = (x_f32 + proj_out).astype(jnp.bfloat16)
        grad_wout = jnp.dot(head_out.T, gy_img, preferred_element_type=jnp.float32)
        grad_o = jnp.dot(gy_img, w_out.T, preferred_element_type=jnp.float32).astype(jnp.bfloat16)
        grad_oh = grad_o.reshape(TOKENS, NUM_HEADS, HEAD_DIM).astype(jnp.float32)
        grad_attn = jnp.einsum('nhi,nhj->hij', grad_oh, v_act)
        grad_v = jnp.einsum('nhi,hij->nhj', grad_oh, attn_pb)
        grad_gram, grad_sqq, grad_skk, grad_temp = attn_pull(grad_attn)
        gram_gb = grad_gram.astype(jnp.bfloat16).astype(jnp.float32)
        grad_q = jnp.einsum('nhj,hij->nhi', k_act, gram_gb) + 2.0 * grad_sqq * q_act
        grad_k = jnp.einsum('nhi,hij->nhj', q_act, gram_gb) + 2.0 * grad_skk * k_act
        grad_qkv = jnp.stack([grad_q, grad_k, grad_v], axis=1).reshape(TOKENS, 3 * MODEL_DIM).astype(jnp.bfloat16)
        grad_wqkv = jnp.dot(u_act.T, grad_qkv, preferred_element_type=jnp.float32)
        grad_u = jnp.dot(grad_qkv, w_qkv.T, preferred_element_type=jnp.float32).astype(jnp.bfloat16)
        grad_xln, grad_gamma, grad_beta = ln_pull(grad_u.astype(jnp.float32))
        grad_x = (gy_img.astype(jnp.float32) + grad_xln).astype(jnp.bfloat16)
        new_sums = (acc_sums[0] + grad_wqkv, acc_sums[1] + grad_wout, acc_sums[2] + grad_gamma, acc_sums[3] + grad_beta, acc_sums[4] + grad_temp)
        return new_sums, (y_img, grad_x)

    zero_sums = (jnp.zeros((MODEL_DIM, 3 * MODEL_DIM), jnp.float32), jnp.zeros((MODEL_DIM, MODEL_DIM), jnp.float32), jnp.zeros((MODEL_DIM,), jnp.float32), jnp.zeros((MODEL_DIM,), jnp.float32), jnp.zeros((NUM_HEADS,), jnp.float32))
    final_sums, (y_out, grad_x) = lax.scan(image_step, zero_sums, (x_in, grad_y))
    return y_out, grad_x, final_sums[0], final_sums[1], final_sums[2], final_sums[3], final_sums[4]
```

```python
import functools

import jax
import jax.numpy as jnp
from jax import lax
from jax.experimental import pallas as pl
from jax.experimental.pallas import tpu as pltpu
from jax.sharding import PartitionSpec as P

LN_EPS = 1e-6
BF = jnp.bfloat16
F32 = jnp.float32
MESH = pl.DeviceIdType.MESH
WIN = 256
LANES = 128
SUB = 256


def _dot(a, b):
    return lax.dot_general(a, b, (((1,), (0,)), ((), ())), preferred_element_type=F32)


def _dot_nt(a, b):
    return lax.dot_general(a, b, (((1,), (1,)), ((), ())), preferred_element_type=F32)


def _column(row):
    return jnp.transpose(jnp.broadcast_to(row, (LANES, row.shape[1])))


def _twice(x):
    return jnp.concatenate([x, x], axis=1)


def _kernel(cfg, x_hbm, gy_hbm, gam_hbm, bet_hbm, wqkv_hbm, wout_hbm, tau_ref,
            y_hbm, gx_hbm, dwqkv_ref, dwout_ref, dgam_ref, dbet_ref, dtau_ref,
            x_v, gy_v, x_t, gy_t, u_t, q_t, k_t, v_t, do_t, o_t, dqkv_t,
            mean_v, rstd_v, w_v, w_t, wo_v, wo_t, gam_v, bet_v, gam_c, bet_c,
            g_lo, g_hi, da_lo, da_hi, sq_acc, sk_acc, dgam_acc, dbet_acc,
            a_f32, scale_f32, g_f32, a_lo, a_hi, at_lo, at_hi, dg_lo, dg_hi, dgt_lo, dgt_hi,
            cq_c, ck_c, srow, rqcol,
            ex1_src, ex1_rc, ex1_x, ex1_fin, ex2_src, ex2_rc, ex2_x, ex2_fin,
            acc_e, acc_l, d2d_e, d2d_l, rs_e, rs_l, ag_e, ag_l,
            gb_src, gb_rc, gb_all,
            x_sem, gy_sem, y_sem, gx_sem, w_sem,
            ex1_ss, ex1_rs, ex2_ss, ex2_rs,
            d2d_ss, d2d_rs, rs_ss, rs_rs, ag_ss, ag_rs, gb_ss, gb_rs):
    n_chip, n_img, n_blk, blk, dim, n_head = cfg
    hd = dim // n_head
    n_lo = WIN // hd
    r_lo = n_lo * hd
    hi0 = dim - WIN
    off_hi = r_lo - hi0
    r_hi = dim - r_lo
    n_sub = blk // SUB
    inv_d = 1.0 / dim
    data_i = lax.axis_index('data')
    img_i = lax.axis_index('img')
    seq_i = lax.axis_index('seq')
    core = lax.rem(seq_i, 2)
    chip = seq_i // 2

    def dev(chip_to, core_to, img_to):
        return (data_i, img_to, chip_to * 2 + core_to)

    partner = dev(chip, 1 - core, img_i)

    def rcopy(src, dst, ssem, rsem, to):
        return pltpu.make_async_remote_copy(src_ref=src, dst_ref=dst, send_sem=ssem, recv_sem=rsem,
                                            device_id=to, device_id_type=MESH)

    offsets = [(dc, di) for dc in range(n_chip) for di in range(n_img) if (dc, di) != (0, 0)]

    def peer(dc, di):
        return lax.rem(chip + dc, n_chip), lax.rem(img_i + di, n_img)

    def x_copy(i):
        return pltpu.make_async_copy(x_hbm.at[0, pl.ds(i * blk, blk), :], x_v.at[i], x_sem.at[i])

    def gy_copy(i):
        return pltpu.make_async_copy(gy_hbm.at[0, pl.ds(i * blk, blk), :], gy_v.at[i], gy_sem.at[i])

    def y_copy(i):
        return pltpu.make_async_copy(x_v.at[i], y_hbm.at[0, pl.ds(i * blk, blk), :], y_sem.at[i])

    def gx_copy(i):
        return pltpu.make_async_copy(gy_v.at[i], gx_hbm.at[0, pl.ds(i * blk, blk), :], gx_sem.at[i])

    small = [(gam_hbm, gam_v), (bet_hbm, bet_v), (wqkv_hbm, w_v), (wout_hbm, wo_v)]
    loads = [pltpu.make_async_copy(s, d, w_sem.at[n]) for n, (s, d) in enumerate(small)]
    loads[0].start()
    loads[1].start()
    x_copy(0).start()
    loads[2].start()
    for i in range(1, n_blk):
        x_copy(i).start()
    loads[3].start()
    for i in range(n_blk):
        gy_copy(i).start()

    barrier = pltpu.get_barrier_semaphore()
    pl.semaphore_signal(barrier, inc=1, device_id=partner, device_id_type=MESH)
    for dc, di in offsets:
        pc, pi = peer(dc, di)
        pl.semaphore_signal(barrier, inc=1, device_id=dev(pc, core, pi), device_id_type=MESH)

    for ref in (g_lo, g_hi, da_lo, da_hi, sq_acc, sk_acc, dgam_acc, dbet_acc, acc_e, acc_l):
        ref[...] = jnp.zeros_like(ref)

    loads[0].wait()
    loads[1].wait()
    gam_c[...] = _column(gam_v[...])
    bet_c[...] = _column(bet_v[...])
    loads[2].wait()
    for c in range(3):
        w_t[c * dim:(c + 1) * dim, :] = jnp.transpose(w_v[:, c * dim:(c + 1) * dim])
    loads[3].wait()
    wo_t[...] = jnp.transpose(wo_v[...])

    def sub(n):
        return slice(n * SUB, (n + 1) * SUB)

    def body_qk(i, _):
        x_copy(i).wait()
        for n in range(n_sub):
            x_t[i, :, sub(n)] = jnp.transpose(x_v[i, sub(n), :])
        for c in range(blk // LANES):
            cols = slice(c * LANES, (c + 1) * LANES)
            xs = x_t[i, :, cols].astype(F32)
            mean = jnp.sum(xs, axis=0, keepdims=True) * inv_d
            cen = xs - mean
            var = jnp.sum(cen * cen, axis=0, keepdims=True) * inv_d
            rstd = lax.rsqrt(var + LN_EPS)
            mean_v[i, :, cols] = mean
            rstd_v[i, :, cols] = rstd
            u_t[i, :, cols] = (cen * rstd * gam_c[...] + bet_c[...]).astype(BF)
        for n in range(n_sub):
            u_n = u_t[i, :, sub(n)]
            for part, ref, acc in ((0, q_t, sq_acc), (1, k_t, sk_acc)):
                r = _dot(w_t[part * dim:(part + 1) * dim, :], u_n).astype(BF)
                ref[i, :, sub(n)] = r
                rf = r.astype(F32)
                rf = rf * rf
                acc[...] += rf[:, :LANES] + rf[:, LANES:]
        g_lo[...] += _dot_nt(q_t[i, :r_lo, :], k_t[i, :WIN, :])
        g_hi[...] += _dot_nt(q_t[i, r_lo:, :], k_t[i, hi0:, :])
        return 0

    lax.fori_loop(0, n_blk, body_qk, 0)

    def pack(lo, hi, put):
        col = lax.broadcasted_iota(jnp.int32, (hd, WIN), 1)
        t_lo = jnp.zeros((hd, WIN), F32)
        for h in range(n_lo):
            t_lo += jnp.where((col >= h * hd) & (col < (h + 1) * hd), lo[h * hd:(h + 1) * hd, :], 0.0)
        t_hi = jnp.zeros((hd, WIN), F32)
        for h in range(n_lo, n_head):
            b = h * hd - hi0
            r = h * hd - r_lo
            t_hi += jnp.where((col >= b) & (col < b + hd), hi[r:r + hd, :], 0.0)
        put(jnp.concatenate([t_lo[:, :hi0], t_lo[:, hi0:] + t_hi[:, :WIN - hi0], t_hi[:, WIN - hi0:]], axis=1))

    def ex_pair(src, rc, ss, rs):
        return rcopy(src.at[1 - core], rc, ss.at[0], rs.at[0], partner)

    def ex_chip(buf, ss, rs, dc):
        return rcopy(buf.at[chip], buf.at[chip], ss.at[dc], rs.at[dc], dev(lax.rem(chip + dc, n_chip), core, img_i))

    def ex_swap(fin, ss, rs):
        return rcopy(fin.at[core], fin.at[core], ss.at[n_chip], rs.at[n_chip], partner)

    def ex_step2(src, rc, buf, ss, rs):
        ex_pair(src, rc, ss, rs).wait()
        buf[chip] = src[core] + rc[...]
        for dc in range(1, n_chip):
            ex_chip(buf, ss, rs, dc).start()

    def ex_step3(buf, fin, ss, rs):
        for dc in range(1, n_chip):
            ex_chip(buf, ss, rs, dc).wait()
        tot = buf[0]
        for j in range(1, n_chip):
            tot += buf[j]
        fin[core] = tot
        ex_swap(fin, ss, rs).start()

    def put_g(t):
        h1 = ex1_src.shape[1]
        sq = jnp.sum(jnp.transpose(sq_acc[...]), axis=0, keepdims=True)
        sk = jnp.sum(jnp.transpose(sk_acc[...]), axis=0, keepdims=True)
        ex1_src[0] = t[:h1]
        ex1_src[1, :hd - h1] = t[h1:]
        ex1_src[1, hd - h1:hd - h1 + 8] = jnp.broadcast_to(sq, (8, dim))
        ex1_src[1, hd - h1 + 8:] = jnp.broadcast_to(sk, (8, dim))

    def put_da(t):
        ex2_src[0] = t[:hd // 2]
        ex2_src[1] = t[hd // 2:]

    pack(g_lo, g_hi, put_g)
    pl.semaphore_wait(barrier, 1 + len(offsets))
    ex_pair(ex1_src, ex1_rc, ex1_ss, ex1_rs).start()

    def body_v(i, _):
        gy_copy(i).wait()
        for n in range(n_sub):
            gy_t[i, :, sub(n)] = jnp.transpose(gy_v[i, sub(n), :])
        for n in range(n_sub):
            v_t[i, :, sub(n)] = _dot(w_t[2 * dim:, :], u_t[i, :, sub(n)]).astype(BF)
            do_t[i, :, sub(n)] = _dot(wo_v[...], gy_t[i, :, sub(n)]).astype(BF)
        da_lo[...] += _dot_nt(do_t[i, :r_lo, :], v_t[i, :WIN, :])
        da_hi[...] += _dot_nt(do_t[i, r_lo:, :], v_t[i, hi0:, :])

        @pl.when(i == 0)
        def _():
            ex_step2(ex1_src, ex1_rc, ex1_x, ex1_ss, ex1_rs)
        return 0

    lax.fori_loop(0, n_blk, body_v, 0)

    pack(da_lo, da_hi, put_da)
    ex_pair(ex2_src, ex2_rc, ex2_ss, ex2_rs).start()
    ex_step3(ex1_x, ex1_fin, ex1_ss, ex1_rs)
    ex_swap(ex1_fin, ex1_ss, ex1_rs).wait()

    def head_mask(rows, row0, col0):
        r = lax.broadcasted_iota(jnp.int32, (rows, WIN), 0) + row0
        c = lax.broadcasted_iota(jnp.int32, (rows, WIN), 1) + col0
        out = (r < 0)
        for h in range(n_head):
            out |= (r >= h * hd) & (r < (h + 1) * hd) & (c >= h * hd) & (c < (h + 1) * hd)
        return out

    windows = ((0, r_lo, 0, n_lo), (r_lo, r_hi, hi0, n_head - n_lo))
    h1 = ex1_fin.shape[1]
    gcat = jnp.concatenate([ex1_fin[0], ex1_fin[1, :hd - h1]], axis=0)
    sq = ex1_fin[1, hd - h1:hd - h1 + 1]
    sk = ex1_fin[1, hd - h1 + 8:hd - h1 + 9]
    rk = lax.rsqrt(sk)
    srow[0:1] = sk
    srow[1:2] = rk
    sq_c = _column(sq)
    rq_c = lax.rsqrt(sq_c)
    rqcol[0] = sq_c
    rqcol[1] = rq_c
    tau_c = jnp.concatenate([jnp.full((hd, LANES), tau_ref[h], F32) for h in range(n_head)], axis=0)
    rqcol[2] = tau_c
    for w, (row0, rows, col0, heads) in enumerate(windows):
        g = jnp.concatenate([gcat[:, col0:col0 + WIN]] * heads, axis=0)
        mask = head_mask(rows, row0, col0)
        scale = _twice((tau_c * rq_c)[row0:row0 + rows]) * rk[:, col0:col0 + WIN]
        s = g * scale
        top = jnp.max(jnp.where(mask, s, -jnp.inf), axis=1, keepdims=True)
        e = jnp.where(mask, jnp.exp(jnp.where(mask, s - top, 0.0)), 0.0)
        a = e / jnp.sum(e, axis=1, keepdims=True)
        a_f32[row0:row0 + rows] = a
        scale_f32[row0:row0 + rows] = scale
        g_f32[row0:row0 + rows] = g
        if w == 0:
            full = jnp.concatenate([a, jnp.zeros((WIN - rows, WIN), F32)], axis=0)
            a_lo[...] = full.astype(BF)
            at_lo[...] = jnp.transpose(full).astype(BF)
        else:
            full = jnp.concatenate([jnp.zeros((WIN - rows, WIN), F32), a], axis=0)
            a_hi[...] = full.astype(BF)
            at_hi[...] = jnp.transpose(full).astype(BF)

    ex_step2(ex2_src, ex2_rc, ex2_x, ex2_ss, ex2_rs)

    def add_rows(acc, g, val):
        rb = dim // (2 * n_chip)
        n_a = n_img // 2
        rc = rb // n_a
        for s in range(2 * n_chip):
            for a in range(n_a):
                acc[s % 2, s // 2, 2 * a + g] += val[s * rb + a * rc:s * rb + (a + 1) * rc]

    def body_ov(i, _):
        for n in range(n_sub):
            o_t[i, :r_lo, sub(n)] = _dot(a_lo[:r_lo], v_t[i, :WIN, sub(n)]).astype(BF)
            o_t[i, r_lo:, sub(n)] = _dot(a_hi[off_hi:], v_t[i, hi0:, sub(n)]).astype(BF)
            dqkv_t[i, 2 * dim:2 * dim + r_lo, sub(n)] = _dot(at_lo[:r_lo], do_t[i, :WIN, sub(n)]).astype(BF)
            dqkv_t[i, 2 * dim + r_lo:, sub(n)] = _dot(at_hi[off_hi:], do_t[i, hi0:, sub(n)]).astype(BF)
        add_rows(acc_e, 0, _dot(o_t[i], gy_v[i]))
        add_rows(acc_e, 1, _dot_nt(u_t[i], dqkv_t[i, 2 * dim:, :]))
        return 0

    lax.fori_loop(0, n_blk, body_ov, 0)

    def pair_copy(r, acc, buf):
        return rcopy(acc.at[1 - core], buf, d2d_ss.at[r], d2d_rs.at[r], partner)

    def rs_copy(r, acc, buf, n):
        pc, pi = peer(*offsets[n])
        return rcopy(acc.at[core, pc, pi], buf.at[n], rs_ss.at[r, n], rs_rs.at[r, n], dev(pc, core, pi))

    def ag_copy(r, buf, di):
        return rcopy(buf.at[img_i], buf.at[img_i], ag_ss.at[r, di], ag_rs.at[r, di],
                     dev(chip, core, lax.rem(img_i + di, n_img)))

    def rs_start(r, acc, buf, rbuf):
        pair_copy(r, acc, buf).wait()
        for j in range(n_chip):
            acc[core, j] += buf[j]
        for n in range(len(offsets)):
            rs_copy(r, acc, rbuf, n).start()

    def rs_finish(r, acc, rbuf, gbuf):
        tot = acc[core, chip, img_i]
        for n in range(len(offsets)):
            rs_copy(r, acc, rbuf, n).wait()
            tot += rbuf[n]
        gbuf[img_i] = tot
        for di in range(1, n_img):
            ag_copy(r, gbuf, di).start()

    pair_copy(0, acc_e, d2d_e).start()
    ex_step3(ex2_x, ex2_fin, ex2_ss, ex2_rs)
    ex_swap(ex2_fin, ex2_ss, ex2_rs).wait()

    dacat = jnp.concatenate([ex2_fin[0], ex2_fin[1]], axis=0)
    sq_c = rqcol[0]
    rq_c = rqcol[1]
    tau_c = rqcol[2]
    sk = srow[0:1]
    rk = srow[1:2]
    row_sums = []
    col_sums = []
    for w, (row0, rows, col0, heads) in enumerate(windows):
        da = jnp.concatenate([dacat[:, col0:col0 + WIN]] * heads, axis=0)
        a = a_f32[row0:row0 + rows]
        ds = a * (da - jnp.sum(a * da, axis=1, keepdims=True))
        dg = ds * scale_f32[row0:row0 + rows]
        dscale = ds * g_f32[row0:row0 + rows]
        row_sums.append(jnp.broadcast_to(jnp.sum(dscale * rk[:, col0:col0 + WIN], axis=1, keepdims=True),
                                         (rows, LANES)))
        col_sums.append(jnp.sum(dscale * _twice((tau_c * rq_c)[row0:row0 + rows]), axis=0, keepdims=True))
        if w == 0:
            full = jnp.concatenate([dg, jnp.zeros((WIN - rows, WIN), F32)], axis=0)
            dg_lo[...] = full.astype(BF)
            dgt_lo[...] = jnp.transpose(full).astype(BF)
        else:
            full = jnp.concatenate([jnp.zeros((WIN - rows, WIN), F32), dg], axis=0)
            dg_hi[...] = full.astype(BF)
            dgt_hi[...] = jnp.transpose(full).astype(BF)
    t_row = jnp.concatenate(row_sums, axis=0)
    cl, ch = col_sums
    w_col = jnp.concatenate([cl[:, :hi0], cl[:, hi0:] + ch[:, :WIN - hi0], ch[:, WIN - hi0:]], axis=1)
    cq_c[...] = 2.0 * (-0.5 * rq_c / sq_c * (tau_c * t_row))
    ck_c[...] = _column(2.0 * (-0.5 * rk / sk * w_col))
    lane = lax.broadcasted_iota(jnp.int32, (1, LANES), 1)
    dtau_row = jnp.zeros((1, LANES), F32)
    for h in range(n_head):
        part = jnp.sum((rq_c * t_row)[h * hd:(h + 1) * hd], axis=0, keepdims=True)
        dtau_row += jnp.where(lane == h, part, 0.0)
    gb_src[6:7] = jnp.where(seq_i == 0, dtau_row, 0.0)
    gb_src[7:8] = jnp.zeros((1, LANES), F32)

    rs_start(0, acc_e, d2d_e, rs_e)

    def body_qk_back(i, _):
        for n in range(n_sub):
            k_n = k_t[i, :, sub(n)]
            q_n = q_t[i, :, sub(n)]
            dq = jnp.concatenate([_dot(dg_lo[:r_lo], k_n[:WIN]), _dot(dg_hi[off_hi:], k_n[hi0:])], axis=0)
            dqkv_t[i, :dim, sub(n)] = (dq + _twice(cq_c[...]) * q_n.astype(F32)).astype(BF)
            dk = jnp.concatenate([_dot(dgt_lo[:r_lo], q_n[:WIN]), _dot(dgt_hi[off_hi:], q_n[hi0:])], axis=0)
            dqkv_t[i, dim:2 * dim, sub(n)] = (dk + _twice(ck_c[...]) * k_n.astype(F32)).astype(BF)
        dw = _dot_nt(u_t[i], dqkv_t[i, :2 * dim, :])
        add_rows(acc_l, 0, dw[:, :dim])
        add_rows(acc_l, 1, dw[:, dim:])
        return 0

    lax.fori_loop(0, n_blk, body_qk_back, 0)
    pair_copy(1, acc_l, d2d_l).start()

    def body_y(i, _):
        for n in range(n_sub):
            proj = _dot(wo_t[...], o_t[i, :, sub(n)])
            x_v[i, sub(n), :] = jnp.transpose((x_t[i, :, sub(n)].astype(F32) + proj).astype(BF))
        y_copy(i).start()
        return 0

    lax.fori_loop(0, n_blk, body_y, 0)
    rs_start(1, acc_l, d2d_l, rs_l)
    rs_finish(0, acc_e, rs_e, ag_e)

    def body_x(i, _):
        for n in range(n_sub):
            du = _dot(w_v[...], dqkv_t[i, :, sub(n)]).astype(BF)
            for c in range(SUB // LANES):
                cols = slice(n * SUB + c * LANES, n * SUB + (c + 1) * LANES)
                du_c = du[:, c * LANES:(c + 1) * LANES].astype(F32)
                rstd = rstd_v[i, :, cols]
                xh = (x_t[i, :, cols].astype(F32) - mean_v[i, :, cols]) * rstd
                dgam_acc[...] += du_c * xh
                dbet_acc[...] += du_c
                g = du_c * gam_c[...]
                c1 = jnp.sum(g, axis=0, keepdims=True) * inv_d
                c2 = jnp.sum(g * xh, axis=0, keepdims=True) * inv_d
                gx = gy_t[i, :, cols].astype(F32) + rstd * (g - c1 - xh * c2)
                gy_v[i, cols, :] = jnp.transpose(gx.astype(BF))
        gx_copy(i).start()
        return 0

    lax.fori_loop(0, n_blk, body_x, 0)

    for b, acc in ((0, dgam_acc), (3, dbet_acc)):
        row = jnp.sum(jnp.transpose(acc[...]), axis=0, keepdims=True)
        for c in range(dim // LANES):
            gb_src[b + c:b + c + 1] = row[:, c * LANES:(c + 1) * LANES]
    gb_pair = rcopy(gb_src, gb_rc, gb_ss.at[0], gb_rs.at[0], partner)
    gb_pair.start()

    rs_finish(1, acc_l, rs_l, ag_l)

    gb_pair.wait()
    gb_all[chip, img_i] = gb_src[...] + gb_rc[...]

    def gb_copy(n):
        pc, pi = peer(*offsets[n])
        return rcopy(gb_all.at[chip, img_i], gb_all.at[chip, img_i], gb_ss.at[1 + n], gb_rs.at[1 + n],
                     dev(pc, core, pi))

    for n in range(len(offsets)):
        gb_copy(n).start()

    def emit(r, gbuf, outs):
        for di in range(1, n_img):
            ag_copy(r, gbuf, di).wait()
        rc = gbuf.shape[1]
        for a in range(n_img // 2):
            for g, (ref, col) in enumerate(outs):
                ref[a * rc:(a + 1) * rc, col:col + dim] = gbuf[2 * a + g]

    emit(0, ag_e, ((dwout_ref, 0), (dwqkv_ref, 2 * dim)))
    for n in range(len(offsets)):
        gb_copy(n).wait()
    tot = jnp.zeros(gb_src.shape, F32)
    for j in range(n_chip):
        for m in range(n_img):
            tot += gb_all[j, m]
    for c in range(dim // LANES):
        dgam_ref[:, c * LANES:(c + 1) * LANES] = tot[c:c + 1]
        dbet_ref[:, c * LANES:(c + 1) * LANES] = tot[3 + c:4 + c]
    dtau_ref[...] = tot[6:7]
    emit(1, ag_l, ((dwqkv_ref, 0), (dwqkv_ref, dim)))
    for i in range(n_blk):
        y_copy(i).wait()
        gx_copy(i).wait()


def solution(mesh):
    act_spec = P(('data', 'img'), 'seq', None)
    row_spec = P(('data', 'seq'), None)
    in_specs = (act_spec, act_spec, P(), P(), P(), P(), P())
    out_specs = (act_spec, act_spec, row_spec, row_spec, P('data'), P('data'), P('data'))
    n_img = mesh.shape['img']
    n_seq = mesh.shape['seq']
    n_chip = n_seq // 2

    def local_block(x_in, grad_y, ln_gamma, ln_beta, w_qkv, w_out, head_temp):
        _, n_tok, dim = x_in.shape
        n_head = head_temp.shape[0]
        hd = dim // n_head
        blk = min(1024, n_tok)
        n_blk = n_tok // blk
        rb = dim // n_seq
        rc = rb // (n_img // 2)
        h1 = (hd + 16) // 2
        hbm = pl.BlockSpec(memory_space=pl.ANY)
        vmem = pl.BlockSpec(memory_space=pltpu.VMEM)
        smem = pl.BlockSpec(memory_space=pltpu.SMEM)
        V = pltpu.VMEM
        n_off = n_chip * n_img - 1
        n_hi = n_head - WIN // hd
        r_hi = n_hi * hd
        r_lo = dim - r_hi
        feat = V((n_blk, dim, blk), BF)
        tok = V((n_blk, blk, dim), BF)
        stat = V((n_blk, 1, blk), F32)
        col = V((dim, LANES), F32)
        sqr = V((WIN, WIN), BF)
        acc = V((2, n_chip, n_img, rc, dim), F32)
        dma = pltpu.SemaphoreType.DMA
        scratch = [
            tok, tok, feat, feat, feat, feat, feat, feat, feat, feat, V((n_blk, 3 * dim, blk), BF),
            stat, stat, V((dim, 3 * dim), BF), V((3 * dim, dim), BF), V((dim, dim), BF), V((dim, dim), BF),
            V((1, dim), F32), V((1, dim), F32), col, col,
            V((r_lo, WIN), F32), V((r_hi, WIN), F32), V((r_lo, WIN), F32), V((r_hi, WIN), F32),
            col, col, col, col,
            V((dim, WIN), F32), V((dim, WIN), F32), V((dim, WIN), F32),
            sqr, sqr, sqr, sqr, sqr, sqr, sqr, sqr,
            col, col, V((8, dim), F32), V((3, dim, LANES), F32),
            V((2, h1, dim), F32), V((h1, dim), F32), V((n_chip, h1, dim), F32), V((2, h1, dim), F32),
            V((2, hd // 2, dim), F32), V((hd // 2, dim), F32), V((n_chip, hd // 2, dim), F32),
            V((2, hd // 2, dim), F32),
            acc, acc, V((n_chip, n_img, rc, dim), F32), V((n_chip, n_img, rc, dim), F32),
            V((n_off, rc, dim), F32), V((n_off, rc, dim), F32), V((n_img, rc, dim), F32), V((n_img, rc, dim), F32),
            V((8, LANES), F32), V((8, LANES), F32), V((n_chip, n_img, 8, LANES), F32),
            dma((n_blk,)), dma((n_blk,)), dma((n_blk,)), dma((n_blk,)), dma((4,)),
            dma((n_chip + 1,)), dma((n_chip + 1,)), dma((n_chip + 1,)), dma((n_chip + 1,)),
            dma((2,)), dma((2,)), dma((2, n_off)), dma((2, n_off)), dma((2, n_img)), dma((2, n_img)),
            dma((1 + n_off,)), dma((1 + n_off,)),
        ]
        out_shape = (
            jax.ShapeDtypeStruct(x_in.shape, BF), jax.ShapeDtypeStruct(x_in.shape, BF),
            jax.ShapeDtypeStruct((rb, 3 * dim), F32), jax.ShapeDtypeStruct((rb, dim), F32),
            jax.ShapeDtypeStruct((1, dim), F32), jax.ShapeDtypeStruct((1, dim), F32),
            jax.ShapeDtypeStruct((1, LANES), F32),
        )
        cfg = (n_chip, n_img, n_blk, blk, dim, n_head)
        y, gx, dwqkv, dwout, dgam, dbet, dtau = pl.pallas_call(
            functools.partial(_kernel, cfg),
            out_shape=out_shape,
            in_specs=[hbm, hbm, hbm, hbm, hbm, hbm, smem],
            out_specs=(hbm, hbm, vmem, vmem, vmem, vmem, vmem),
            scratch_shapes=scratch,
            compiler_params=pltpu.CompilerParams(collective_id=0, has_side_effects=True,
                                                 vmem_limit_bytes=62 * 1024 * 1024),
        )(x_in, grad_y, ln_gamma.reshape(1, dim), ln_beta.reshape(1, dim), w_qkv, w_out, head_temp)
        return (y, gx, dwqkv, dwout, dgam.reshape(dim), dbet.reshape(dim), dtau[0, :n_head])

    return jax.shard_map(local_block, mesh=mesh, in_specs=in_specs, out_specs=out_specs, check_vma=False)
```

```python
import functools

import jax
import jax.numpy as jnp
from jax import lax
from jax.experimental import pallas as pl
from jax.experimental.pallas import tpu as pltpu
from jax.sharding import PartitionSpec as P

LN_EPS = 1e-6
BF = jnp.bfloat16
F32 = jnp.float32
MESH = pl.DeviceIdType.MESH
WIN = 256
LANES = 128
SUB = 256
VMEM_MAIN = 56 * 1024 * 1024


def _dot(a, b):
    return lax.dot_general(a, b, (((1,), (0,)), ((), ())), preferred_element_type=F32)


def _dot_nt(a, b):
    return lax.dot_general(a, b, (((1,), (1,)), ((), ())), preferred_element_type=F32)


def _column(row):
    return jnp.transpose(jnp.broadcast_to(row, (LANES, row.shape[1])))


def _twice(x):
    return jnp.concatenate([x, x], axis=1)


def _kernel(cfg, x_hbm, gy_hbm, gam_hbm, bet_hbm, wqkv_hbm, wout_hbm, tau_ref,
            x_v, gy_v, dwqkv_ref, dwout_ref, dgam_ref, dbet_ref, dtau_ref,
            x_t, gy_t, u_t, q_t, k_t, v_t, do_t, o_t, dqkv_t,
            mean_v, rstd_v, w_v, w_t, wo_v, wo_t, gam_v, bet_v, gam_c, bet_c,
            g_lo, g_hi, da_lo, da_hi, sq_acc, sk_acc, dgam_acc, dbet_acc,
            a_f32, scale_f32, g_f32, a_lo, a_hi, at_lo, at_hi, dg_lo, dg_hi, dgt_lo, dgt_hi,
            cq_c, ck_c, srow, rqcol,
            ex1_src, ex1_rc, ex1_x, ex1_fin, ex2_src, ex2_rc, ex2_x, ex2_fin,
            acc_e, acc_l, d2d_e, d2d_l, rs_e, rs_l, ag_e, ag_l,
            gb_src, gb_rc, gb_all,
            x_sem, gy_sem, w_sem,
            ex1_ss, ex1_rs, ex2_ss, ex2_rs,
            d2d_ss, d2d_rs, rs_ss, rs_rs, ag_ss, ag_rs, gb_ss, gb_rs):
    n_chip, n_img, n_blk, blk, dim, n_head = cfg
    hd = dim // n_head
    n_lo = WIN // hd
    r_lo = n_lo * hd
    hi0 = dim - WIN
    off_hi = r_lo - hi0
    r_hi = dim - r_lo
    n_sub = blk // SUB
    inv_d = 1.0 / dim
    data_i = lax.axis_index('data')
    img_i = lax.axis_index('img')
    seq_i = lax.axis_index('seq')
    core = lax.rem(seq_i, 2)
    chip = seq_i // 2

    def dev(chip_to, core_to, img_to):
        return (data_i, img_to, chip_to * 2 + core_to)

    partner = dev(chip, 1 - core, img_i)

    def rcopy(src, dst, ssem, rsem, to):
        return pltpu.make_async_remote_copy(src_ref=src, dst_ref=dst, send_sem=ssem, recv_sem=rsem,
                                            device_id=to, device_id_type=MESH)

    offsets = [(dc, di) for dc in range(n_chip) for di in range(n_img) if (dc, di) != (0, 0)]

    def peer(dc, di):
        return lax.rem(chip + dc, n_chip), lax.rem(img_i + di, n_img)

    def x_copy(i):
        return pltpu.make_async_copy(x_hbm.at[0, pl.ds(i * blk, blk), :], x_v.at[i], x_sem.at[i])

    def gy_copy(i):
        return pltpu.make_async_copy(gy_hbm.at[0, pl.ds(i * blk, blk), :], gy_v.at[i], gy_sem.at[i])

    small = [(gam_hbm, gam_v), (bet_hbm, bet_v), (wqkv_hbm, w_v), (wout_hbm, wo_v)]
    loads = [pltpu.make_async_copy(s, d, w_sem.at[n]) for n, (s, d) in enumerate(small)]
    loads[0].start()
    loads[1].start()
    x_copy(0).start()
    loads[2].start()
    for i in range(1, n_blk):
        x_copy(i).start()
    loads[3].start()
    for i in range(n_blk):
        gy_copy(i).start()

    barrier = pltpu.get_barrier_semaphore()
    pl.semaphore_signal(barrier, inc=1, device_id=partner, device_id_type=MESH)
    for dc, di in offsets:
        pc, pi = peer(dc, di)
        pl.semaphore_signal(barrier, inc=1, device_id=dev(pc, core, pi), device_id_type=MESH)

    for ref in (g_lo, g_hi, da_lo, da_hi, sq_acc, sk_acc, dgam_acc, dbet_acc, acc_e, acc_l):
        ref[...] = jnp.zeros_like(ref)

    loads[0].wait()
    loads[1].wait()
    gam_c[...] = _column(gam_v[...].reshape(1, dim))
    bet_c[...] = _column(bet_v[...].reshape(1, dim))
    loads[2].wait()
    for c in range(3):
        w_t[c * dim:(c + 1) * dim, :] = jnp.transpose(w_v[:, c * dim:(c + 1) * dim])
    loads[3].wait()
    wo_t[...] = jnp.transpose(wo_v[...])

    def sub(n):
        return slice(n * SUB, (n + 1) * SUB)

    def body_qk(i, _):
        x_copy(i).wait()
        for n in range(n_sub):
            x_t[i, :, sub(n)] = jnp.transpose(x_v[i, sub(n), :])
        for c in range(blk // LANES):
            cols = slice(c * LANES, (c + 1) * LANES)
            xs = x_t[i, :, cols].astype(F32)
            mean = jnp.sum(xs, axis=0, keepdims=True) * inv_d
            cen = xs - mean
            var = jnp.sum(cen * cen, axis=0, keepdims=True) * inv_d
            rstd = lax.rsqrt(var + LN_EPS)
            mean_v[i, :, cols] = mean
            rstd_v[i, :, cols] = rstd
            u_t[i, :, cols] = (cen * rstd * gam_c[...] + bet_c[...]).astype(BF)
        for n in range(n_sub):
            u_n = u_t[i, :, sub(n)]
            for part, ref, acc in ((0, q_t, sq_acc), (1, k_t, sk_acc)):
                r = _dot(w_t[part * dim:(part + 1) * dim, :], u_n).astype(BF)
                ref[i, :, sub(n)] = r
                rf = r.astype(F32)
                rf = rf * rf
                acc[...] += rf[:, :LANES] + rf[:, LANES:]
        g_lo[...] += _dot_nt(q_t[i, :r_lo, :], k_t[i, :WIN, :])
        g_hi[...] += _dot_nt(q_t[i, r_lo:, :], k_t[i, hi0:, :])
        return 0

    lax.fori_loop(0, n_blk, body_qk, 0)

    def pack(lo, hi, put):
        col = lax.broadcasted_iota(jnp.int32, (hd, WIN), 1)
        t_lo = jnp.zeros((hd, WIN), F32)
        for h in range(n_lo):
            t_lo += jnp.where((col >= h * hd) & (col < (h + 1) * hd), lo[h * hd:(h + 1) * hd, :], 0.0)
        t_hi = jnp.zeros((hd, WIN), F32)
        for h in range(n_lo, n_head):
            b = h * hd - hi0
            r = h * hd - r_lo
            t_hi += jnp.where((col >= b) & (col < b + hd), hi[r:r + hd, :], 0.0)
        put(jnp.concatenate([t_lo[:, :hi0], t_lo[:, hi0:] + t_hi[:, :WIN - hi0], t_hi[:, WIN - hi0:]], axis=1))

    def ex_pair(src, rc, ss, rs):
        return rcopy(src.at[1 - core], rc, ss.at[0], rs.at[0], partner)

    def ex_chip(buf, ss, rs, dc):
        return rcopy(buf.at[chip], buf.at[chip], ss.at[dc], rs.at[dc], dev(lax.rem(chip + dc, n_chip), core, img_i))

    def ex_swap(fin, ss, rs):
        return rcopy(fin.at[core], fin.at[core], ss.at[n_chip], rs.at[n_chip], partner)

    def ex_step2(src, rc, buf, ss, rs):
        ex_pair(src, rc, ss, rs).wait()
        buf[chip] = src[core] + rc[...]
        for dc in range(1, n_chip):
            ex_chip(buf, ss, rs, dc).start()

    def ex_step3(buf, fin, ss, rs):
        for dc in range(1, n_chip):
            ex_chip(buf, ss, rs, dc).wait()
        tot = buf[0]
        for j in range(1, n_chip):
            tot += buf[j]
        fin[core] = tot
        ex_swap(fin, ss, rs).start()

    def put_g(t):
        h1 = ex1_src.shape[1]
        sq = jnp.sum(jnp.transpose(sq_acc[...]), axis=0, keepdims=True)
        sk = jnp.sum(jnp.transpose(sk_acc[...]), axis=0, keepdims=True)
        ex1_src[0] = t[:h1]
        ex1_src[1, :hd - h1] = t[h1:]
        ex1_src[1, hd - h1:hd - h1 + 8] = jnp.broadcast_to(sq, (8, dim))
        ex1_src[1, hd - h1 + 8:] = jnp.broadcast_to(sk, (8, dim))

    def put_da(t):
        ex2_src[0] = t[:hd // 2]
        ex2_src[1] = t[hd // 2:]

    pack(g_lo, g_hi, put_g)
    pl.semaphore_wait(barrier, 1 + len(offsets))
    ex_pair(ex1_src, ex1_rc, ex1_ss, ex1_rs).start()

    def body_v(i, _):
        gy_copy(i).wait()
        for n in range(n_sub):
            gy_t[i, :, sub(n)] = jnp.transpose(gy_v[i, sub(n), :])
        for n in range(n_sub):
            v_t[i, :, sub(n)] = _dot(w_t[2 * dim:, :], u_t[i, :, sub(n)]).astype(BF)
            do_t[i, :, sub(n)] = _dot(wo_v[...], gy_t[i, :, sub(n)]).astype(BF)
        da_lo[...] += _dot_nt(do_t[i, :r_lo, :], v_t[i, :WIN, :])
        da_hi[...] += _dot_nt(do_t[i, r_lo:, :], v_t[i, hi0:, :])

        @pl.when(i == 0)
        def _():
            ex_step2(ex1_src, ex1_rc, ex1_x, ex1_ss, ex1_rs)
        return 0

    lax.fori_loop(0, n_blk, body_v, 0)

    pack(da_lo, da_hi, put_da)
    ex_pair(ex2_src, ex2_rc, ex2_ss, ex2_rs).start()
    ex_step3(ex1_x, ex1_fin, ex1_ss, ex1_rs)
    ex_swap(ex1_fin, ex1_ss, ex1_rs).wait()

    def head_mask(rows, row0, col0):
        r = lax.broadcasted_iota(jnp.int32, (rows, WIN), 0) + row0
        c = lax.broadcasted_iota(jnp.int32, (rows, WIN), 1) + col0
        out = (r < 0)
        for h in range(n_head):
            out |= (r >= h * hd) & (r < (h + 1) * hd) & (c >= h * hd) & (c < (h + 1) * hd)
        return out

    windows = ((0, r_lo, 0, n_lo), (r_lo, r_hi, hi0, n_head - n_lo))
    h1 = ex1_fin.shape[1]
    gcat = jnp.concatenate([ex1_fin[0], ex1_fin[1, :hd - h1]], axis=0)
    sq = ex1_fin[1, hd - h1:hd - h1 + 1]
    sk = ex1_fin[1, hd - h1 + 8:hd - h1 + 9]
    rk = lax.rsqrt(sk)
    srow[0:1] = sk
    srow[1:2] = rk
    sq_c = _column(sq)
    rq_c = lax.rsqrt(sq_c)
    rqcol[0] = sq_c
    rqcol[1] = rq_c
    tau_c = jnp.concatenate([jnp.full((hd, LANES), tau_ref[h], F32) for h in range(n_head)], axis=0)
    rqcol[2] = tau_c
    for w, (row0, rows, col0, heads) in enumerate(windows):
        g = jnp.concatenate([gcat[:, col0:col0 + WIN]] * heads, axis=0)
        mask = head_mask(rows, row0, col0)
        scale = _twice((tau_c * rq_c)[row0:row0 + rows]) * rk[:, col0:col0 + WIN]
        s = g * scale
        top = jnp.max(jnp.where(mask, s, -jnp.inf), axis=1, keepdims=True)
        e = jnp.where(mask, jnp.exp(jnp.where(mask, s - top, 0.0)), 0.0)
        a = e / jnp.sum(e, axis=1, keepdims=True)
        a_f32[row0:row0 + rows] = a
        scale_f32[row0:row0 + rows] = scale
        g_f32[row0:row0 + rows] = g
        if w == 0:
            full = jnp.concatenate([a, jnp.zeros((WIN - rows, WIN), F32)], axis=0)
            a_lo[...] = full.astype(BF)
            at_lo[...] = jnp.transpose(full).astype(BF)
        else:
            full = jnp.concatenate([jnp.zeros((WIN - rows, WIN), F32), a], axis=0)
            a_hi[...] = full.astype(BF)
            at_hi[...] = jnp.transpose(full).astype(BF)

    ex_step2(ex2_src, ex2_rc, ex2_x, ex2_ss, ex2_rs)

    def add_rows(acc, g, val):
        rb = dim // (2 * n_chip)
        n_a = n_img // 2
        rc = rb // n_a
        for s in range(2 * n_chip):
            for a in range(n_a):
                acc[s % 2, s // 2, 2 * a + g] += val[s * rb + a * rc:s * rb + (a + 1) * rc]

    def body_ov(i, _):
        for n in range(n_sub):
            o_t[i, :r_lo, sub(n)] = _dot(a_lo[:r_lo], v_t[i, :WIN, sub(n)]).astype(BF)
            o_t[i, r_lo:, sub(n)] = _dot(a_hi[off_hi:], v_t[i, hi0:, sub(n)]).astype(BF)
            dqkv_t[i, 2 * dim:2 * dim + r_lo, sub(n)] = _dot(at_lo[:r_lo], do_t[i, :WIN, sub(n)]).astype(BF)
            dqkv_t[i, 2 * dim + r_lo:, sub(n)] = _dot(at_hi[off_hi:], do_t[i, hi0:, sub(n)]).astype(BF)
        add_rows(acc_e, 0, _dot(o_t[i], gy_v[i]))
        add_rows(acc_e, 1, _dot_nt(u_t[i], dqkv_t[i, 2 * dim:, :]))
        return 0

    lax.fori_loop(0, n_blk, body_ov, 0)

    def pair_copy(r, acc, buf):
        return rcopy(acc.at[1 - core], buf, d2d_ss.at[r], d2d_rs.at[r], partner)

    def rs_copy(r, acc, buf, n):
        pc, pi = peer(*offsets[n])
        return rcopy(acc.at[core, pc, pi], buf.at[n], rs_ss.at[r, n], rs_rs.at[r, n], dev(pc, core, pi))

    def ag_copy(r, buf, di):
        return rcopy(buf.at[img_i], buf.at[img_i], ag_ss.at[r, di], ag_rs.at[r, di],
                     dev(chip, core, lax.rem(img_i + di, n_img)))

    def rs_start(r, acc, buf, rbuf):
        pair_copy(r, acc, buf).wait()
        for j in range(n_chip):
            acc[core, j] += buf[j]
        for n in range(len(offsets)):
            rs_copy(r, acc, rbuf, n).start()

    def rs_finish(r, acc, rbuf, gbuf):
        tot = acc[core, chip, img_i]
        for n in range(len(offsets)):
            rs_copy(r, acc, rbuf, n).wait()
            tot += rbuf[n]
        gbuf[img_i] = tot
        for di in range(1, n_img):
            ag_copy(r, gbuf, di).start()

    pair_copy(0, acc_e, d2d_e).start()
    ex_step3(ex2_x, ex2_fin, ex2_ss, ex2_rs)
    ex_swap(ex2_fin, ex2_ss, ex2_rs).wait()

    dacat = jnp.concatenate([ex2_fin[0], ex2_fin[1]], axis=0)
    sq_c = rqcol[0]
    rq_c = rqcol[1]
    tau_c = rqcol[2]
    sk = srow[0:1]
    rk = srow[1:2]
    row_sums = []
    col_sums = []
    for w, (row0, rows, col0, heads) in enumerate(windows):
        da = jnp.concatenate([dacat[:, col0:col0 + WIN]] * heads, axis=0)
        a = a_f32[row0:row0 + rows]
        ds = a * (da - jnp.sum(a * da, axis=1, keepdims=True))
        dg = ds * scale_f32[row0:row0 + rows]
        dscale = ds * g_f32[row0:row0 + rows]
        row_sums.append(jnp.broadcast_to(jnp.sum(dscale * rk[:, col0:col0 + WIN], axis=1, keepdims=True),
                                         (rows, LANES)))
        col_sums.append(jnp.sum(dscale * _twice((tau_c * rq_c)[row0:row0 + rows]), axis=0, keepdims=True))
        if w == 0:
            full = jnp.concatenate([dg, jnp.zeros((WIN - rows, WIN), F32)], axis=0)
            dg_lo[...] = full.astype(BF)
            dgt_lo[...] = jnp.transpose(full).astype(BF)
        else:
            full = jnp.concatenate([jnp.zeros((WIN - rows, WIN), F32), dg], axis=0)
            dg_hi[...] = full.astype(BF)
            dgt_hi[...] = jnp.transpose(full).astype(BF)
    t_row = jnp.concatenate(row_sums, axis=0)
    cl, ch = col_sums
    w_col = jnp.concatenate([cl[:, :hi0], cl[:, hi0:] + ch[:, :WIN - hi0], ch[:, WIN - hi0:]], axis=1)
    cq_c[...] = 2.0 * (-0.5 * rq_c / sq_c * (tau_c * t_row))
    ck_c[...] = _column(2.0 * (-0.5 * rk / sk * w_col))
    lane = lax.broadcasted_iota(jnp.int32, (1, LANES), 1)
    dtau_row = jnp.zeros((1, LANES), F32)
    for h in range(n_head):
        part = jnp.sum((rq_c * t_row)[h * hd:(h + 1) * hd], axis=0, keepdims=True)
        dtau_row += jnp.where(lane == h, part, 0.0)
    gb_src[6:7] = jnp.where(seq_i == 0, dtau_row, 0.0)
    gb_src[7:8] = jnp.zeros((1, LANES), F32)

    rs_start(0, acc_e, d2d_e, rs_e)

    def body_qk_back(i, _):
        for n in range(n_sub):
            k_n = k_t[i, :, sub(n)]
            q_n = q_t[i, :, sub(n)]
            dq = jnp.concatenate([_dot(dg_lo[:r_lo], k_n[:WIN]), _dot(dg_hi[off_hi:], k_n[hi0:])], axis=0)
            dqkv_t[i, :dim, sub(n)] = (dq + _twice(cq_c[...]) * q_n.astype(F32)).astype(BF)
            dk = jnp.concatenate([_dot(dgt_lo[:r_lo], q_n[:WIN]), _dot(dgt_hi[off_hi:], q_n[hi0:])], axis=0)
            dqkv_t[i, dim:2 * dim, sub(n)] = (dk + _twice(ck_c[...]) * k_n.astype(F32)).astype(BF)
        dw = _dot_nt(u_t[i], dqkv_t[i, :2 * dim, :])
        add_rows(acc_l, 0, dw[:, :dim])
        add_rows(acc_l, 1, dw[:, dim:])
        return 0

    lax.fori_loop(0, n_blk, body_qk_back, 0)
    pair_copy(1, acc_l, d2d_l).start()

    def body_y(i, _):
        for n in range(n_sub):
            proj = _dot(wo_t[...], o_t[i, :, sub(n)])
            x_v[i, sub(n), :] = jnp.transpose((x_t[i, :, sub(n)].astype(F32) + proj).astype(BF))
        return 0

    lax.fori_loop(0, n_blk, body_y, 0)
    rs_start(1, acc_l, d2d_l, rs_l)
    rs_finish(0, acc_e, rs_e, ag_e)

    def body_x(i, _):
        for n in range(n_sub):
            du = _dot(w_v[...], dqkv_t[i, :, sub(n)]).astype(BF)
            for c in range(SUB // LANES):
                cols = slice(n * SUB + c * LANES, n * SUB + (c + 1) * LANES)
                du_c = du[:, c * LANES:(c + 1) * LANES].astype(F32)
                rstd = rstd_v[i, :, cols]
                xh = (x_t[i, :, cols].astype(F32) - mean_v[i, :, cols]) * rstd
                dgam_acc[...] += du_c * xh
                dbet_acc[...] += du_c
                g = du_c * gam_c[...]
                c1 = jnp.sum(g, axis=0, keepdims=True) * inv_d
                c2 = jnp.sum(g * xh, axis=0, keepdims=True) * inv_d
                gx = gy_t[i, :, cols].astype(F32) + rstd * (g - c1 - xh * c2)
                gy_v[i, cols, :] = jnp.transpose(gx.astype(BF))
        return 0

    lax.fori_loop(0, n_blk, body_x, 0)

    for b, acc in ((0, dgam_acc), (3, dbet_acc)):
        row = jnp.sum(jnp.transpose(acc[...]), axis=0, keepdims=True)
        for c in range(dim // LANES):
            gb_src[b + c:b + c + 1] = row[:, c * LANES:(c + 1) * LANES]
    gb_pair = rcopy(gb_src, gb_rc, gb_ss.at[0], gb_rs.at[0], partner)
    gb_pair.start()

    gb_pair.wait()
    gb_all[chip, img_i] = gb_src[...] + gb_rc[...]

    def gb_copy(n):
        pc, pi = peer(*offsets[n])
        return rcopy(gb_all.at[chip, img_i], gb_all.at[chip, img_i], gb_ss.at[1 + n], gb_rs.at[1 + n],
                     dev(pc, core, pi))

    for n in range(len(offsets)):
        gb_copy(n).start()
    rs_finish(1, acc_l, rs_l, ag_l)

    def emit(r, gbuf, outs):
        for di in range(1, n_img):
            ag_copy(r, gbuf, di).wait()
        rc = gbuf.shape[1]
        for a in range(n_img // 2):
            for g, (ref, col) in enumerate(outs):
                ref[a * rc:(a + 1) * rc, col:col + dim] = gbuf[2 * a + g]

    emit(0, ag_e, ((dwout_ref, 0), (dwqkv_ref, 2 * dim)))
    for n in range(len(offsets)):
        gb_copy(n).wait()
    tot = jnp.zeros(gb_src.shape, F32)
    for j in range(n_chip):
        for m in range(n_img):
            tot += gb_all[j, m]
    n_row = dim // LANES
    for b, ref in ((0, dgam_ref), (n_row, dbet_ref)):
        ref[...] = jnp.concatenate([tot[b + c:b + c + 1] for c in range(n_row)], axis=1).reshape(dim)
    dtau_ref[...] = tot[6:7, :n_head].reshape(n_head)
    emit(1, ag_l, ((dwqkv_ref, 0), (dwqkv_ref, dim)))


def _write(n_blk, blk, *refs):
    srcs, dsts, act_sem, sem = refs[:7], refs[7:14], refs[14], refs[15]
    copies = []
    for a in range(2):
        for i in range(n_blk):
            copies.append(pltpu.make_async_copy(srcs[a].at[i], dsts[a].at[0, pl.ds(i * blk, blk), :],
                                                act_sem.at[a, i]))
    for n in range(5):
        copies.append(pltpu.make_async_copy(srcs[2 + n], dsts[2 + n], sem.at[n]))
    for c in copies:
        c.start()
    for c in copies:
        c.wait()


def solution(mesh):
    act_spec = P(('data', 'img'), 'seq', None)
    row_spec = P(('data', 'seq'), None)
    in_specs = (act_spec, act_spec, P(), P(), P(), P(), P())
    out_specs = (act_spec, act_spec, row_spec, row_spec, P('data'), P('data'), P('data'))
    n_img = mesh.shape['img']
    n_seq = mesh.shape['seq']
    n_chip = n_seq // 2

    def local_block(x_in, grad_y, ln_gamma, ln_beta, w_qkv, w_out, head_temp):
        _, n_tok, dim = x_in.shape
        n_head = head_temp.shape[0]
        hd = dim // n_head
        blk = min(1024, n_tok)
        n_blk = n_tok // blk
        rb = dim // n_seq
        rc = rb // (n_img // 2)
        h1 = (hd + 16) // 2
        hbm = pl.BlockSpec(memory_space=pltpu.HBM)
        vmem = pl.BlockSpec(memory_space=pltpu.VMEM)
        smem = pl.BlockSpec(memory_space=pltpu.SMEM)
        V = pltpu.VMEM
        n_off = n_chip * n_img - 1
        n_hi = n_head - WIN // hd
        r_hi = n_hi * hd
        r_lo = dim - r_hi
        feat = V((n_blk, dim, blk), BF)
        stat = V((n_blk, 1, blk), F32)
        col = V((dim, LANES), F32)
        sqr = V((WIN, WIN), BF)
        acc = V((2, n_chip, n_img, rc, dim), F32)
        dma = pltpu.SemaphoreType.DMA
        scratch = [
            feat, feat, feat, feat, feat, feat, feat, feat, V((n_blk, 3 * dim, blk), BF),
            stat, stat, V((dim, 3 * dim), BF), V((3 * dim, dim), BF), V((dim, dim), BF), V((dim, dim), BF),
            V((dim,), F32), V((dim,), F32), col, col,
            V((r_lo, WIN), F32), V((r_hi, WIN), F32), V((r_lo, WIN), F32), V((r_hi, WIN), F32),
            col, col, col, col,
            V((dim, WIN), F32), V((dim, WIN), F32), V((dim, WIN), F32),
            sqr, sqr, sqr, sqr, sqr, sqr, sqr, sqr,
            col, col, V((8, dim), F32), V((3, dim, LANES), F32),
            V((2, h1, dim), F32), V((h1, dim), F32), V((n_chip, h1, dim), F32), V((2, h1, dim), F32),
            V((2, hd // 2, dim), F32), V((hd // 2, dim), F32), V((n_chip, hd // 2, dim), F32),
            V((2, hd // 2, dim), F32),
            acc, acc, V((n_chip, n_img, rc, dim), F32), V((n_chip, n_img, rc, dim), F32),
            V((n_off, rc, dim), F32), V((n_off, rc, dim), F32), V((n_img, rc, dim), F32), V((n_img, rc, dim), F32),
            V((8, LANES), F32), V((8, LANES), F32), V((n_chip, n_img, 8, LANES), F32),
            dma((n_blk,)), dma((n_blk,)), dma((4,)),
            dma((n_chip + 1,)), dma((n_chip + 1,)), dma((n_chip + 1,)), dma((n_chip + 1,)),
            dma((2,)), dma((2,)), dma((2, n_off)), dma((2, n_off)), dma((2, n_img)), dma((2, n_img)),
            dma((1 + n_off,)), dma((1 + n_off,)),
        ]
        out_shape = (
            V((n_blk, blk, dim), BF), V((n_blk, blk, dim), BF), V((rb, 3 * dim), F32), V((rb, dim), F32),
            V((dim,), F32), V((dim,), F32), V((n_head,), F32),
        )
        cfg = (n_chip, n_img, n_blk, blk, dim, n_head)
        outs = pl.pallas_call(
            functools.partial(_kernel, cfg),
            out_shape=out_shape,
            in_specs=[hbm, hbm, hbm, hbm, hbm, hbm, smem],
            out_specs=(vmem,) * 7,
            scratch_shapes=scratch,
            compiler_params=pltpu.CompilerParams(collective_id=0, has_side_effects=True,
                                                 vmem_limit_bytes=VMEM_MAIN),
        )(x_in, grad_y, ln_gamma, ln_beta, w_qkv, w_out, head_temp)
        finals = (
            jax.ShapeDtypeStruct(x_in.shape, BF), jax.ShapeDtypeStruct(x_in.shape, BF),
            jax.ShapeDtypeStruct((rb, 3 * dim), F32), jax.ShapeDtypeStruct((rb, dim), F32),
            jax.ShapeDtypeStruct((dim,), F32), jax.ShapeDtypeStruct((dim,), F32),
            jax.ShapeDtypeStruct((n_head,), F32),
        )
        return pl.pallas_call(
            functools.partial(_write, n_blk, blk),
            out_shape=finals,
            in_specs=[vmem] * 7,
            out_specs=(hbm,) * 7,
            scratch_shapes=[dma((2, n_blk)), dma((5,))],
            compiler_params=pltpu.CompilerParams(vmem_limit_bytes=1 << 20),
        )(*outs)

    return jax.shard_map(local_block, mesh=mesh, in_specs=in_specs, out_specs=out_specs, check_vma=False)
```

```python
import functools

import jax
import jax.numpy as jnp
from jax import lax
from jax.experimental import pallas as pl
from jax.experimental.pallas import tpu as pltpu
from jax.sharding import PartitionSpec as P

LN_EPS = 1e-6
BF = jnp.bfloat16
F32 = jnp.float32
MESH = pl.DeviceIdType.MESH
WIN = 256
LANES = 128
SUB = 256
VMEM_MAIN = 56 * 1024 * 1024


def _dot(a, b):
    return lax.dot_general(a, b, (((1,), (0,)), ((), ())), preferred_element_type=F32)


def _dot_nt(a, b):
    return lax.dot_general(a, b, (((1,), (1,)), ((), ())), preferred_element_type=F32)


def _column(row):
    return jnp.transpose(jnp.broadcast_to(row, (LANES, row.shape[1])))


def _twice(x):
    return jnp.concatenate([x, x], axis=1)


def _kernel(cfg, x_hbm, gy_hbm, gam_hbm, bet_hbm, wqkv_hbm, wout_hbm, tau_ref,
            x_v, gy_v, dwqkv_ref, dwout_ref, dgam_ref, dbet_ref, dtau_ref,
            x_t, gy_t, u_t, q_t, k_t, v_t, do_t, o_t, dqkv_t,
            mean_v, rstd_v, w_v, w_t, wo_v, wo_t, gam_v, bet_v, gam_c, bet_c,
            g_lo, g_hi, da_lo, da_hi, sq_acc, sk_acc, dgam_acc, dbet_acc,
            a_f32, scale_f32, g_f32, a_lo, a_hi, at_lo, at_hi, dg_lo, dg_hi, dgt_lo, dgt_hi,
            cq_c, ck_c, srow, rqcol,
            ex1_src, ex1_rc, ex1_x, ex1_fin, ex2_src, ex2_rc, ex2_x, ex2_fin,
            acc_e, acc_q, acc_k, d2d_e, d2d_q, d2d_k, ring1, ring2, yrs_e, ag_e, rs_q, rs_k, ag_q, ag_k,
            gb_src, gb_rc, gb_all,
            x_sem, gy_sem, w_sem,
            ex1_ss, ex1_rs, ex2_ss, ex2_rs,
            d2d_ss, d2d_rs, ring_ss, ring_rs, yrs_ss, yrs_rs, age_ss, age_rs,
            rs_ss, rs_rs, ag_ss, ag_rs, gb_ss, gb_rs):
    n_chip, n_img, n_blk, blk, dim, n_head = cfg
    hd = dim // n_head
    n_lo = WIN // hd
    r_lo = n_lo * hd
    hi0 = dim - WIN
    off_hi = r_lo - hi0
    r_hi = dim - r_lo
    n_sub = blk // SUB
    inv_d = 1.0 / dim
    data_i = lax.axis_index('data')
    img_i = lax.axis_index('img')
    seq_i = lax.axis_index('seq')
    core = lax.rem(seq_i, 2)
    chip = seq_i // 2

    def dev(chip_to, core_to, img_to):
        return (data_i, img_to, chip_to * 2 + core_to)

    partner = dev(chip, 1 - core, img_i)

    def rcopy(src, dst, ssem, rsem, to):
        return pltpu.make_async_remote_copy(src_ref=src, dst_ref=dst, send_sem=ssem, recv_sem=rsem,
                                            device_id=to, device_id_type=MESH)

    offsets = [(dc, di) for dc in range(n_chip) for di in range(n_img) if (dc, di) != (0, 0)]

    def peer(dc, di):
        return lax.rem(chip + dc, n_chip), lax.rem(img_i + di, n_img)

    def x_copy(i):
        return pltpu.make_async_copy(x_hbm.at[0, pl.ds(i * blk, blk), :], x_v.at[i], x_sem.at[i])

    def gy_copy(i):
        return pltpu.make_async_copy(gy_hbm.at[0, pl.ds(i * blk, blk), :], gy_v.at[i], gy_sem.at[i])

    small = [(gam_hbm, gam_v), (bet_hbm, bet_v), (wqkv_hbm, w_v), (wout_hbm, wo_v)]
    loads = [pltpu.make_async_copy(s, d, w_sem.at[n]) for n, (s, d) in enumerate(small)]
    loads[0].start()
    loads[1].start()
    x_copy(0).start()
    loads[2].start()
    for i in range(1, n_blk):
        x_copy(i).start()
    loads[3].start()
    for i in range(n_blk):
        gy_copy(i).start()

    barrier = pltpu.get_barrier_semaphore()
    pl.semaphore_signal(barrier, inc=1, device_id=partner, device_id_type=MESH)
    for dc, di in offsets:
        pc, pi = peer(dc, di)
        pl.semaphore_signal(barrier, inc=1, device_id=dev(pc, core, pi), device_id_type=MESH)

    for ref in (g_lo, g_hi, da_lo, da_hi, sq_acc, sk_acc, dgam_acc, dbet_acc, acc_e, acc_q, acc_k):
        ref[...] = jnp.zeros_like(ref)

    loads[0].wait()
    loads[1].wait()
    gam_c[...] = _column(gam_v[...].reshape(1, dim))
    bet_c[...] = _column(bet_v[...].reshape(1, dim))
    loads[2].wait()
    for c in range(3):
        w_t[c * dim:(c + 1) * dim, :] = jnp.transpose(w_v[:, c * dim:(c + 1) * dim])
    loads[3].wait()
    wo_t[...] = jnp.transpose(wo_v[...])

    def sub(n):
        return slice(n * SUB, (n + 1) * SUB)

    def body_qk(i, _):
        x_copy(i).wait()
        for n in range(n_sub):
            x_t[i, :, sub(n)] = jnp.transpose(x_v[i, sub(n), :])
        for c in range(blk // LANES):
            cols = slice(c * LANES, (c + 1) * LANES)
            xs = x_t[i, :, cols].astype(F32)
            mean = jnp.sum(xs, axis=0, keepdims=True) * inv_d
            cen = xs - mean
            var = jnp.sum(cen * cen, axis=0, keepdims=True) * inv_d
            rstd = lax.rsqrt(var + LN_EPS)
            mean_v[i, :, cols] = mean
            rstd_v[i, :, cols] = rstd
            u_t[i, :, cols] = (cen * rstd * gam_c[...] + bet_c[...]).astype(BF)
        for n in range(n_sub):
            u_n = u_t[i, :, sub(n)]
            for part, ref, acc in ((0, q_t, sq_acc), (1, k_t, sk_acc)):
                r = _dot(w_t[part * dim:(part + 1) * dim, :], u_n).astype(BF)
                ref[i, :, sub(n)] = r
                rf = r.astype(F32)
                rf = rf * rf
                acc[...] += rf[:, :LANES] + rf[:, LANES:]
        g_lo[...] += _dot_nt(q_t[i, :r_lo, :], k_t[i, :WIN, :])
        g_hi[...] += _dot_nt(q_t[i, r_lo:, :], k_t[i, hi0:, :])
        return 0

    lax.fori_loop(0, n_blk, body_qk, 0)

    def pack(lo, hi, put):
        col = lax.broadcasted_iota(jnp.int32, (hd, WIN), 1)
        t_lo = jnp.zeros((hd, WIN), F32)
        for h in range(n_lo):
            t_lo += jnp.where((col >= h * hd) & (col < (h + 1) * hd), lo[h * hd:(h + 1) * hd, :], 0.0)
        t_hi = jnp.zeros((hd, WIN), F32)
        for h in range(n_lo, n_head):
            b = h * hd - hi0
            r = h * hd - r_lo
            t_hi += jnp.where((col >= b) & (col < b + hd), hi[r:r + hd, :], 0.0)
        put(jnp.concatenate([t_lo[:, :hi0], t_lo[:, hi0:] + t_hi[:, :WIN - hi0], t_hi[:, WIN - hi0:]], axis=1))

    def ex_pair(src, rc, ss, rs):
        return rcopy(src.at[1 - core], rc, ss.at[0], rs.at[0], partner)

    def ex_chip(buf, ss, rs, dc):
        return rcopy(buf.at[chip], buf.at[chip], ss.at[dc], rs.at[dc], dev(lax.rem(chip + dc, n_chip), core, img_i))

    def ex_swap(fin, ss, rs):
        return rcopy(fin.at[core], fin.at[core], ss.at[n_chip], rs.at[n_chip], partner)

    def ex_step2(src, rc, buf, ss, rs):
        ex_pair(src, rc, ss, rs).wait()
        buf[chip] = src[core] + rc[...]
        for dc in range(1, n_chip):
            ex_chip(buf, ss, rs, dc).start()

    def ex_step3(buf, fin, ss, rs):
        for dc in range(1, n_chip):
            ex_chip(buf, ss, rs, dc).wait()
        tot = buf[0]
        for j in range(1, n_chip):
            tot += buf[j]
        fin[core] = tot
        ex_swap(fin, ss, rs).start()

    def put_g(t):
        h1 = ex1_src.shape[1]
        sq = jnp.sum(jnp.transpose(sq_acc[...]), axis=0, keepdims=True)
        sk = jnp.sum(jnp.transpose(sk_acc[...]), axis=0, keepdims=True)
        ex1_src[0] = t[:h1]
        ex1_src[1, :hd - h1] = t[h1:]
        ex1_src[1, hd - h1:hd - h1 + 8] = jnp.broadcast_to(sq, (8, dim))
        ex1_src[1, hd - h1 + 8:] = jnp.broadcast_to(sk, (8, dim))

    def put_da(t):
        ex2_src[0] = t[:hd // 2]
        ex2_src[1] = t[hd // 2:]

    pack(g_lo, g_hi, put_g)
    pl.semaphore_wait(barrier, 1 + len(offsets))
    ex_pair(ex1_src, ex1_rc, ex1_ss, ex1_rs).start()

    def body_v(i, _):
        gy_copy(i).wait()
        for n in range(n_sub):
            gy_t[i, :, sub(n)] = jnp.transpose(gy_v[i, sub(n), :])
        for n in range(n_sub):
            v_t[i, :, sub(n)] = _dot(w_t[2 * dim:, :], u_t[i, :, sub(n)]).astype(BF)
            do_t[i, :, sub(n)] = _dot(wo_v[...], gy_t[i, :, sub(n)]).astype(BF)
        da_lo[...] += _dot_nt(do_t[i, :r_lo, :], v_t[i, :WIN, :])
        da_hi[...] += _dot_nt(do_t[i, r_lo:, :], v_t[i, hi0:, :])

        @pl.when(i == 0)
        def _():
            ex_step2(ex1_src, ex1_rc, ex1_x, ex1_ss, ex1_rs)
        return 0

    lax.fori_loop(0, n_blk, body_v, 0)

    pack(da_lo, da_hi, put_da)
    ex_pair(ex2_src, ex2_rc, ex2_ss, ex2_rs).start()
    ex_step3(ex1_x, ex1_fin, ex1_ss, ex1_rs)
    ex_swap(ex1_fin, ex1_ss, ex1_rs).wait()

    def head_mask(rows, row0, col0):
        r = lax.broadcasted_iota(jnp.int32, (rows, WIN), 0) + row0
        c = lax.broadcasted_iota(jnp.int32, (rows, WIN), 1) + col0
        out = (r < 0)
        for h in range(n_head):
            out |= (r >= h * hd) & (r < (h + 1) * hd) & (c >= h * hd) & (c < (h + 1) * hd)
        return out

    windows = ((0, r_lo, 0, n_lo), (r_lo, r_hi, hi0, n_head - n_lo))
    h1 = ex1_fin.shape[1]
    gcat = jnp.concatenate([ex1_fin[0], ex1_fin[1, :hd - h1]], axis=0)
    sq = ex1_fin[1, hd - h1:hd - h1 + 1]
    sk = ex1_fin[1, hd - h1 + 8:hd - h1 + 9]
    rk = lax.rsqrt(sk)
    srow[0:1] = sk
    srow[1:2] = rk
    sq_c = _column(sq)
    rq_c = lax.rsqrt(sq_c)
    rqcol[0] = sq_c
    rqcol[1] = rq_c
    tau_c = jnp.concatenate([jnp.full((hd, LANES), tau_ref[h], F32) for h in range(n_head)], axis=0)
    rqcol[2] = tau_c
    for w, (row0, rows, col0, heads) in enumerate(windows):
        g = jnp.concatenate([gcat[:, col0:col0 + WIN]] * heads, axis=0)
        mask = head_mask(rows, row0, col0)
        scale = _twice((tau_c * rq_c)[row0:row0 + rows]) * rk[:, col0:col0 + WIN]
        s = g * scale
        top = jnp.max(jnp.where(mask, s, -jnp.inf), axis=1, keepdims=True)
        e = jnp.where(mask, jnp.exp(jnp.where(mask, s - top, 0.0)), 0.0)
        a = e / jnp.sum(e, axis=1, keepdims=True)
        a_f32[row0:row0 + rows] = a
        scale_f32[row0:row0 + rows] = scale
        g_f32[row0:row0 + rows] = g
        if w == 0:
            full = jnp.concatenate([a, jnp.zeros((WIN - rows, WIN), F32)], axis=0)
            a_lo[...] = full.astype(BF)
            at_lo[...] = jnp.transpose(full).astype(BF)
        else:
            full = jnp.concatenate([jnp.zeros((WIN - rows, WIN), F32), a], axis=0)
            a_hi[...] = full.astype(BF)
            at_hi[...] = jnp.transpose(full).astype(BF)

    ex_step2(ex2_src, ex2_rc, ex2_x, ex2_ss, ex2_rs)

    def add_rows(acc, g, val):
        rb = dim // (2 * n_chip)
        n_a = n_img // 2
        rc = rb // n_a
        for s in range(2 * n_chip):
            for a in range(n_a):
                acc[s % 2, s // 2, 2 * a + g] += val[s * rb + a * rc:s * rb + (a + 1) * rc]

    n_ct = dim // LANES

    def add_cols(acc, val):
        rb = dim // (2 * n_chip)
        for s in range(2 * n_chip):
            for ct in range(n_ct):
                acc[s % 2, s // 2, ct] += val[s * rb:(s + 1) * rb, ct * LANES:(ct + 1) * LANES]

    def body_ov(i, _):
        for n in range(n_sub):
            o_t[i, :r_lo, sub(n)] = _dot(a_lo[:r_lo], v_t[i, :WIN, sub(n)]).astype(BF)
            o_t[i, r_lo:, sub(n)] = _dot(a_hi[off_hi:], v_t[i, hi0:, sub(n)]).astype(BF)
            dqkv_t[i, 2 * dim:2 * dim + r_lo, sub(n)] = _dot(at_lo[:r_lo], do_t[i, :WIN, sub(n)]).astype(BF)
            dqkv_t[i, 2 * dim + r_lo:, sub(n)] = _dot(at_hi[off_hi:], do_t[i, hi0:, sub(n)]).astype(BF)
        add_rows(acc_e, 0, _dot(o_t[i], gy_v[i]))
        add_rows(acc_e, 1, _dot_nt(u_t[i], dqkv_t[i, 2 * dim:, :]))
        return 0

    lax.fori_loop(0, n_blk, body_ov, 0)

    def pair_copy(r, acc, buf):
        return rcopy(acc.at[1 - core], buf, d2d_ss.at[r], d2d_rs.at[r], partner)

    hn = n_img // 2
    right = lax.rem(chip + 1, n_chip)
    left = lax.rem(chip + n_chip - 1, n_chip)
    opp = lax.rem(chip + 2, n_chip)

    def ring_copy(n):
        to = dev((right, left)[n % 2], core, img_i)
        if n == 0:
            src, dst = acc_e.at[core, opp, pl.ds(0, hn)], ring1.at[0]
        elif n == 1:
            src, dst = acc_e.at[core, opp, pl.ds(hn, hn)], ring1.at[1]
        else:
            src, dst = acc_e.at[core, (right, left)[n % 2]], ring2.at[n % 2]
        return rcopy(src, dst, ring_ss.at[n], ring_rs.at[n], to)

    def yrs_copy(di):
        pi = lax.rem(img_i + di, n_img)
        return rcopy(acc_e.at[core, chip, pi], yrs_e.at[di - 1], yrs_ss.at[di - 1], yrs_rs.at[di - 1],
                     dev(chip, core, pi))

    def age_copy(di):
        return rcopy(ag_e.at[img_i], ag_e.at[img_i], age_ss.at[di - 1], age_rs.at[di - 1],
                     dev(chip, core, lax.rem(img_i + di, n_img)))

    def e_step1():
        pair_copy(0, acc_e, d2d_e).wait()
        for j in range(n_chip):
            acc_e[core, j] += d2d_e[j]
        ring_copy(0).start()
        ring_copy(1).start()

    def e_step2():
        ring_copy(0).wait()
        ring_copy(1).wait()
        acc_e[core, right, :hn] += ring1[0]
        acc_e[core, left, hn:] += ring1[1]
        ring_copy(2).start()
        ring_copy(3).start()

    def e_step3():
        ring_copy(2).wait()
        ring_copy(3).wait()
        acc_e[core, chip] += ring2[0] + ring2[1]
        for di in range(1, n_img):
            yrs_copy(di).start()

    def e_step4():
        tot = acc_e[core, chip, img_i]
        for di in range(1, n_img):
            yrs_copy(di).wait()
            tot += yrs_e[di - 1]
        ag_e[img_i] = tot
        for di in range(1, n_img):
            age_copy(di).start()

    def owner(r, ct):
        return (2 * r + ct) % n_img

    def rs_copy(r, acc, buf, ct, dc):
        pc = lax.rem(chip + dc, n_chip)
        sl = ct // n_img
        return rcopy(acc.at[core, pc, ct], buf.at[sl, dc, img_i], rs_ss.at[r, ct, dc], rs_rs.at[r, sl, dc, img_i],
                     dev(pc, core, owner(r, ct)))

    def each_send(r, do):
        for dc in range(n_chip):
            for ct in range(n_ct):
                if dc:
                    do(ct, dc)
                else:
                    pl.when(img_i != owner(r, ct))(functools.partial(do, ct, dc))

    def rs_start(r, acc, d2d, buf):
        pair_copy(1 + r, acc, d2d).wait()
        for j in range(n_chip):
            acc[core, j] += d2d[j]
        each_send(r, lambda ct, dc: rs_copy(r, acc, buf, ct, dc).start())

    def ag_copy(r, gbuf, ct, di):
        return rcopy(gbuf.at[ct], gbuf.at[ct], ag_ss.at[r, ct, di - 1], ag_rs.at[r, ct],
                     dev(chip, core, lax.rem(img_i + di, n_img)))

    def rs_finish(r, acc, buf, gbuf):
        for ct in range(n_ct):
            @pl.when(img_i == owner(r, ct))
            def _(ct=ct):
                sl = ct // n_img
                tot = acc[core, chip, ct]
                for dc in range(n_chip):
                    for im in range(n_img):
                        if dc == 0 and im == owner(r, ct):
                            continue
                        rcopy(buf.at[sl, dc, im], buf.at[sl, dc, im], rs_ss.at[r, ct, dc], rs_rs.at[r, sl, dc, im],
                              partner).wait_recv()
                        tot += buf[sl, dc, im]
                gbuf[ct] = tot
                for di in range(1, n_img):
                    ag_copy(r, gbuf, ct, di).start()

    def rs_end(r, acc, buf, gbuf, ref, col):
        each_send(r, lambda ct, dc: rs_copy(r, acc, buf, ct, dc).wait_send())
        for ct in range(n_ct):
            @pl.when(img_i == owner(r, ct))
            def _(ct=ct):
                for di in range(1, n_img):
                    ag_copy(r, gbuf, ct, di).wait_send()

            @pl.when(img_i != owner(r, ct))
            def _(ct=ct):
                ag_copy(r, gbuf, ct, 1).wait_recv()
            ref[:, col + ct * LANES:col + (ct + 1) * LANES] = gbuf[ct]

    ex_step3(ex2_x, ex2_fin, ex2_ss, ex2_rs)
    pair_copy(0, acc_e, d2d_e).start()
    ex_swap(ex2_fin, ex2_ss, ex2_rs).wait()

    dacat = jnp.concatenate([ex2_fin[0], ex2_fin[1]], axis=0)
    sq_c = rqcol[0]
    rq_c = rqcol[1]
    tau_c = rqcol[2]
    sk = srow[0:1]
    rk = srow[1:2]
    row_sums = []
    col_sums = []
    for w, (row0, rows, col0, heads) in enumerate(windows):
        da = jnp.concatenate([dacat[:, col0:col0 + WIN]] * heads, axis=0)
        a = a_f32[row0:row0 + rows]
        ds = a * (da - jnp.sum(a * da, axis=1, keepdims=True))
        dg = ds * scale_f32[row0:row0 + rows]
        dscale = ds * g_f32[row0:row0 + rows]
        row_sums.append(jnp.broadcast_to(jnp.sum(dscale * rk[:, col0:col0 + WIN], axis=1, keepdims=True),
                                         (rows, LANES)))
        col_sums.append(jnp.sum(dscale * _twice((tau_c * rq_c)[row0:row0 + rows]), axis=0, keepdims=True))
        if w == 0:
            full = jnp.concatenate([dg, jnp.zeros((WIN - rows, WIN), F32)], axis=0)
            dg_lo[...] = full.astype(BF)
            dgt_lo[...] = jnp.transpose(full).astype(BF)
        else:
            full = jnp.concatenate([jnp.zeros((WIN - rows, WIN), F32), dg], axis=0)
            dg_hi[...] = full.astype(BF)
            dgt_hi[...] = jnp.transpose(full).astype(BF)
    t_row = jnp.concatenate(row_sums, axis=0)
    cl, ch = col_sums
    w_col = jnp.concatenate([cl[:, :hi0], cl[:, hi0:] + ch[:, :WIN - hi0], ch[:, WIN - hi0:]], axis=1)
    cq_c[...] = 2.0 * (-0.5 * rq_c / sq_c * (tau_c * t_row))
    ck_c[...] = _column(2.0 * (-0.5 * rk / sk * w_col))
    lane = lax.broadcasted_iota(jnp.int32, (1, LANES), 1)
    dtau_row = jnp.zeros((1, LANES), F32)
    for h in range(n_head):
        part = jnp.sum((rq_c * t_row)[h * hd:(h + 1) * hd], axis=0, keepdims=True)
        dtau_row += jnp.where(lane == h, part, 0.0)
    gb_src[6:7] = jnp.where(seq_i == 0, dtau_row, 0.0)
    gb_src[7:8] = jnp.zeros((1, LANES), F32)

    e_step1()

    def body_qk_back(i, _):
        for n in range(n_sub):
            k_n = k_t[i, :, sub(n)]
            q_n = q_t[i, :, sub(n)]
            dq = jnp.concatenate([_dot(dg_lo[:r_lo], k_n[:WIN]), _dot(dg_hi[off_hi:], k_n[hi0:])], axis=0)
            dqkv_t[i, :dim, sub(n)] = (dq + _twice(cq_c[...]) * q_n.astype(F32)).astype(BF)
            dk = jnp.concatenate([_dot(dgt_lo[:r_lo], q_n[:WIN]), _dot(dgt_hi[off_hi:], q_n[hi0:])], axis=0)
            dqkv_t[i, dim:2 * dim, sub(n)] = (dk + _twice(ck_c[...]) * k_n.astype(F32)).astype(BF)
        add_cols(acc_q, _dot_nt(u_t[i], dqkv_t[i, :dim, :]))
        return 0

    lax.fori_loop(0, n_blk, body_qk_back, 0)
    pair_copy(1, acc_q, d2d_q).start()
    e_step2()

    def body_wk(i, _):
        add_cols(acc_k, _dot_nt(u_t[i], dqkv_t[i, dim:2 * dim, :]))
        return 0

    lax.fori_loop(0, n_blk, body_wk, 0)
    pair_copy(2, acc_k, d2d_k).start()
    rs_start(0, acc_q, d2d_q, rs_q)

    def body_y(i, _):
        for n in range(n_sub):
            proj = _dot(wo_t[...], o_t[i, :, sub(n)])
            x_v[i, sub(n), :] = jnp.transpose((x_t[i, :, sub(n)].astype(F32) + proj).astype(BF))
        return 0

    lax.fori_loop(0, n_blk, body_y, 0)
    rs_start(1, acc_k, d2d_k, rs_k)

    def body_x(i, _):
        for n in range(n_sub):
            du = _dot(w_v[...], dqkv_t[i, :, sub(n)]).astype(BF)
            for c in range(SUB // LANES):
                cols = slice(n * SUB + c * LANES, n * SUB + (c + 1) * LANES)
                du_c = du[:, c * LANES:(c + 1) * LANES].astype(F32)
                rstd = rstd_v[i, :, cols]
                xh = (x_t[i, :, cols].astype(F32) - mean_v[i, :, cols]) * rstd
                dgam_acc[...] += du_c * xh
                dbet_acc[...] += du_c
                g = du_c * gam_c[...]
                c1 = jnp.sum(g, axis=0, keepdims=True) * inv_d
                c2 = jnp.sum(g * xh, axis=0, keepdims=True) * inv_d
                gx = gy_t[i, :, cols].astype(F32) + rstd * (g - c1 - xh * c2)
                gy_v[i, cols, :] = jnp.transpose(gx.astype(BF))

        @pl.when(i == 0)
        def _():
            e_step3()
        return 0

    lax.fori_loop(0, n_blk, body_x, 0)

    for b, acc in ((0, dgam_acc), (3, dbet_acc)):
        row = jnp.sum(jnp.transpose(acc[...]), axis=0, keepdims=True)
        for c in range(dim // LANES):
            gb_src[b + c:b + c + 1] = row[:, c * LANES:(c + 1) * LANES]
    gb_pair = rcopy(gb_src, gb_rc, gb_ss.at[0], gb_rs.at[0], partner)
    gb_pair.start()

    gb_pair.wait()
    gb_all[chip, img_i] = gb_src[...] + gb_rc[...]

    def gb_copy(n):
        pc, pi = peer(*offsets[n])
        return rcopy(gb_all.at[chip, img_i], gb_all.at[chip, img_i], gb_ss.at[1 + n], gb_rs.at[1 + n],
                     dev(pc, core, pi))

    for n in range(len(offsets)):
        gb_copy(n).start()
    rs_finish(0, acc_q, rs_q, ag_q)
    e_step4()
    rs_finish(1, acc_k, rs_k, ag_k)

    for n in range(len(offsets)):
        gb_copy(n).wait()
    tot = jnp.zeros(gb_src.shape, F32)
    for j in range(n_chip):
        for m in range(n_img):
            tot += gb_all[j, m]
    n_row = dim // LANES
    for b, ref in ((0, dgam_ref), (n_row, dbet_ref)):
        ref[...] = jnp.concatenate([tot[b + c:b + c + 1] for c in range(n_row)], axis=1).reshape(dim)
    dtau_ref[...] = tot[6:7, :n_head].reshape(n_head)
    rs_end(0, acc_q, rs_q, ag_q, dwqkv_ref, 0)
    for di in range(1, n_img):
        age_copy(di).wait()
    rc = ag_e.shape[1]
    for a in range(hn):
        for g, (ref, col) in enumerate(((dwout_ref, 0), (dwqkv_ref, 2 * dim))):
            ref[a * rc:(a + 1) * rc, col:col + dim] = ag_e[2 * a + g]
    rs_end(1, acc_k, rs_k, ag_k, dwqkv_ref, dim)


def _write(n_blk, blk, *refs):
    srcs, dsts, act_sem, sem = refs[:7], refs[7:14], refs[14], refs[15]
    copies = []
    for a in range(2):
        for i in range(n_blk):
            copies.append(pltpu.make_async_copy(srcs[a].at[i], dsts[a].at[0, pl.ds(i * blk, blk), :],
                                                act_sem.at[a, i]))
    for n in range(5):
        copies.append(pltpu.make_async_copy(srcs[2 + n], dsts[2 + n], sem.at[n]))
    for c in copies:
        c.start()
    for c in copies:
        c.wait()


def solution(mesh):
    act_spec = P(('data', 'img'), 'seq', None)
    row_spec = P(('data', 'seq'), None)
    in_specs = (act_spec, act_spec, P(), P(), P(), P(), P())
    out_specs = (act_spec, act_spec, row_spec, row_spec, P('data'), P('data'), P('data'))
    n_img = mesh.shape['img']
    n_seq = mesh.shape['seq']
    n_chip = n_seq // 2

    def local_block(x_in, grad_y, ln_gamma, ln_beta, w_qkv, w_out, head_temp):
        _, n_tok, dim = x_in.shape
        n_head = head_temp.shape[0]
        hd = dim // n_head
        blk = min(1024, n_tok)
        n_blk = n_tok // blk
        rb = dim // n_seq
        rc = rb // (n_img // 2)
        h1 = (hd + 16) // 2
        hbm = pl.BlockSpec(memory_space=pltpu.HBM)
        vmem = pl.BlockSpec(memory_space=pltpu.VMEM)
        smem = pl.BlockSpec(memory_space=pltpu.SMEM)
        V = pltpu.VMEM
        n_off = n_chip * n_img - 1
        n_hi = n_head - WIN // hd
        r_hi = n_hi * hd
        r_lo = dim - r_hi
        feat = V((n_blk, dim, blk), BF)
        stat = V((n_blk, 1, blk), F32)
        col = V((dim, LANES), F32)
        sqr = V((WIN, WIN), BF)
        acc = V((2, n_chip, n_img, rc, dim), F32)
        n_ct = dim // LANES
        n_sl = -(-n_ct // n_img)
        accc = V((2, n_chip, n_ct, rb, LANES), F32)
        dma = pltpu.SemaphoreType.DMA
        scratch = [
            feat, feat, feat, feat, feat, feat, feat, feat, V((n_blk, 3 * dim, blk), BF),
            stat, stat, V((dim, 3 * dim), BF), V((3 * dim, dim), BF), V((dim, dim), BF), V((dim, dim), BF),
            V((dim,), F32), V((dim,), F32), col, col,
            V((r_lo, WIN), F32), V((r_hi, WIN), F32), V((r_lo, WIN), F32), V((r_hi, WIN), F32),
            col, col, col, col,
            V((dim, WIN), F32), V((dim, WIN), F32), V((dim, WIN), F32),
            sqr, sqr, sqr, sqr, sqr, sqr, sqr, sqr,
            col, col, V((8, dim), F32), V((3, dim, LANES), F32),
            V((2, h1, dim), F32), V((h1, dim), F32), V((n_chip, h1, dim), F32), V((2, h1, dim), F32),
            V((2, hd // 2, dim), F32), V((hd // 2, dim), F32), V((n_chip, hd // 2, dim), F32),
            V((2, hd // 2, dim), F32),
            acc, accc, accc, V((n_chip, n_img, rc, dim), F32), V((n_chip, n_ct, rb, LANES), F32),
            V((n_chip, n_ct, rb, LANES), F32), V((2, n_img // 2, rc, dim), F32), V((2, n_img, rc, dim), F32),
            V((n_img - 1, rc, dim), F32), V((n_img, rc, dim), F32), V((n_sl, n_chip, n_img, rb, LANES), F32),
            V((n_sl, n_chip, n_img, rb, LANES), F32), V((n_ct, rb, LANES), F32), V((n_ct, rb, LANES), F32),
            V((8, LANES), F32), V((8, LANES), F32), V((n_chip, n_img, 8, LANES), F32),
            dma((n_blk,)), dma((n_blk,)), dma((4,)),
            dma((n_chip + 1,)), dma((n_chip + 1,)), dma((n_chip + 1,)), dma((n_chip + 1,)),
            dma((3,)), dma((3,)), dma((4,)), dma((4,)), dma((n_img - 1,)), dma((n_img - 1,)),
            dma((n_img - 1,)), dma((n_img - 1,)),
            dma((2, n_ct, n_chip)), dma((2, n_sl, n_chip, n_img)), dma((2, n_ct, n_img - 1)), dma((2, n_ct)),
            dma((1 + n_off,)), dma((1 + n_off,)),
        ]
        out_shape = (
            V((n_blk, blk, dim), BF), V((n_blk, blk, dim), BF), V((rb, 3 * dim), F32), V((rb, dim), F32),
            V((dim,), F32), V((dim,), F32), V((n_head,), F32),
        )
        cfg = (n_chip, n_img, n_blk, blk, dim, n_head)
        outs = pl.pallas_call(
            functools.partial(_kernel, cfg),
            out_shape=out_shape,
            in_specs=[hbm, hbm, hbm, hbm, hbm, hbm, smem],
            out_specs=(vmem,) * 7,
            scratch_shapes=scratch,
            compiler_params=pltpu.CompilerParams(collective_id=0, has_side_effects=True,
                                                 vmem_limit_bytes=VMEM_MAIN),
        )(x_in, grad_y, ln_gamma, ln_beta, w_qkv, w_out, head_temp)
        finals = (
            jax.ShapeDtypeStruct(x_in.shape, BF), jax.ShapeDtypeStruct(x_in.shape, BF),
            jax.ShapeDtypeStruct((rb, 3 * dim), F32), jax.ShapeDtypeStruct((rb, dim), F32),
            jax.ShapeDtypeStruct((dim,), F32), jax.ShapeDtypeStruct((dim,), F32),
            jax.ShapeDtypeStruct((n_head,), F32),
        )
        return pl.pallas_call(
            functools.partial(_write, n_blk, blk),
            out_shape=finals,
            in_specs=[vmem] * 7,
            out_specs=(hbm,) * 7,
            scratch_shapes=[dma((2, n_blk)), dma((5,))],
            compiler_params=pltpu.CompilerParams(vmem_limit_bytes=1 << 20),
        )(*outs)

    return jax.shard_map(local_block, mesh=mesh, in_specs=in_specs, out_specs=out_specs, check_vma=False)
```

```python
import functools

import jax
import jax.numpy as jnp
from jax import lax
from jax.experimental import pallas as pl
from jax.experimental.pallas import tpu as pltpu
from jax.sharding import PartitionSpec as P

LN_EPS = 1e-6
BF = jnp.bfloat16
F32 = jnp.float32
MESH = pl.DeviceIdType.MESH
WIN = 256
LANES = 128
SUB = 256
VMEM_MAIN = 56 * 1024 * 1024


def _dot(a, b):
    return lax.dot_general(a, b, (((1,), (0,)), ((), ())), preferred_element_type=F32)


def _dot_nt(a, b):
    return lax.dot_general(a, b, (((1,), (1,)), ((), ())), preferred_element_type=F32)


def _column(row):
    return jnp.transpose(jnp.broadcast_to(row, (LANES, row.shape[1])))


def _twice(x):
    return jnp.concatenate([x, x], axis=1)


def _kernel(cfg, x_hbm, gy_hbm, gam_hbm, bet_hbm, wqkv_hbm, wout_hbm, tau_ref,
            x_v, gy_v, dwqkv_ref, dwout_ref, dgam_ref, dbet_ref, dtau_ref,
            x_t, gy_t, u_t, q_t, k_t, v_t, do_t, o_t, dqkv_t,
            mean_v, rstd_v, k1_v, k2_v, w_v, w_t, wo_v, wo_t, gam_v, bet_v, gam_c, bet_c,
            g_lo, g_hi, da_lo, da_hi, sq_acc, sk_acc, dgam_acc, dbet_acc,
            a_f32, scale_f32, g_f32, a_lo, a_hi, at_lo, at_hi, dg_lo, dg_hi, dgt_lo, dgt_hi,
            cq_c, ck_c, srow, rqcol,
            ex1_src, ex1_rc, ex1_x, ex1_fin, ex2_src, ex2_rc, ex2_x, ex2_fin,
            acc_e, acc_l, d2d_e, d2d_l, rs_e, rs_l, ag_e, ag_l,
            gb_src, gb_rc, gb_all,
            x_sem, gy_sem, w_sem,
            ex1_ss, ex1_rs, ex2_ss, ex2_rs,
            d2d_ss, d2d_rs, rs_ss, rs_rs, ag_ss, ag_rs, gb_ss, gb_rs):
    n_chip, n_img, n_blk, blk, dim, n_head = cfg
    hd = dim // n_head
    n_lo = WIN // hd
    r_lo = n_lo * hd
    hi0 = dim - WIN
    off_hi = r_lo - hi0
    r_hi = dim - r_lo
    n_sub = blk // SUB
    inv_d = 1.0 / dim
    data_i = lax.axis_index('data')
    img_i = lax.axis_index('img')
    seq_i = lax.axis_index('seq')
    core = lax.rem(seq_i, 2)
    chip = seq_i // 2

    def dev(chip_to, core_to, img_to):
        return (data_i, img_to, chip_to * 2 + core_to)

    partner = dev(chip, 1 - core, img_i)

    def rcopy(src, dst, ssem, rsem, to):
        return pltpu.make_async_remote_copy(src_ref=src, dst_ref=dst, send_sem=ssem, recv_sem=rsem,
                                            device_id=to, device_id_type=MESH)

    offsets = [(dc, di) for dc in range(n_chip) for di in range(n_img) if (dc, di) != (0, 0)]

    def peer(dc, di):
        return lax.rem(chip + dc, n_chip), lax.rem(img_i + di, n_img)

    def x_copy(i):
        return pltpu.make_async_copy(x_hbm.at[0, pl.ds(i * blk, blk), :], x_v.at[i], x_sem.at[i])

    def gy_copy(i):
        return pltpu.make_async_copy(gy_hbm.at[0, pl.ds(i * blk, blk), :], gy_v.at[i], gy_sem.at[i])

    small = [(gam_hbm, gam_v), (bet_hbm, bet_v), (wqkv_hbm, w_v), (wout_hbm, wo_v)]
    loads = [pltpu.make_async_copy(s, d, w_sem.at[n]) for n, (s, d) in enumerate(small)]
    loads[0].start()
    loads[1].start()
    x_copy(0).start()
    loads[2].start()
    for i in range(1, n_blk):
        x_copy(i).start()
    loads[3].start()
    for i in range(n_blk):
        gy_copy(i).start()

    barrier = pltpu.get_barrier_semaphore()
    pl.semaphore_signal(barrier, inc=1, device_id=partner, device_id_type=MESH)
    for dc, di in offsets:
        pc, pi = peer(dc, di)
        pl.semaphore_signal(barrier, inc=1, device_id=dev(pc, core, pi), device_id_type=MESH)

    spread = n_blk % n_chip == 0
    zero = (da_lo, da_hi, dgam_acc, dbet_acc) + (() if spread else (acc_e, acc_l))
    for ref in zero:
        ref[...] = jnp.zeros_like(ref)

    def sub(n):
        return slice(n * SUB, (n + 1) * SUB)

    def norm(i, cols):
        rows = 48
        cuts = [slice(r, r + rows) for r in range(0, dim, rows)]

        def fold(v):
            t = v[0:8]
            for r in range(8, rows, 8):
                t += v[r:r + 8]
            return t

        s = jnp.zeros((8, LANES), F32)
        for cut in cuts:
            s += fold(x_t[i, cut, cols].astype(F32))
        mean = jnp.sum(s, axis=0, keepdims=True) * inv_d
        s = jnp.zeros((8, LANES), F32)
        for cut in cuts:
            cen = x_t[i, cut, cols].astype(F32) - mean
            s += fold(cen * cen)
        var = jnp.sum(s, axis=0, keepdims=True) * inv_d
        rstd = lax.rsqrt(var + LN_EPS)
        mean_v[i, :, cols] = mean
        rstd_v[i, :, cols] = rstd
        for cut in cuts:
            cen = x_t[i, cut, cols].astype(F32) - mean
            u_t[i, cut, cols] = (cen * rstd * gam_c[cut] + bet_c[cut]).astype(BF)

    def norm_sub(i, n):
        x_t[i, :, sub(n)] = jnp.transpose(x_v[i, sub(n), :])
        for c in range(SUB // LANES):
            norm(i, slice(n * SUB + c * LANES, n * SUB + (c + 1) * LANES))

    for ld in loads:
        ld.wait()
    x_copy(0).wait()
    gam_c[...] = _column(gam_v[...].reshape(1, dim))
    bet_c[...] = _column(bet_v[...].reshape(1, dim))
    for n in range(n_sub):
        norm_sub(0, n)
    for c in range(3):
        w_t[c * dim:(c + 1) * dim, :] = jnp.transpose(w_v[:, c * dim:(c + 1) * dim])
    wo_t[...] = jnp.transpose(wo_v[...])
    for i in range(1, n_blk):
        x_copy(i).wait()
    for i in range(n_blk):
        for n in range(n_sub):
            u_n = u_t[i, :, sub(n)]
            for part, ref in ((0, q_t), (1, k_t)):
                r = _dot(w_t[part * dim:(part + 1) * dim, :], u_n).astype(BF)
                ref[i, :, sub(n)] = r
                rf = r.astype(F32)
                rf = rf * rf
                acc = (sq_acc, sk_acc)[part]
                val = rf[:, :LANES] + rf[:, LANES:]
                if i == 0 and n == 0:
                    acc[...] = val
                else:
                    acc[...] += val
            if i + 1 < n_blk:
                norm_sub(i + 1, n)
        lo = _dot_nt(q_t[i, :r_lo, :], k_t[i, :WIN, :])
        hi = _dot_nt(q_t[i, r_lo:, :], k_t[i, hi0:, :])
        if i == 0:
            g_lo[...] = lo
            g_hi[...] = hi
        else:
            g_lo[...] += lo
            g_hi[...] += hi

    def pack(lo, hi, put):
        col = lax.broadcasted_iota(jnp.int32, (hd, WIN), 1)
        t_lo = jnp.zeros((hd, WIN), F32)
        for h in range(n_lo):
            t_lo += jnp.where((col >= h * hd) & (col < (h + 1) * hd), lo[h * hd:(h + 1) * hd, :], 0.0)
        t_hi = jnp.zeros((hd, WIN), F32)
        for h in range(n_lo, n_head):
            b = h * hd - hi0
            r = h * hd - r_lo
            t_hi += jnp.where((col >= b) & (col < b + hd), hi[r:r + hd, :], 0.0)
        put(jnp.concatenate([t_lo[:, :hi0], t_lo[:, hi0:] + t_hi[:, :WIN - hi0], t_hi[:, WIN - hi0:]], axis=1))

    def ex_pair(src, rc, ss, rs):
        return rcopy(src.at[1 - core], rc, ss.at[0], rs.at[0], partner)

    def ex_chip(buf, ss, rs, dc):
        return rcopy(buf.at[chip], buf.at[chip], ss.at[dc], rs.at[dc], dev(lax.rem(chip + dc, n_chip), core, img_i))

    def ex_swap(fin, ss, rs):
        return rcopy(fin.at[core], fin.at[core], ss.at[n_chip], rs.at[n_chip], partner)

    def ex_step2(src, rc, buf, ss, rs):
        ex_pair(src, rc, ss, rs).wait()
        buf[chip] = src[core] + rc[...]
        for dc in sorted(range(1, n_chip), key=lambda d: -min(d, n_chip - d)):
            ex_chip(buf, ss, rs, dc).start()

    def ex_step3(buf, fin, ss, rs):
        for dc in range(1, n_chip):
            ex_chip(buf, ss, rs, dc).wait()
        tot = buf[0]
        for j in range(1, n_chip):
            tot += buf[j]
        fin[core] = tot
        ex_swap(fin, ss, rs).start()

    def put_g(t):
        h1 = ex1_src.shape[1]
        sq = jnp.sum(jnp.transpose(sq_acc[...]), axis=0, keepdims=True)
        sk = jnp.sum(jnp.transpose(sk_acc[...]), axis=0, keepdims=True)
        ex1_src[0] = t[:h1]
        ex1_src[1, :hd - h1] = t[h1:]
        ex1_src[1, hd - h1:hd - h1 + 8] = jnp.broadcast_to(sq, (8, dim))
        ex1_src[1, hd - h1 + 8:] = jnp.broadcast_to(sk, (8, dim))

    def put_da(t):
        ex2_src[0] = t[:hd // 2]
        ex2_src[1] = t[hd // 2:]

    pack(g_lo, g_hi, put_g)
    pl.semaphore_wait(barrier, 1 + len(offsets))
    ex_pair(ex1_src, ex1_rc, ex1_ss, ex1_rs).start()

    def body_v(i, _):
        gy_copy(i).wait()
        for n in range(n_sub):
            gy_t[i, :, sub(n)] = jnp.transpose(gy_v[i, sub(n), :])
        for n in range(n_sub):
            v_t[i, :, sub(n)] = _dot(w_t[2 * dim:, :], u_t[i, :, sub(n)]).astype(BF)
            do_t[i, :, sub(n)] = _dot(wo_v[...], gy_t[i, :, sub(n)]).astype(BF)
        if spread:
            for acc in (acc_e, acc_l):
                for p in range(2):
                    acc[p, lax.rem(i, n_chip)] = jnp.zeros(acc.shape[2:], F32)
        da_lo[...] += _dot_nt(do_t[i, :r_lo, :], v_t[i, :WIN, :])
        da_hi[...] += _dot_nt(do_t[i, r_lo:, :], v_t[i, hi0:, :])

        @pl.when(i == 0)
        def _():
            ex_step2(ex1_src, ex1_rc, ex1_x, ex1_ss, ex1_rs)
        return 0

    lax.fori_loop(0, n_blk, body_v, 0)

    pack(da_lo, da_hi, put_da)
    ex_pair(ex2_src, ex2_rc, ex2_ss, ex2_rs).start()
    ex_step3(ex1_x, ex1_fin, ex1_ss, ex1_rs)
    ex_step2(ex2_src, ex2_rc, ex2_x, ex2_ss, ex2_rs)
    ex_swap(ex1_fin, ex1_ss, ex1_rs).wait()

    def head_mask(rows, row0, col0):
        r = lax.broadcasted_iota(jnp.int32, (rows, WIN), 0) + row0
        c = lax.broadcasted_iota(jnp.int32, (rows, WIN), 1) + col0
        out = (r < 0)
        for h in range(n_head):
            out |= (r >= h * hd) & (r < (h + 1) * hd) & (c >= h * hd) & (c < (h + 1) * hd)
        return out

    windows = ((0, r_lo, 0, n_lo), (r_lo, r_hi, hi0, n_head - n_lo))
    h1 = ex1_fin.shape[1]
    gcat = jnp.concatenate([ex1_fin[0], ex1_fin[1, :hd - h1]], axis=0)
    sq = ex1_fin[1, hd - h1:hd - h1 + 1]
    sk = ex1_fin[1, hd - h1 + 8:hd - h1 + 9]
    rk = lax.rsqrt(sk)
    srow[0:1] = sk
    srow[1:2] = rk
    sq_c = _column(sq)
    rq_c = lax.rsqrt(sq_c)
    rqcol[0] = sq_c
    rqcol[1] = rq_c
    tau_c = jnp.concatenate([jnp.full((hd, LANES), tau_ref[h], F32) for h in range(n_head)], axis=0)
    rqcol[2] = tau_c
    for w, (row0, rows, col0, heads) in enumerate(windows):
        g = jnp.concatenate([gcat[:, col0:col0 + WIN]] * heads, axis=0)
        mask = head_mask(rows, row0, col0)
        scale = _twice((tau_c * rq_c)[row0:row0 + rows]) * rk[:, col0:col0 + WIN]
        s = g * scale
        top = jnp.max(jnp.where(mask, s, -jnp.inf), axis=1, keepdims=True)
        e = jnp.where(mask, jnp.exp(jnp.where(mask, s - top, 0.0)), 0.0)
        a = e / jnp.sum(e, axis=1, keepdims=True)
        a_f32[row0:row0 + rows] = a
        scale_f32[row0:row0 + rows] = scale
        g_f32[row0:row0 + rows] = g
        if w == 0:
            full = jnp.concatenate([a, jnp.zeros((WIN - rows, WIN), F32)], axis=0)
            a_lo[...] = full.astype(BF)
            at_lo[...] = jnp.transpose(full).astype(BF)
        else:
            full = jnp.concatenate([jnp.zeros((WIN - rows, WIN), F32), a], axis=0)
            a_hi[...] = full.astype(BF)
            at_hi[...] = jnp.transpose(full).astype(BF)

    def add_rows(acc, g, val):
        rb = dim // (2 * n_chip)
        n_a = n_img // 2
        rc = rb // n_a
        for s in range(2 * n_chip):
            for a in range(n_a):
                acc[s % 2, s // 2, 2 * a + g] += val[s * rb + a * rc:s * rb + (a + 1) * rc]

    def body_ov(i, _):
        for n in range(n_sub):
            o_t[i, :r_lo, sub(n)] = _dot(a_lo[:r_lo], v_t[i, :WIN, sub(n)]).astype(BF)
            o_t[i, r_lo:, sub(n)] = _dot(a_hi[off_hi:], v_t[i, hi0:, sub(n)]).astype(BF)
            dqkv_t[i, 2 * dim:2 * dim + r_lo, sub(n)] = _dot(at_lo[:r_lo], do_t[i, :WIN, sub(n)]).astype(BF)
            dqkv_t[i, 2 * dim + r_lo:, sub(n)] = _dot(at_hi[off_hi:], do_t[i, hi0:, sub(n)]).astype(BF)
        add_rows(acc_e, 0, _dot(o_t[i], gy_v[i]))
        add_rows(acc_e, 1, _dot_nt(u_t[i], dqkv_t[i, 2 * dim:, :]))
        return 0

    lax.fori_loop(0, n_blk, body_ov, 0)

    def pair_copy(r, acc, buf):
        return rcopy(acc.at[1 - core], buf, d2d_ss.at[r], d2d_rs.at[r], partner)

    def rs_copy(r, acc, buf, n):
        pc, pi = peer(*offsets[n])
        return rcopy(acc.at[core, pc, pi], buf.at[n], rs_ss.at[r, n], rs_rs.at[r, n], dev(pc, core, pi))

    def ag_copy(r, buf, di):
        return rcopy(buf.at[img_i], buf.at[img_i], ag_ss.at[r, di], ag_rs.at[r, di],
                     dev(chip, core, lax.rem(img_i + di, n_img)))

    def rs_start(r, acc, buf, rbuf):
        pair_copy(r, acc, buf).wait()
        for j in range(n_chip):
            acc[core, j] += buf[j]
        for n in range(len(offsets)):
            rs_copy(r, acc, rbuf, n).start()

    def rs_finish(r, acc, rbuf, gbuf):
        tot = acc[core, chip, img_i]
        for n in range(len(offsets)):
            rs_copy(r, acc, rbuf, n).wait()
            tot += rbuf[n]
        gbuf[img_i] = tot
        for di in range(1, n_img):
            ag_copy(r, gbuf, di).start()

    pair_copy(0, acc_e, d2d_e).start()
    ex_step3(ex2_x, ex2_fin, ex2_ss, ex2_rs)
    ex_swap(ex2_fin, ex2_ss, ex2_rs).wait()

    dacat = jnp.concatenate([ex2_fin[0], ex2_fin[1]], axis=0)
    sq_c = rqcol[0]
    rq_c = rqcol[1]
    tau_c = rqcol[2]
    sk = srow[0:1]
    rk = srow[1:2]
    row_sums = []
    col_sums = []
    for w, (row0, rows, col0, heads) in enumerate(windows):
        da = jnp.concatenate([dacat[:, col0:col0 + WIN]] * heads, axis=0)
        a = a_f32[row0:row0 + rows]
        ds = a * (da - jnp.sum(a * da, axis=1, keepdims=True))
        dg = ds * scale_f32[row0:row0 + rows]
        dscale = ds * g_f32[row0:row0 + rows]
        row_sums.append(jnp.broadcast_to(jnp.sum(dscale * rk[:, col0:col0 + WIN], axis=1, keepdims=True),
                                         (rows, LANES)))
        col_sums.append(jnp.sum(dscale * _twice((tau_c * rq_c)[row0:row0 + rows]), axis=0, keepdims=True))
        if w == 0:
            full = jnp.concatenate([dg, jnp.zeros((WIN - rows, WIN), F32)], axis=0)
            dg_lo[...] = full.astype(BF)
            dgt_lo[...] = jnp.transpose(full).astype(BF)
        else:
            full = jnp.concatenate([jnp.zeros((WIN - rows, WIN), F32), dg], axis=0)
            dg_hi[...] = full.astype(BF)
            dgt_hi[...] = jnp.transpose(full).astype(BF)
    t_row = jnp.concatenate(row_sums, axis=0)
    cl, ch = col_sums
    w_col = jnp.concatenate([cl[:, :hi0], cl[:, hi0:] + ch[:, :WIN - hi0], ch[:, WIN - hi0:]], axis=1)
    cq_c[...] = 2.0 * (-0.5 * rq_c / sq_c * (tau_c * t_row))
    ck_c[...] = _column(2.0 * (-0.5 * rk / sk * w_col))
    lane = lax.broadcasted_iota(jnp.int32, (1, LANES), 1)
    dtau_row = jnp.zeros((1, LANES), F32)
    for h in range(n_head):
        part = jnp.sum((rq_c * t_row)[h * hd:(h + 1) * hd], axis=0, keepdims=True)
        dtau_row += jnp.where(lane == h, part, 0.0)
    gb_src[6:7] = jnp.where(seq_i == 0, dtau_row, 0.0)
    gb_src[7:8] = jnp.zeros((1, LANES), F32)

    rs_start(0, acc_e, d2d_e, rs_e)

    def body_qk_back(i, _):
        for n in range(n_sub):
            k_n = k_t[i, :, sub(n)]
            q_n = q_t[i, :, sub(n)]
            dq = jnp.concatenate([_dot(dg_lo[:r_lo], k_n[:WIN]), _dot(dg_hi[off_hi:], k_n[hi0:])], axis=0)
            dqkv_t[i, :dim, sub(n)] = (dq + _twice(cq_c[...]) * q_n.astype(F32)).astype(BF)
            dk = jnp.concatenate([_dot(dgt_lo[:r_lo], q_n[:WIN]), _dot(dgt_hi[off_hi:], q_n[hi0:])], axis=0)
            dqkv_t[i, dim:2 * dim, sub(n)] = (dk + _twice(ck_c[...]) * k_n.astype(F32)).astype(BF)
        dw = _dot_nt(u_t[i], dqkv_t[i, :2 * dim, :])
        add_rows(acc_l, 0, dw[:, :dim])
        add_rows(acc_l, 1, dw[:, dim:])
        return 0

    lax.fori_loop(0, n_blk, body_qk_back, 0)
    pair_copy(1, acc_l, d2d_l).start()

    def body_du(i, _):
        for n in range(n_sub):
            du = _dot(w_v[...], dqkv_t[i, :, sub(n)]).astype(BF)
            do_t[i, :, sub(n)] = du
            for c in range(SUB // LANES):
                cols = slice(n * SUB + c * LANES, n * SUB + (c + 1) * LANES)
                du_c = du[:, c * LANES:(c + 1) * LANES].astype(F32)
                rstd = rstd_v[i, :, cols]
                xh = (x_t[i, :, cols].astype(F32) - mean_v[i, :, cols]) * rstd
                p = du_c * xh
                dgam_acc[...] += p
                dbet_acc[...] += du_c
                c1 = jnp.sum(du_c * gam_c[...], axis=0, keepdims=True) * inv_d
                c2 = jnp.sum(p * gam_c[...], axis=0, keepdims=True) * inv_d
                k1_v[i, :, cols] = rstd * c1
                k2_v[i, :, cols] = rstd * rstd * c2

        @pl.when(i == min(1, n_blk - 1))
        def _():
            rs_start(1, acc_l, d2d_l, rs_l)
        return 0

    lax.fori_loop(0, n_blk, body_du, 0)

    for b, acc in ((0, dgam_acc), (dim // LANES, dbet_acc)):
        row = jnp.sum(jnp.transpose(acc[...]), axis=0, keepdims=True)
        for c in range(dim // LANES):
            gb_src[b + c:b + c + 1] = row[:, c * LANES:(c + 1) * LANES]
    gb_pair = rcopy(gb_src, gb_rc, gb_ss.at[0], gb_rs.at[0], partner)
    gb_pair.start()

    def gb_copy(n):
        pc, pi = peer(*offsets[n])
        return rcopy(gb_all.at[chip, img_i], gb_all.at[chip, img_i], gb_ss.at[1 + n], gb_rs.at[1 + n],
                     dev(pc, core, pi))

    rs_finish(0, acc_e, rs_e, ag_e)

    def body_x(i, _):
        for n in range(n_sub):
            proj = _dot(wo_t[...], o_t[i, :, sub(n)])
            x_v[i, sub(n), :] = jnp.transpose((x_t[i, :, sub(n)].astype(F32) + proj).astype(BF))
            for c in range(SUB // LANES):
                cols = slice(n * SUB + c * LANES, n * SUB + (c + 1) * LANES)
                g = do_t[i, :, cols].astype(F32) * gam_c[...] * rstd_v[i, :, cols]
                cen = x_t[i, :, cols].astype(F32) - mean_v[i, :, cols]
                gx = gy_t[i, :, cols].astype(F32) + (g - k1_v[i, :, cols] - cen * k2_v[i, :, cols])
                gy_v[i, cols, :] = jnp.transpose(gx.astype(BF))

        @pl.when(i == 0)
        def _():
            gb_pair.wait()
            gb_all[chip, img_i] = gb_src[...] + gb_rc[...]
            for n in range(len(offsets)):
                gb_copy(n).start()
        return 0

    lax.fori_loop(0, n_blk, body_x, 0)
    rs_finish(1, acc_l, rs_l, ag_l)

    def emit(r, gbuf, outs):
        for di in range(1, n_img):
            ag_copy(r, gbuf, di).wait()
        rc = gbuf.shape[1]
        for a in range(n_img // 2):
            for g, (ref, col) in enumerate(outs):
                ref[a * rc:(a + 1) * rc, col:col + dim] = gbuf[2 * a + g]

    emit(0, ag_e, ((dwout_ref, 0), (dwqkv_ref, 2 * dim)))
    for n in range(len(offsets)):
        gb_copy(n).wait()
    tot = jnp.zeros(gb_src.shape, F32)
    for j in range(n_chip):
        for m in range(n_img):
            tot += gb_all[j, m]
    n_row = dim // LANES
    for b, ref in ((0, dgam_ref), (n_row, dbet_ref)):
        ref[...] = jnp.concatenate([tot[b + c:b + c + 1] for c in range(n_row)], axis=1).reshape(dim)
    dtau_ref[...] = tot[6:7, :n_head].reshape(n_head)
    emit(1, ag_l, ((dwqkv_ref, 0), (dwqkv_ref, dim)))


def _write(n_blk, blk, *refs):
    srcs, dsts, act_sem, sem = refs[:7], refs[7:14], refs[14], refs[15]
    copies = []
    for a in range(2):
        for i in range(n_blk):
            copies.append(pltpu.make_async_copy(srcs[a].at[i], dsts[a].at[0, pl.ds(i * blk, blk), :],
                                                act_sem.at[a, i]))
    for n in range(5):
        copies.append(pltpu.make_async_copy(srcs[2 + n], dsts[2 + n], sem.at[n]))
    for c in copies:
        c.start()
    for c in copies:
        c.wait()


def solution(mesh):
    act_spec = P(('data', 'img'), 'seq', None)
    row_spec = P(('data', 'seq'), None)
    in_specs = (act_spec, act_spec, P(), P(), P(), P(), P())
    out_specs = (act_spec, act_spec, row_spec, row_spec, P('data'), P('data'), P('data'))
    n_img = mesh.shape['img']
    n_seq = mesh.shape['seq']
    n_chip = n_seq // 2

    def local_block(x_in, grad_y, ln_gamma, ln_beta, w_qkv, w_out, head_temp):
        _, n_tok, dim = x_in.shape
        n_head = head_temp.shape[0]
        hd = dim // n_head
        blk = min(1024, n_tok)
        n_blk = n_tok // blk
        rb = dim // n_seq
        rc = rb // (n_img // 2)
        h1 = (hd + 16) // 2
        hbm = pl.BlockSpec(memory_space=pltpu.HBM)
        vmem = pl.BlockSpec(memory_space=pltpu.VMEM)
        smem = pl.BlockSpec(memory_space=pltpu.SMEM)
        V = pltpu.VMEM
        n_off = n_chip * n_img - 1
        n_hi = n_head - WIN // hd
        r_hi = n_hi * hd
        r_lo = dim - r_hi
        feat = V((n_blk, dim, blk), BF)
        stat = V((n_blk, 1, blk), F32)
        col = V((dim, LANES), F32)
        sqr = V((WIN, WIN), BF)
        acc = V((2, n_chip, n_img, rc, dim), F32)
        dma = pltpu.SemaphoreType.DMA
        scratch = [
            feat, feat, feat, feat, feat, feat, feat, feat, V((n_blk, 3 * dim, blk), BF),
            stat, stat, stat, stat, V((dim, 3 * dim), BF), V((3 * dim, dim), BF), V((dim, dim), BF), V((dim, dim), BF),
            V((dim,), F32), V((dim,), F32), col, col,
            V((r_lo, WIN), F32), V((r_hi, WIN), F32), V((r_lo, WIN), F32), V((r_hi, WIN), F32),
            col, col, col, col,
            V((dim, WIN), F32), V((dim, WIN), F32), V((dim, WIN), F32),
            sqr, sqr, sqr, sqr, sqr, sqr, sqr, sqr,
            col, col, V((8, dim), F32), V((3, dim, LANES), F32),
            V((2, h1, dim), F32), V((h1, dim), F32), V((n_chip, h1, dim), F32), V((2, h1, dim), F32),
            V((2, hd // 2, dim), F32), V((hd // 2, dim), F32), V((n_chip, hd // 2, dim), F32),
            V((2, hd // 2, dim), F32),
            acc, acc, V((n_chip, n_img, rc, dim), F32), V((n_chip, n_img, rc, dim), F32),
            V((n_off, rc, dim), F32), V((n_off, rc, dim), F32), V((n_img, rc, dim), F32), V((n_img, rc, dim), F32),
            V((8, LANES), F32), V((8, LANES), F32), V((n_chip, n_img, 8, LANES), F32),
            dma((n_blk,)), dma((n_blk,)), dma((4,)),
            dma((n_chip + 1,)), dma((n_chip + 1,)), dma((n_chip + 1,)), dma((n_chip + 1,)),
            dma((2,)), dma((2,)), dma((2, n_off)), dma((2, n_off)), dma((2, n_img)), dma((2, n_img)),
            dma((1 + n_off,)), dma((1 + n_off,)),
        ]
        out_shape = (
            V((n_blk, blk, dim), BF), V((n_blk, blk, dim), BF), V((rb, 3 * dim), F32), V((rb, dim), F32),
            V((dim,), F32), V((dim,), F32), V((n_head,), F32),
        )
        cfg = (n_chip, n_img, n_blk, blk, dim, n_head)
        outs = pl.pallas_call(
            functools.partial(_kernel, cfg),
            out_shape=out_shape,
            in_specs=[hbm, hbm, hbm, hbm, hbm, hbm, smem],
            out_specs=(vmem,) * 7,
            scratch_shapes=scratch,
            compiler_params=pltpu.CompilerParams(collective_id=0, has_side_effects=True,
                                                 vmem_limit_bytes=VMEM_MAIN),
        )(x_in, grad_y, ln_gamma, ln_beta, w_qkv, w_out, head_temp)
        finals = (
            jax.ShapeDtypeStruct(x_in.shape, BF), jax.ShapeDtypeStruct(x_in.shape, BF),
            jax.ShapeDtypeStruct((rb, 3 * dim), F32), jax.ShapeDtypeStruct((rb, dim), F32),
            jax.ShapeDtypeStruct((dim,), F32), jax.ShapeDtypeStruct((dim,), F32),
            jax.ShapeDtypeStruct((n_head,), F32),
        )
        return pl.pallas_call(
            functools.partial(_write, n_blk, blk),
            out_shape=finals,
            in_specs=[vmem] * 7,
            out_specs=(hbm,) * 7,
            scratch_shapes=[dma((2, n_blk)), dma((5,))],
            compiler_params=pltpu.CompilerParams(vmem_limit_bytes=1 << 20),
        )(*outs)

    return jax.shard_map(local_block, mesh=mesh, in_specs=in_specs, out_specs=out_specs, check_vma=False)
```

```python
import functools

import jax
import jax.numpy as jnp
from jax import lax
from jax.experimental import pallas as pl
from jax.experimental.pallas import tpu as pltpu
from jax.sharding import PartitionSpec as P

LN_EPS = 1e-6
BF = jnp.bfloat16
F32 = jnp.float32
MESH = pl.DeviceIdType.MESH
WIN = 256
LANES = 128
SUB = 256
VMEM_MAIN = 56 * 1024 * 1024


def _dot(a, b):
    return lax.dot_general(a, b, (((1,), (0,)), ((), ())), preferred_element_type=F32)


def _dot_nt(a, b):
    return lax.dot_general(a, b, (((1,), (1,)), ((), ())), preferred_element_type=F32)


def _column(row):
    return jnp.transpose(jnp.broadcast_to(row, (LANES, row.shape[1])))


def _twice(x):
    return jnp.concatenate([x, x], axis=1)


def _kernel(cfg, x_hbm, gy_hbm, gam_hbm, bet_hbm, wqkv_hbm, wout_hbm, tau_ref,
            x_v, gy_v, dwqkv_ref, dwout_ref, dgam_ref, dbet_ref, dtau_ref,
            x_t, gy_t, u_t, q_t, k_t, v_t, do_t, o_t, dqkv_t,
            mean_v, rstd_v, k1_v, k2_v, w_v, w_t, wo_v, wo_t, gam_v, bet_v, gam_c, bet_c,
            g_lo, g_hi, da_lo, da_hi, sq_acc, sk_acc, dgam_acc, dbet_acc,
            a_f32, scale_f32, g_f32, a_lo, a_hi, at_lo, at_hi, dg_lo, dg_hi, dgt_lo, dgt_hi,
            cq_c, ck_c, srow, rqcol,
            ex1_src, ex1_rc, ex1_x, ex1_fin, ex2_src, ex2_rc, ex2_x, ex2_fin,
            acc_e, acc_q, acc_k, d2d_e, d2d_q, d2d_k, ring1, ring2, yrs_e, ag_e, rs_q, rs_k, ag_q, ag_k,
            gb_src, gb_rc, gb_all,
            x_sem, gy_sem, w_sem,
            ex1_ss, ex1_rs, ex2_ss, ex2_rs,
            d2d_ss, d2d_rs, ring_ss, ring_rs, yrs_ss, yrs_rs, age_ss, age_rs,
            rs_ss, rs_rs, ag_ss, ag_rs, gb_ss, gb_rs):
    n_chip, n_img, n_blk, blk, dim, n_head = cfg
    hd = dim // n_head
    n_lo = WIN // hd
    r_lo = n_lo * hd
    hi0 = dim - WIN
    off_hi = r_lo - hi0
    r_hi = dim - r_lo
    n_sub = blk // SUB
    inv_d = 1.0 / dim
    data_i = lax.axis_index('data')
    img_i = lax.axis_index('img')
    seq_i = lax.axis_index('seq')
    core = lax.rem(seq_i, 2)
    chip = seq_i // 2

    def dev(chip_to, core_to, img_to):
        return (data_i, img_to, chip_to * 2 + core_to)

    partner = dev(chip, 1 - core, img_i)

    def rcopy(src, dst, ssem, rsem, to):
        return pltpu.make_async_remote_copy(src_ref=src, dst_ref=dst, send_sem=ssem, recv_sem=rsem,
                                            device_id=to, device_id_type=MESH)

    offsets = [(dc, di) for dc in range(n_chip) for di in range(n_img) if (dc, di) != (0, 0)]

    def peer(dc, di):
        return lax.rem(chip + dc, n_chip), lax.rem(img_i + di, n_img)

    def x_copy(i):
        return pltpu.make_async_copy(x_hbm.at[0, pl.ds(i * blk, blk), :], x_v.at[i], x_sem.at[i])

    def gy_copy(i):
        return pltpu.make_async_copy(gy_hbm.at[0, pl.ds(i * blk, blk), :], gy_v.at[i], gy_sem.at[i])

    small = [(gam_hbm, gam_v), (bet_hbm, bet_v), (wqkv_hbm, w_v), (wout_hbm, wo_v)]
    loads = [pltpu.make_async_copy(s, d, w_sem.at[n]) for n, (s, d) in enumerate(small)]
    loads[0].start()
    loads[1].start()
    x_copy(0).start()
    loads[2].start()
    for i in range(1, n_blk):
        x_copy(i).start()
    loads[3].start()
    for i in range(n_blk):
        gy_copy(i).start()

    barrier = pltpu.get_barrier_semaphore()
    pl.semaphore_signal(barrier, inc=1, device_id=partner, device_id_type=MESH)
    for dc, di in offsets:
        pc, pi = peer(dc, di)
        pl.semaphore_signal(barrier, inc=1, device_id=dev(pc, core, pi), device_id_type=MESH)

    spread = n_blk % n_chip == 0
    zero = (da_lo, da_hi, dgam_acc, dbet_acc) + (() if spread else (acc_e,))
    for ref in zero:
        ref[...] = jnp.zeros_like(ref)

    def sub(n):
        return slice(n * SUB, (n + 1) * SUB)

    def norm(i, cols):
        rows = 48
        cuts = [slice(r, r + rows) for r in range(0, dim, rows)]

        def fold(v):
            t = v[0:8]
            for r in range(8, rows, 8):
                t += v[r:r + 8]
            return t

        s = jnp.zeros((8, LANES), F32)
        for cut in cuts:
            s += fold(x_t[i, cut, cols].astype(F32))
        mean = jnp.sum(s, axis=0, keepdims=True) * inv_d
        s = jnp.zeros((8, LANES), F32)
        for cut in cuts:
            cen = x_t[i, cut, cols].astype(F32) - mean
            s += fold(cen * cen)
        var = jnp.sum(s, axis=0, keepdims=True) * inv_d
        rstd = lax.rsqrt(var + LN_EPS)
        mean_v[i, :, cols] = mean
        rstd_v[i, :, cols] = rstd
        for cut in cuts:
            cen = x_t[i, cut, cols].astype(F32) - mean
            u_t[i, cut, cols] = (cen * rstd * gam_c[cut] + bet_c[cut]).astype(BF)

    def norm_sub(i, n):
        x_t[i, :, sub(n)] = jnp.transpose(x_v[i, sub(n), :])
        for c in range(SUB // LANES):
            norm(i, slice(n * SUB + c * LANES, n * SUB + (c + 1) * LANES))

    for ld in loads:
        ld.wait()
    x_copy(0).wait()
    gam_c[...] = _column(gam_v[...].reshape(1, dim))
    bet_c[...] = _column(bet_v[...].reshape(1, dim))
    for n in range(n_sub):
        norm_sub(0, n)
    for c in range(3):
        w_t[c * dim:(c + 1) * dim, :] = jnp.transpose(w_v[:, c * dim:(c + 1) * dim])
    wo_t[...] = jnp.transpose(wo_v[...])
    for i in range(1, n_blk):
        x_copy(i).wait()
    for i in range(n_blk):
        for n in range(n_sub):
            u_n = u_t[i, :, sub(n)]
            for part, ref in ((0, q_t), (1, k_t)):
                r = _dot(w_t[part * dim:(part + 1) * dim, :], u_n).astype(BF)
                ref[i, :, sub(n)] = r
                rf = r.astype(F32)
                rf = rf * rf
                acc = (sq_acc, sk_acc)[part]
                val = rf[:, :LANES] + rf[:, LANES:]
                if i == 0 and n == 0:
                    acc[...] = val
                else:
                    acc[...] += val
            if i + 1 < n_blk:
                norm_sub(i + 1, n)
        lo = _dot_nt(q_t[i, :r_lo, :], k_t[i, :WIN, :])
        hi = _dot_nt(q_t[i, r_lo:, :], k_t[i, hi0:, :])
        if i == 0:
            g_lo[...] = lo
            g_hi[...] = hi
        else:
            g_lo[...] += lo
            g_hi[...] += hi

    def pack(lo, hi, put):
        col = lax.broadcasted_iota(jnp.int32, (hd, WIN), 1)
        t_lo = jnp.zeros((hd, WIN), F32)
        for h in range(n_lo):
            t_lo += jnp.where((col >= h * hd) & (col < (h + 1) * hd), lo[h * hd:(h + 1) * hd, :], 0.0)
        t_hi = jnp.zeros((hd, WIN), F32)
        for h in range(n_lo, n_head):
            b = h * hd - hi0
            r = h * hd - r_lo
            t_hi += jnp.where((col >= b) & (col < b + hd), hi[r:r + hd, :], 0.0)
        put(jnp.concatenate([t_lo[:, :hi0], t_lo[:, hi0:] + t_hi[:, :WIN - hi0], t_hi[:, WIN - hi0:]], axis=1))

    def ex_pair(src, rc, ss, rs):
        return rcopy(src.at[1 - core], rc, ss.at[0], rs.at[0], partner)

    def ex_chip(buf, ss, rs, dc):
        return rcopy(buf.at[chip], buf.at[chip], ss.at[dc], rs.at[dc], dev(lax.rem(chip + dc, n_chip), core, img_i))

    def ex_swap(fin, ss, rs):
        return rcopy(fin.at[core], fin.at[core], ss.at[n_chip], rs.at[n_chip], partner)

    def ex_step2(src, rc, buf, ss, rs):
        ex_pair(src, rc, ss, rs).wait()
        buf[chip] = src[core] + rc[...]
        for dc in sorted(range(1, n_chip), key=lambda d: -min(d, n_chip - d)):
            ex_chip(buf, ss, rs, dc).start()

    def ex_step3(buf, fin, ss, rs):
        for dc in range(1, n_chip):
            ex_chip(buf, ss, rs, dc).wait()
        tot = buf[0]
        for j in range(1, n_chip):
            tot += buf[j]
        fin[core] = tot
        ex_swap(fin, ss, rs).start()

    def put_g(t):
        h1 = ex1_src.shape[1]
        sq = jnp.sum(jnp.transpose(sq_acc[...]), axis=0, keepdims=True)
        sk = jnp.sum(jnp.transpose(sk_acc[...]), axis=0, keepdims=True)
        ex1_src[0] = t[:h1]
        ex1_src[1, :hd - h1] = t[h1:]
        ex1_src[1, hd - h1:hd - h1 + 8] = jnp.broadcast_to(sq, (8, dim))
        ex1_src[1, hd - h1 + 8:] = jnp.broadcast_to(sk, (8, dim))

    def put_da(t):
        ex2_src[0] = t[:hd // 2]
        ex2_src[1] = t[hd // 2:]

    pack(g_lo, g_hi, put_g)
    pl.semaphore_wait(barrier, 1 + len(offsets))
    ex_pair(ex1_src, ex1_rc, ex1_ss, ex1_rs).start()

    def body_v(i, _):
        gy_copy(i).wait()
        for n in range(n_sub):
            gy_t[i, :, sub(n)] = jnp.transpose(gy_v[i, sub(n), :])
        for n in range(n_sub):
            v_t[i, :, sub(n)] = _dot(w_t[2 * dim:, :], u_t[i, :, sub(n)]).astype(BF)
            do_t[i, :, sub(n)] = _dot(wo_v[...], gy_t[i, :, sub(n)]).astype(BF)
        if spread:
            for p in range(2):
                acc_e[p, lax.rem(i, n_chip)] = jnp.zeros(acc_e.shape[2:], F32)
        da_lo[...] += _dot_nt(do_t[i, :r_lo, :], v_t[i, :WIN, :])
        da_hi[...] += _dot_nt(do_t[i, r_lo:, :], v_t[i, hi0:, :])

        @pl.when(i == 0)
        def _():
            ex_step2(ex1_src, ex1_rc, ex1_x, ex1_ss, ex1_rs)
        return 0

    lax.fori_loop(0, n_blk, body_v, 0)

    pack(da_lo, da_hi, put_da)
    ex_pair(ex2_src, ex2_rc, ex2_ss, ex2_rs).start()
    ex_step3(ex1_x, ex1_fin, ex1_ss, ex1_rs)
    ex_step2(ex2_src, ex2_rc, ex2_x, ex2_ss, ex2_rs)
    ex_swap(ex1_fin, ex1_ss, ex1_rs).wait()

    def head_mask(rows, row0, col0):
        r = lax.broadcasted_iota(jnp.int32, (rows, WIN), 0) + row0
        c = lax.broadcasted_iota(jnp.int32, (rows, WIN), 1) + col0
        out = (r < 0)
        for h in range(n_head):
            out |= (r >= h * hd) & (r < (h + 1) * hd) & (c >= h * hd) & (c < (h + 1) * hd)
        return out

    windows = ((0, r_lo, 0, n_lo), (r_lo, r_hi, hi0, n_head - n_lo))
    h1 = ex1_fin.shape[1]
    gcat = jnp.concatenate([ex1_fin[0], ex1_fin[1, :hd - h1]], axis=0)
    sq = ex1_fin[1, hd - h1:hd - h1 + 1]
    sk = ex1_fin[1, hd - h1 + 8:hd - h1 + 9]
    rk = lax.rsqrt(sk)
    srow[0:1] = sk
    srow[1:2] = rk
    sq_c = _column(sq)
    rq_c = lax.rsqrt(sq_c)
    rqcol[0] = sq_c
    rqcol[1] = rq_c
    tau_c = jnp.concatenate([jnp.full((hd, LANES), tau_ref[h], F32) for h in range(n_head)], axis=0)
    rqcol[2] = tau_c
    for w, (row0, rows, col0, heads) in enumerate(windows):
        g = jnp.concatenate([gcat[:, col0:col0 + WIN]] * heads, axis=0)
        mask = head_mask(rows, row0, col0)
        scale = _twice((tau_c * rq_c)[row0:row0 + rows]) * rk[:, col0:col0 + WIN]
        s = g * scale
        top = jnp.max(jnp.where(mask, s, -jnp.inf), axis=1, keepdims=True)
        e = jnp.where(mask, jnp.exp(jnp.where(mask, s - top, 0.0)), 0.0)
        a = e / jnp.sum(e, axis=1, keepdims=True)
        a_f32[row0:row0 + rows] = a
        scale_f32[row0:row0 + rows] = scale
        g_f32[row0:row0 + rows] = g
        if w == 0:
            full = jnp.concatenate([a, jnp.zeros((WIN - rows, WIN), F32)], axis=0)
            a_lo[...] = full.astype(BF)
            at_lo[...] = jnp.transpose(full).astype(BF)
        else:
            full = jnp.concatenate([jnp.zeros((WIN - rows, WIN), F32), a], axis=0)
            a_hi[...] = full.astype(BF)
            at_hi[...] = jnp.transpose(full).astype(BF)

    def add_rows(acc, g, val):
        rb = dim // (2 * n_chip)
        n_a = n_img // 2
        rc = rb // n_a
        for s in range(2 * n_chip):
            for a in range(n_a):
                acc[s % 2, s // 2, 2 * a + g] += val[s * rb + a * rc:s * rb + (a + 1) * rc]

    n_ct = dim // LANES

    def add_cols(acc, val, first):
        rb = dim // (2 * n_chip)
        for s in range(2 * n_chip):
            for ct in range(n_ct):
                part = val[s * rb:(s + 1) * rb, ct * LANES:(ct + 1) * LANES]
                if first:
                    acc[s % 2, s // 2, ct] = part
                else:
                    acc[s % 2, s // 2, ct] += part

    def body_ov(i, _):
        for n in range(n_sub):
            o_t[i, :r_lo, sub(n)] = _dot(a_lo[:r_lo], v_t[i, :WIN, sub(n)]).astype(BF)
            o_t[i, r_lo:, sub(n)] = _dot(a_hi[off_hi:], v_t[i, hi0:, sub(n)]).astype(BF)
            dqkv_t[i, 2 * dim:2 * dim + r_lo, sub(n)] = _dot(at_lo[:r_lo], do_t[i, :WIN, sub(n)]).astype(BF)
            dqkv_t[i, 2 * dim + r_lo:, sub(n)] = _dot(at_hi[off_hi:], do_t[i, hi0:, sub(n)]).astype(BF)
        add_rows(acc_e, 0, _dot(o_t[i], gy_v[i]))
        add_rows(acc_e, 1, _dot_nt(u_t[i], dqkv_t[i, 2 * dim:, :]))

        @pl.when(i == max(n_blk - 2, 0))
        def _():
            ex_step3(ex2_x, ex2_fin, ex2_ss, ex2_rs)
        return 0

    lax.fori_loop(0, n_blk, body_ov, 0)

    def pair_copy(r, acc, buf):
        return rcopy(acc.at[1 - core], buf, d2d_ss.at[r], d2d_rs.at[r], partner)

    hn = n_img // 2
    right = lax.rem(chip + 1, n_chip)
    left = lax.rem(chip + n_chip - 1, n_chip)
    opp = lax.rem(chip + 2, n_chip)

    def ring_copy(n):
        to = dev((right, left)[n % 2], core, img_i)
        if n == 0:
            src, dst = acc_e.at[core, opp, pl.ds(0, hn)], ring1.at[0]
        elif n == 1:
            src, dst = acc_e.at[core, opp, pl.ds(hn, hn)], ring1.at[1]
        else:
            src, dst = acc_e.at[core, (right, left)[n % 2]], ring2.at[n % 2]
        return rcopy(src, dst, ring_ss.at[n], ring_rs.at[n], to)

    def yrs_copy(di):
        pi = lax.rem(img_i + di, n_img)
        return rcopy(acc_e.at[core, chip, pi], yrs_e.at[di - 1], yrs_ss.at[di - 1], yrs_rs.at[di - 1],
                     dev(chip, core, pi))

    def age_copy(di):
        return rcopy(ag_e.at[img_i], ag_e.at[img_i], age_ss.at[di - 1], age_rs.at[di - 1],
                     dev(chip, core, lax.rem(img_i + di, n_img)))

    def e_step1():
        pair_copy(0, acc_e, d2d_e).wait()
        for j in range(n_chip):
            acc_e[core, j] += d2d_e[j]
        ring_copy(0).start()
        ring_copy(1).start()

    def e_step2():
        ring_copy(0).wait()
        ring_copy(1).wait()
        acc_e[core, right, :hn] += ring1[0]
        acc_e[core, left, hn:] += ring1[1]
        ring_copy(2).start()
        ring_copy(3).start()

    def e_step3():
        ring_copy(2).wait()
        ring_copy(3).wait()
        acc_e[core, chip] += ring2[0] + ring2[1]
        for di in range(1, n_img):
            yrs_copy(di).start()

    def e_step4():
        tot = acc_e[core, chip, img_i]
        for di in range(1, n_img):
            yrs_copy(di).wait()
            tot += yrs_e[di - 1]
        ag_e[img_i] = tot
        for di in range(1, n_img):
            age_copy(di).start()

    def owner(r, ct):
        return (2 * r + ct) % n_img

    def rs_copy(r, acc, buf, ct, dc):
        pc = lax.rem(chip + dc, n_chip)
        sl = ct // n_img
        return rcopy(acc.at[core, pc, ct], buf.at[sl, dc, img_i], rs_ss.at[r, ct, dc], rs_rs.at[r, sl, dc, img_i],
                     dev(pc, core, owner(r, ct)))

    def each_send(r, do):
        for dc in range(n_chip):
            for ct in range(n_ct):
                if dc:
                    do(ct, dc)
                else:
                    pl.when(img_i != owner(r, ct))(functools.partial(do, ct, dc))

    def rs_start(r, acc, d2d, buf):
        pair_copy(1 + r, acc, d2d).wait()
        for j in range(n_chip):
            acc[core, j] += d2d[j]
        each_send(r, lambda ct, dc: rs_copy(r, acc, buf, ct, dc).start())

    def ag_copy(r, gbuf, ct, di):
        return rcopy(gbuf.at[ct], gbuf.at[ct], ag_ss.at[r, ct, di - 1], ag_rs.at[r, ct],
                     dev(chip, core, lax.rem(img_i + di, n_img)))

    def rs_finish(r, acc, buf, gbuf):
        for ct in range(n_ct):
            @pl.when(img_i == owner(r, ct))
            def _(ct=ct):
                sl = ct // n_img
                tot = acc[core, chip, ct]
                for dc in range(n_chip):
                    for im in range(n_img):
                        if dc == 0 and im == owner(r, ct):
                            continue
                        rcopy(buf.at[sl, dc, im], buf.at[sl, dc, im], rs_ss.at[r, ct, dc], rs_rs.at[r, sl, dc, im],
                              partner).wait_recv()
                        tot += buf[sl, dc, im]
                gbuf[ct] = tot
                for di in range(1, n_img):
                    ag_copy(r, gbuf, ct, di).start()

    def rs_end(r, acc, buf, gbuf, ref, col):
        each_send(r, lambda ct, dc: rs_copy(r, acc, buf, ct, dc).wait_send())
        for ct in range(n_ct):
            @pl.when(img_i == owner(r, ct))
            def _(ct=ct):
                for di in range(1, n_img):
                    ag_copy(r, gbuf, ct, di).wait_send()

            @pl.when(img_i != owner(r, ct))
            def _(ct=ct):
                ag_copy(r, gbuf, ct, 1).wait_recv()
            ref[:, col + ct * LANES:col + (ct + 1) * LANES] = gbuf[ct]

    pair_copy(0, acc_e, d2d_e).start()
    ex_swap(ex2_fin, ex2_ss, ex2_rs).wait()

    dacat = jnp.concatenate([ex2_fin[0], ex2_fin[1]], axis=0)
    sq_c = rqcol[0]
    rq_c = rqcol[1]
    tau_c = rqcol[2]
    sk = srow[0:1]
    rk = srow[1:2]
    row_sums = []
    col_sums = []
    for w, (row0, rows, col0, heads) in enumerate(windows):
        da = jnp.concatenate([dacat[:, col0:col0 + WIN]] * heads, axis=0)
        a = a_f32[row0:row0 + rows]
        ds = a * (da - jnp.sum(a * da, axis=1, keepdims=True))
        dg = ds * scale_f32[row0:row0 + rows]
        dscale = ds * g_f32[row0:row0 + rows]
        row_sums.append(jnp.broadcast_to(jnp.sum(dscale * rk[:, col0:col0 + WIN], axis=1, keepdims=True),
                                         (rows, LANES)))
        col_sums.append(jnp.sum(dscale * _twice((tau_c * rq_c)[row0:row0 + rows]), axis=0, keepdims=True))
        if w == 0:
            full = jnp.concatenate([dg, jnp.zeros((WIN - rows, WIN), F32)], axis=0)
            dg_lo[...] = full.astype(BF)
            dgt_lo[...] = jnp.transpose(full).astype(BF)
        else:
            full = jnp.concatenate([jnp.zeros((WIN - rows, WIN), F32), dg], axis=0)
            dg_hi[...] = full.astype(BF)
            dgt_hi[...] = jnp.transpose(full).astype(BF)
    t_row = jnp.concatenate(row_sums, axis=0)
    cl, ch = col_sums
    w_col = jnp.concatenate([cl[:, :hi0], cl[:, hi0:] + ch[:, :WIN - hi0], ch[:, WIN - hi0:]], axis=1)
    cq_c[...] = 2.0 * (-0.5 * rq_c / sq_c * (tau_c * t_row))
    ck_c[...] = _column(2.0 * (-0.5 * rk / sk * w_col))
    lane = lax.broadcasted_iota(jnp.int32, (1, LANES), 1)
    dtau_row = jnp.zeros((1, LANES), F32)
    for h in range(n_head):
        part = jnp.sum((rq_c * t_row)[h * hd:(h + 1) * hd], axis=0, keepdims=True)
        dtau_row += jnp.where(lane == h, part, 0.0)
    gb_src[6:7] = jnp.where(seq_i == 0, dtau_row, 0.0)
    gb_src[7:8] = jnp.zeros((1, LANES), F32)

    def back(i, part):
        lo, hi, a_t, b_t, c = ((dg_lo, dg_hi, k_t, q_t, cq_c), (dgt_lo, dgt_hi, q_t, k_t, ck_c))[part]
        base = part * dim
        for n in range(n_sub):
            a_n = a_t[i, :, sub(n)]
            d = jnp.concatenate([_dot(lo[:r_lo], a_n[:WIN]), _dot(hi[off_hi:], a_n[hi0:])], axis=0)
            dqkv_t[i, base:base + dim, sub(n)] = (d + _twice(c[...]) * b_t[i, :, sub(n)].astype(F32)).astype(BF)
        add_cols((acc_q, acc_k)[part], _dot_nt(u_t[i], dqkv_t[i, base:base + dim, :]), i == 0)

    back(0, 0)
    e_step1()
    for i in range(1, n_blk):
        back(i, 0)
    pair_copy(1, acc_q, d2d_q).start()
    for i in range(n_blk):
        back(i, 1)
        if i == min(1, n_blk - 1):
            rs_start(0, acc_q, d2d_q, rs_q)
            e_step2()
    pair_copy(2, acc_k, d2d_k).start()

    def body_du(i, _):
        for n in range(n_sub):
            du = _dot(w_v[...], dqkv_t[i, :, sub(n)]).astype(BF)
            do_t[i, :, sub(n)] = du
            for c in range(SUB // LANES):
                cols = slice(n * SUB + c * LANES, n * SUB + (c + 1) * LANES)
                du_c = du[:, c * LANES:(c + 1) * LANES].astype(F32)
                rstd = rstd_v[i, :, cols]
                xh = (x_t[i, :, cols].astype(F32) - mean_v[i, :, cols]) * rstd
                p = du_c * xh
                dgam_acc[...] += p
                dbet_acc[...] += du_c
                c1 = jnp.sum(du_c * gam_c[...], axis=0, keepdims=True) * inv_d
                c2 = jnp.sum(p * gam_c[...], axis=0, keepdims=True) * inv_d
                k1_v[i, :, cols] = rstd * c1
                k2_v[i, :, cols] = rstd * rstd * c2

        @pl.when(i == 0)
        def _():
            rs_start(1, acc_k, d2d_k, rs_k)

        @pl.when(i == min(2, n_blk - 1))
        def _():
            e_step3()
        return 0

    lax.fori_loop(0, n_blk, body_du, 0)

    for b, acc in ((0, dgam_acc), (dim // LANES, dbet_acc)):
        row = jnp.sum(jnp.transpose(acc[...]), axis=0, keepdims=True)
        for c in range(dim // LANES):
            gb_src[b + c:b + c + 1] = row[:, c * LANES:(c + 1) * LANES]
    gb_pair = rcopy(gb_src, gb_rc, gb_ss.at[0], gb_rs.at[0], partner)
    gb_pair.start()

    def gb_copy(n):
        pc, pi = peer(*offsets[n])
        return rcopy(gb_all.at[chip, img_i], gb_all.at[chip, img_i], gb_ss.at[1 + n], gb_rs.at[1 + n],
                     dev(pc, core, pi))

    rs_finish(0, acc_q, rs_q, ag_q)

    def body_x(i, _):
        for n in range(n_sub):
            proj = _dot(wo_t[...], o_t[i, :, sub(n)])
            x_v[i, sub(n), :] = jnp.transpose((x_t[i, :, sub(n)].astype(F32) + proj).astype(BF))
            for c in range(SUB // LANES):
                cols = slice(n * SUB + c * LANES, n * SUB + (c + 1) * LANES)
                g = do_t[i, :, cols].astype(F32) * gam_c[...] * rstd_v[i, :, cols]
                cen = x_t[i, :, cols].astype(F32) - mean_v[i, :, cols]
                gx = gy_t[i, :, cols].astype(F32) + (g - k1_v[i, :, cols] - cen * k2_v[i, :, cols])
                gy_v[i, cols, :] = jnp.transpose(gx.astype(BF))

        @pl.when(i == 0)
        def _():
            gb_pair.wait()
            gb_all[chip, img_i] = gb_src[...] + gb_rc[...]
            for n in range(len(offsets)):
                gb_copy(n).start()
            e_step4()

        @pl.when(i == max(n_blk - 2, 0))
        def _():
            rs_finish(1, acc_k, rs_k, ag_k)
        return 0

    lax.fori_loop(0, n_blk, body_x, 0)
    for n in range(len(offsets)):
        gb_copy(n).wait()
    tot = jnp.zeros(gb_src.shape, F32)
    for j in range(n_chip):
        for m in range(n_img):
            tot += gb_all[j, m]
    n_row = dim // LANES
    for b, ref in ((0, dgam_ref), (n_row, dbet_ref)):
        ref[...] = jnp.concatenate([tot[b + c:b + c + 1] for c in range(n_row)], axis=1).reshape(dim)
    dtau_ref[...] = tot[6:7, :n_head].reshape(n_head)
    rs_end(0, acc_q, rs_q, ag_q, dwqkv_ref, 0)
    for di in range(1, n_img):
        age_copy(di).wait()
    rc = ag_e.shape[1]
    for a in range(hn):
        for g, (ref, col) in enumerate(((dwout_ref, 0), (dwqkv_ref, 2 * dim))):
            ref[a * rc:(a + 1) * rc, col:col + dim] = ag_e[2 * a + g]
    rs_end(1, acc_k, rs_k, ag_k, dwqkv_ref, dim)


def _write(n_blk, blk, *refs):
    srcs, dsts, act_sem, sem = refs[:7], refs[7:14], refs[14], refs[15]
    copies = []
    for a in range(2):
        for i in range(n_blk):
            copies.append(pltpu.make_async_copy(srcs[a].at[i], dsts[a].at[0, pl.ds(i * blk, blk), :],
                                                act_sem.at[a, i]))
    for n in range(5):
        copies.append(pltpu.make_async_copy(srcs[2 + n], dsts[2 + n], sem.at[n]))
    for c in copies:
        c.start()
    for c in copies:
        c.wait()


def solution(mesh):
    act_spec = P(('data', 'img'), 'seq', None)
    row_spec = P(('data', 'seq'), None)
    in_specs = (act_spec, act_spec, P(), P(), P(), P(), P())
    out_specs = (act_spec, act_spec, row_spec, row_spec, P('data'), P('data'), P('data'))
    n_img = mesh.shape['img']
    n_seq = mesh.shape['seq']
    n_chip = n_seq // 2

    def local_block(x_in, grad_y, ln_gamma, ln_beta, w_qkv, w_out, head_temp):
        _, n_tok, dim = x_in.shape
        n_head = head_temp.shape[0]
        hd = dim // n_head
        blk = min(1024, n_tok)
        n_blk = n_tok // blk
        rb = dim // n_seq
        rc = rb // (n_img // 2)
        h1 = (hd + 16) // 2
        hbm = pl.BlockSpec(memory_space=pltpu.HBM)
        vmem = pl.BlockSpec(memory_space=pltpu.VMEM)
        smem = pl.BlockSpec(memory_space=pltpu.SMEM)
        V = pltpu.VMEM
        n_off = n_chip * n_img - 1
        n_hi = n_head - WIN // hd
        r_hi = n_hi * hd
        r_lo = dim - r_hi
        feat = V((n_blk, dim, blk), BF)
        stat = V((n_blk, 1, blk), F32)
        col = V((dim, LANES), F32)
        sqr = V((WIN, WIN), BF)
        acc = V((2, n_chip, n_img, rc, dim), F32)
        n_ct = dim // LANES
        n_sl = -(-n_ct // n_img)
        accc = V((2, n_chip, n_ct, rb, LANES), F32)
        dma = pltpu.SemaphoreType.DMA
        scratch = [
            feat, feat, feat, feat, feat, feat, feat, feat, V((n_blk, 3 * dim, blk), BF),
            stat, stat, stat, stat, V((dim, 3 * dim), BF), V((3 * dim, dim), BF), V((dim, dim), BF), V((dim, dim), BF),
            V((dim,), F32), V((dim,), F32), col, col,
            V((r_lo, WIN), F32), V((r_hi, WIN), F32), V((r_lo, WIN), F32), V((r_hi, WIN), F32),
            col, col, col, col,
            V((dim, WIN), F32), V((dim, WIN), F32), V((dim, WIN), F32),
            sqr, sqr, sqr, sqr, sqr, sqr, sqr, sqr,
            col, col, V((8, dim), F32), V((3, dim, LANES), F32),
            V((2, h1, dim), F32), V((h1, dim), F32), V((n_chip, h1, dim), F32), V((2, h1, dim), F32),
            V((2, hd // 2, dim), F32), V((hd // 2, dim), F32), V((n_chip, hd // 2, dim), F32),
            V((2, hd // 2, dim), F32),
            acc, accc, accc, V((n_chip, n_img, rc, dim), F32), V((n_chip, n_ct, rb, LANES), F32),
            V((n_chip, n_ct, rb, LANES), F32), V((2, n_img // 2, rc, dim), F32), V((2, n_img, rc, dim), F32),
            V((n_img - 1, rc, dim), F32), V((n_img, rc, dim), F32), V((n_sl, n_chip, n_img, rb, LANES), F32),
            V((n_sl, n_chip, n_img, rb, LANES), F32), V((n_ct, rb, LANES), F32), V((n_ct, rb, LANES), F32),
            V((8, LANES), F32), V((8, LANES), F32), V((n_chip, n_img, 8, LANES), F32),
            dma((n_blk,)), dma((n_blk,)), dma((4,)),
            dma((n_chip + 1,)), dma((n_chip + 1,)), dma((n_chip + 1,)), dma((n_chip + 1,)),
            dma((3,)), dma((3,)), dma((4,)), dma((4,)), dma((n_img - 1,)), dma((n_img - 1,)),
            dma((n_img - 1,)), dma((n_img - 1,)),
            dma((2, n_ct, n_chip)), dma((2, n_sl, n_chip, n_img)), dma((2, n_ct, n_img - 1)), dma((2, n_ct)),
            dma((1 + n_off,)), dma((1 + n_off,)),
        ]
        out_shape = (
            V((n_blk, blk, dim), BF), V((n_blk, blk, dim), BF), V((rb, 3 * dim), F32), V((rb, dim), F32),
            V((dim,), F32), V((dim,), F32), V((n_head,), F32),
        )
        cfg = (n_chip, n_img, n_blk, blk, dim, n_head)
        outs = pl.pallas_call(
            functools.partial(_kernel, cfg),
            out_shape=out_shape,
            in_specs=[hbm, hbm, hbm, hbm, hbm, hbm, smem],
            out_specs=(vmem,) * 7,
            scratch_shapes=scratch,
            compiler_params=pltpu.CompilerParams(collective_id=0, has_side_effects=True,
                                                 vmem_limit_bytes=VMEM_MAIN),
        )(x_in, grad_y, ln_gamma, ln_beta, w_qkv, w_out, head_temp)
        finals = (
            jax.ShapeDtypeStruct(x_in.shape, BF), jax.ShapeDtypeStruct(x_in.shape, BF),
            jax.ShapeDtypeStruct((rb, 3 * dim), F32), jax.ShapeDtypeStruct((rb, dim), F32),
            jax.ShapeDtypeStruct((dim,), F32), jax.ShapeDtypeStruct((dim,), F32),
            jax.ShapeDtypeStruct((n_head,), F32),
        )
        return pl.pallas_call(
            functools.partial(_write, n_blk, blk),
            out_shape=finals,
            in_specs=[vmem] * 7,
            out_specs=(hbm,) * 7,
            scratch_shapes=[dma((2, n_blk)), dma((5,))],
            compiler_params=pltpu.CompilerParams(vmem_limit_bytes=1 << 20),
        )(*outs)

    return jax.shard_map(local_block, mesh=mesh, in_specs=in_specs, out_specs=out_specs, check_vma=False)
```

```python
import functools

import jax
import jax.numpy as jnp
from jax import lax
from jax.experimental import pallas as pl
from jax.experimental.pallas import tpu as pltpu
from jax.sharding import PartitionSpec as P

LN_EPS = 1e-6
BF = jnp.bfloat16
F32 = jnp.float32
MESH = pl.DeviceIdType.MESH
WIN = 256
LANES = 128
SUB = 256
VMEM_MAIN = 56 * 1024 * 1024


def _dot(a, b):
    return lax.dot_general(a, b, (((1,), (0,)), ((), ())), preferred_element_type=F32)


def _dot_nt(a, b):
    return lax.dot_general(a, b, (((1,), (1,)), ((), ())), preferred_element_type=F32)


def _column(row):
    return jnp.transpose(jnp.broadcast_to(row, (LANES, row.shape[1])))


def _twice(x):
    return jnp.concatenate([x, x], axis=1)


def _kernel(cfg, x_hbm, gy_hbm, gam_hbm, bet_hbm, wqkv_hbm, wout_hbm, tau_ref,
            x_v, gy_v, dwqkv_ref, dwout_ref, dgam_ref, dbet_ref, dtau_ref,
            x_t, gy_t, u_t, q_t, k_t, v_t, do_t, o_t, dqkv_t,
            mean_v, rstd_v, k1_v, k2_v, w_v, w_t, wo_v, wo_t, gam_v, bet_v, gam_c, bet_c,
            g_lo, g_hi, da_lo, da_hi, sq_acc, sk_acc, dgam_acc, dbet_acc,
            a_f32, scale_f32, g_f32, a_lo, a_hi, at_lo, at_hi, dg_lo, dg_hi, dgt_lo, dgt_hi,
            cq_c, ck_c, srow, rqcol,
            ex1_src, ex1_rc, ex1_x, ex1_fin, ex2_src, ex2_rc, ex2_x, ex2_fin,
            acc_e, acc_q, acc_k, d2d_e, d2d_q, d2d_k, ring1, ring2, yrs_e, ag_e, rs_q, rs_k, ag_q, ag_k,
            gb_src, gb_rc, gb_all,
            x_sem, gy_sem, w_sem,
            ex1_ss, ex1_rs, ex2_ss, ex2_rs,
            d2d_ss, d2d_rs, ring_ss, ring_rs, yrs_ss, yrs_rs, age_ss, age_rs,
            rs_ss, rs_rs, ag_ss, ag_rs, gb_ss, gb_rs):
    n_chip, n_img, n_blk, blk, dim, n_head = cfg
    hd = dim // n_head
    n_lo = WIN // hd
    r_lo = n_lo * hd
    hi0 = dim - WIN
    off_hi = r_lo - hi0
    r_hi = dim - r_lo
    n_sub = blk // SUB
    inv_d = 1.0 / dim
    data_i = lax.axis_index('data')
    img_i = lax.axis_index('img')
    seq_i = lax.axis_index('seq')
    core = lax.rem(seq_i, 2)
    chip = seq_i // 2

    def dev(chip_to, core_to, img_to):
        return (data_i, img_to, chip_to * 2 + core_to)

    partner = dev(chip, 1 - core, img_i)

    def rcopy(src, dst, ssem, rsem, to):
        return pltpu.make_async_remote_copy(src_ref=src, dst_ref=dst, send_sem=ssem, recv_sem=rsem,
                                            device_id=to, device_id_type=MESH)

    offsets = [(dc, di) for dc in range(n_chip) for di in range(n_img) if (dc, di) != (0, 0)]

    def peer(dc, di):
        return lax.rem(chip + dc, n_chip), lax.rem(img_i + di, n_img)

    def x_copy(i):
        return pltpu.make_async_copy(x_hbm.at[0, pl.ds(i * blk, blk), :], x_v.at[i], x_sem.at[i])

    def gy_copy(i):
        return pltpu.make_async_copy(gy_hbm.at[0, pl.ds(i * blk, blk), :], gy_v.at[i], gy_sem.at[i])

    small = [(gam_hbm, gam_v), (bet_hbm, bet_v), (wqkv_hbm, w_v), (wout_hbm, wo_v)]
    loads = [pltpu.make_async_copy(s, d, w_sem.at[n]) for n, (s, d) in enumerate(small)]
    loads[0].start()
    loads[1].start()
    x_copy(0).start()
    loads[2].start()
    loads[3].start()

    barrier = pltpu.get_barrier_semaphore()
    pl.semaphore_signal(barrier, inc=1, device_id=partner, device_id_type=MESH)
    for dc, di in offsets:
        pc, pi = peer(dc, di)
        pl.semaphore_signal(barrier, inc=1, device_id=dev(pc, core, pi), device_id_type=MESH)

    for i in range(1, n_blk):
        x_copy(i).start()

    zero = (dgam_acc, dbet_acc)
    for ref in zero:
        ref[...] = jnp.zeros_like(ref)

    def sub(n):
        return slice(n * SUB, (n + 1) * SUB)

    def norm(i, cols):
        rows = 48
        cuts = [slice(r, r + rows) for r in range(0, dim, rows)]

        def fold(v):
            t = v[0:8]
            for r in range(8, rows, 8):
                t += v[r:r + 8]
            return t

        s = jnp.zeros((8, LANES), F32)
        for cut in cuts:
            s += fold(x_t[i, cut, cols].astype(F32))
        mean = jnp.sum(s, axis=0, keepdims=True) * inv_d
        s = jnp.zeros((8, LANES), F32)
        for cut in cuts:
            cen = x_t[i, cut, cols].astype(F32) - mean
            s += fold(cen * cen)
        var = jnp.sum(s, axis=0, keepdims=True) * inv_d
        rstd = lax.rsqrt(var + LN_EPS)
        mean_v[i, :, cols] = mean
        rstd_v[i, :, cols] = rstd
        for cut in cuts:
            cen = x_t[i, cut, cols].astype(F32) - mean
            u_t[i, cut, cols] = (cen * rstd * gam_c[cut] + bet_c[cut]).astype(BF)

    def norm_sub(i, n):
        x_t[i, :, sub(n)] = jnp.transpose(x_v[i, sub(n), :])
        for c in range(SUB // LANES):
            norm(i, slice(n * SUB + c * LANES, n * SUB + (c + 1) * LANES))

    for ld in loads:
        ld.wait()
    x_copy(0).wait()
    gam_c[...] = _column(gam_v[...].reshape(1, dim))
    bet_c[...] = _column(bet_v[...].reshape(1, dim))
    for n in range(n_sub):
        norm_sub(0, n)
    for c in range(3):
        w_t[c * dim:(c + 1) * dim, :] = jnp.transpose(w_v[:, c * dim:(c + 1) * dim])
    wo_t[...] = jnp.transpose(wo_v[...])
    for i in range(1, n_blk):
        x_copy(i).wait()
    for i in range(n_blk):
        gy_copy(i).start()
    for i in range(n_blk):
        for n in range(n_sub):
            u_n = u_t[i, :, sub(n)]
            for part, ref in ((0, q_t), (1, k_t)):
                r = _dot(w_t[part * dim:(part + 1) * dim, :], u_n).astype(BF)
                ref[i, :, sub(n)] = r
                rf = r.astype(F32)
                rf = rf * rf
                acc = (sq_acc, sk_acc)[part]
                val = rf[:, :LANES] + rf[:, LANES:]
                if i == 0 and n == 0:
                    acc[...] = val
                else:
                    acc[...] += val
            if i + 1 < n_blk:
                norm_sub(i + 1, n)
        lo = _dot_nt(q_t[i, :r_lo, :], k_t[i, :WIN, :])
        hi = _dot_nt(q_t[i, r_lo:, :], k_t[i, hi0:, :])
        if i == 0:
            g_lo[...] = lo
            g_hi[...] = hi
        else:
            g_lo[...] += lo
            g_hi[...] += hi

    def pack(lo, hi, put):
        col = lax.broadcasted_iota(jnp.int32, (hd, WIN), 1)
        t_lo = jnp.zeros((hd, WIN), F32)
        for h in range(n_lo):
            t_lo += jnp.where((col >= h * hd) & (col < (h + 1) * hd), lo[h * hd:(h + 1) * hd, :], 0.0)
        t_hi = jnp.zeros((hd, WIN), F32)
        for h in range(n_lo, n_head):
            b = h * hd - hi0
            r = h * hd - r_lo
            t_hi += jnp.where((col >= b) & (col < b + hd), hi[r:r + hd, :], 0.0)
        put(jnp.concatenate([t_lo[:, :hi0], t_lo[:, hi0:] + t_hi[:, :WIN - hi0], t_hi[:, WIN - hi0:]], axis=1))

    def ex_pair(src, rc, ss, rs):
        return rcopy(src.at[1 - core], rc, ss.at[0], rs.at[0], partner)

    def ex_chip(buf, ss, rs, dc):
        return rcopy(buf.at[chip], buf.at[chip], ss.at[dc], rs.at[dc], dev(lax.rem(chip + dc, n_chip), core, img_i))

    def ex_swap(fin, ss, rs):
        return rcopy(fin.at[core], fin.at[core], ss.at[n_chip], rs.at[n_chip], partner)

    def ex_step2(src, rc, buf, ss, rs):
        ex_pair(src, rc, ss, rs).wait()
        buf[chip] = src[core] + rc[...]
        for dc in sorted(range(1, n_chip), key=lambda d: -min(d, n_chip - d)):
            ex_chip(buf, ss, rs, dc).start()

    def ex_step3(buf, fin, ss, rs):
        for dc in range(1, n_chip):
            ex_chip(buf, ss, rs, dc).wait()
        tot = buf[0]
        for j in range(1, n_chip):
            tot += buf[j]
        fin[core] = tot
        ex_swap(fin, ss, rs).start()

    def put_g(t):
        h1 = ex1_src.shape[1]
        sq = jnp.sum(jnp.transpose(sq_acc[...]), axis=0, keepdims=True)
        sk = jnp.sum(jnp.transpose(sk_acc[...]), axis=0, keepdims=True)
        ex1_src[0] = t[:h1]
        ex1_src[1, :hd - h1] = t[h1:]
        ex1_src[1, hd - h1:hd - h1 + 8] = jnp.broadcast_to(sq, (8, dim))
        ex1_src[1, hd - h1 + 8:] = jnp.broadcast_to(sk, (8, dim))

    def put_da(t):
        ex2_src[0] = t[:hd // 2]
        ex2_src[1] = t[hd // 2:]

    pack(g_lo, g_hi, put_g)
    pl.semaphore_wait(barrier, 1 + len(offsets))
    ex_pair(ex1_src, ex1_rc, ex1_ss, ex1_rs).start()

    for i in range(n_blk):
        gy_copy(i).wait()
    for i in range(n_blk):
        for n in range(n_sub):
            gy_t[i, :, sub(n)] = jnp.transpose(gy_v[i, sub(n), :])
            v_t[i, :, sub(n)] = _dot(w_t[2 * dim:, :], u_t[i, :, sub(n)]).astype(BF)
            do_t[i, :, sub(n)] = _dot(wo_v[...], gy_t[i, :, sub(n)]).astype(BF)
        lo = _dot_nt(do_t[i, :r_lo, :], v_t[i, :WIN, :])
        hi = _dot_nt(do_t[i, r_lo:, :], v_t[i, hi0:, :])
        if i == 0:
            da_lo[...] = lo
            da_hi[...] = hi
            ex_step2(ex1_src, ex1_rc, ex1_x, ex1_ss, ex1_rs)
        else:
            da_lo[...] += lo
            da_hi[...] += hi

    pack(da_lo, da_hi, put_da)
    ex_pair(ex2_src, ex2_rc, ex2_ss, ex2_rs).start()
    ex_step3(ex1_x, ex1_fin, ex1_ss, ex1_rs)
    ex_step2(ex2_src, ex2_rc, ex2_x, ex2_ss, ex2_rs)
    ex_swap(ex1_fin, ex1_ss, ex1_rs).wait()

    def head_mask(rows, row0, col0):
        r = lax.broadcasted_iota(jnp.int32, (rows, WIN), 0) + row0
        c = lax.broadcasted_iota(jnp.int32, (rows, WIN), 1) + col0
        out = (r < 0)
        for h in range(n_head):
            out |= (r >= h * hd) & (r < (h + 1) * hd) & (c >= h * hd) & (c < (h + 1) * hd)
        return out

    windows = ((0, r_lo, 0, n_lo), (r_lo, r_hi, hi0, n_head - n_lo))
    h1 = ex1_fin.shape[1]
    gcat = jnp.concatenate([ex1_fin[0], ex1_fin[1, :hd - h1]], axis=0)
    sq = ex1_fin[1, hd - h1:hd - h1 + 1]
    sk = ex1_fin[1, hd - h1 + 8:hd - h1 + 9]
    rk = lax.rsqrt(sk)
    srow[0:1] = sk
    srow[1:2] = rk
    sq_c = _column(sq)
    rq_c = lax.rsqrt(sq_c)
    rqcol[0] = sq_c
    rqcol[1] = rq_c
    tau_c = jnp.concatenate([jnp.full((hd, LANES), tau_ref[h], F32) for h in range(n_head)], axis=0)
    rqcol[2] = tau_c
    for w, (row0, rows, col0, heads) in enumerate(windows):
        g = jnp.concatenate([gcat[:, col0:col0 + WIN]] * heads, axis=0)
        mask = head_mask(rows, row0, col0)
        scale = _twice((tau_c * rq_c)[row0:row0 + rows]) * rk[:, col0:col0 + WIN]
        s = g * scale
        top = jnp.max(jnp.where(mask, s, -jnp.inf), axis=1, keepdims=True)
        e = jnp.where(mask, jnp.exp(jnp.where(mask, s - top, 0.0)), 0.0)
        a = e / jnp.sum(e, axis=1, keepdims=True)
        a_f32[row0:row0 + rows] = a
        scale_f32[row0:row0 + rows] = scale
        g_f32[row0:row0 + rows] = g
        if w == 0:
            full = jnp.concatenate([a, jnp.zeros((WIN - rows, WIN), F32)], axis=0)
            a_lo[...] = full.astype(BF)
            at_lo[...] = jnp.transpose(full).astype(BF)
        else:
            full = jnp.concatenate([jnp.zeros((WIN - rows, WIN), F32), a], axis=0)
            a_hi[...] = full.astype(BF)
            at_hi[...] = jnp.transpose(full).astype(BF)

    def add_rows(acc, g, val, first):
        rb = dim // (2 * n_chip)
        n_a = n_img // 2
        rc = rb // n_a
        for s in range(2 * n_chip):
            for a in range(n_a):
                part = val[s * rb + a * rc:s * rb + (a + 1) * rc]
                if first:
                    acc[s % 2, s // 2, 2 * a + g] = part
                else:
                    acc[s % 2, s // 2, 2 * a + g] += part

    n_ct = dim // LANES

    def add_cols(acc, val, first):
        rb = dim // (2 * n_chip)
        for s in range(2 * n_chip):
            for ct in range(n_ct):
                part = val[s * rb:(s + 1) * rb, ct * LANES:(ct + 1) * LANES]
                if first:
                    acc[s % 2, s // 2, ct] = part
                else:
                    acc[s % 2, s // 2, ct] += part

    for i in range(n_blk):
        for n in range(n_sub):
            o_t[i, :r_lo, sub(n)] = _dot(a_lo[:r_lo], v_t[i, :WIN, sub(n)]).astype(BF)
            o_t[i, r_lo:, sub(n)] = _dot(a_hi[off_hi:], v_t[i, hi0:, sub(n)]).astype(BF)
            dqkv_t[i, 2 * dim:2 * dim + r_lo, sub(n)] = _dot(at_lo[:r_lo], do_t[i, :WIN, sub(n)]).astype(BF)
            dqkv_t[i, 2 * dim + r_lo:, sub(n)] = _dot(at_hi[off_hi:], do_t[i, hi0:, sub(n)]).astype(BF)
        add_rows(acc_e, 0, _dot(o_t[i], gy_v[i]), i == 0)
        add_rows(acc_e, 1, _dot_nt(u_t[i], dqkv_t[i, 2 * dim:, :]), i == 0)
        if i == max(n_blk - 2, 0):
            ex_step3(ex2_x, ex2_fin, ex2_ss, ex2_rs)

    def pair_copy(r, acc, buf):
        return rcopy(acc.at[1 - core], buf, d2d_ss.at[r], d2d_rs.at[r], partner)

    hn = n_img // 2
    right = lax.rem(chip + 1, n_chip)
    left = lax.rem(chip + n_chip - 1, n_chip)
    opp = lax.rem(chip + 2, n_chip)

    def ring_copy(n):
        to = dev((right, left)[n % 2], core, img_i)
        if n == 0:
            src, dst = acc_e.at[core, opp, pl.ds(0, hn)], ring1.at[0]
        elif n == 1:
            src, dst = acc_e.at[core, opp, pl.ds(hn, hn)], ring1.at[1]
        else:
            src, dst = acc_e.at[core, (right, left)[n % 2]], ring2.at[n % 2]
        return rcopy(src, dst, ring_ss.at[n], ring_rs.at[n], to)

    def yrs_copy(di):
        pi = lax.rem(img_i + di, n_img)
        return rcopy(acc_e.at[core, chip, pi], yrs_e.at[di - 1], yrs_ss.at[di - 1], yrs_rs.at[di - 1],
                     dev(chip, core, pi))

    def age_copy(di):
        return rcopy(ag_e.at[img_i], ag_e.at[img_i], age_ss.at[di - 1], age_rs.at[di - 1],
                     dev(chip, core, lax.rem(img_i + di, n_img)))

    def e_step1():
        pair_copy(0, acc_e, d2d_e).wait()
        for j in range(n_chip):
            acc_e[core, j] += d2d_e[j]
        ring_copy(0).start()
        ring_copy(1).start()

    def e_step2():
        ring_copy(0).wait()
        ring_copy(1).wait()
        acc_e[core, right, :hn] += ring1[0]
        acc_e[core, left, hn:] += ring1[1]
        ring_copy(2).start()
        ring_copy(3).start()

    def e_step3():
        ring_copy(2).wait()
        ring_copy(3).wait()
        acc_e[core, chip] += ring2[0] + ring2[1]
        for di in range(1, n_img):
            yrs_copy(di).start()

    def e_step4():
        tot = acc_e[core, chip, img_i]
        for di in range(1, n_img):
            yrs_copy(di).wait()
            tot += yrs_e[di - 1]
        ag_e[img_i] = tot
        for di in range(1, n_img):
            age_copy(di).start()

    def owner(r, ct):
        return (2 * r + ct) % n_img

    def rs_copy(r, acc, buf, ct, dc):
        pc = lax.rem(chip + dc, n_chip)
        sl = ct // n_img
        return rcopy(acc.at[core, pc, ct], buf.at[sl, dc, img_i], rs_ss.at[r, ct, dc], rs_rs.at[r, sl, dc, img_i],
                     dev(pc, core, owner(r, ct)))

    def each_send(r, do):
        for dc in range(n_chip):
            for ct in range(n_ct):
                if dc:
                    do(ct, dc)
                else:
                    pl.when(img_i != owner(r, ct))(functools.partial(do, ct, dc))

    def rs_start(r, acc, d2d, buf):
        pair_copy(1 + r, acc, d2d).wait()
        for j in range(n_chip):
            acc[core, j] += d2d[j]
        each_send(r, lambda ct, dc: rs_copy(r, acc, buf, ct, dc).start())

    def ag_copy(r, gbuf, ct, di):
        return rcopy(gbuf.at[ct], gbuf.at[ct], ag_ss.at[r, ct, di - 1], ag_rs.at[r, ct],
                     dev(chip, core, lax.rem(img_i + di, n_img)))

    def rs_finish(r, acc, buf, gbuf):
        for ct in range(n_ct):
            @pl.when(img_i == owner(r, ct))
            def _(ct=ct):
                sl = ct // n_img
                tot = acc[core, chip, ct]
                for dc in range(n_chip):
                    for im in range(n_img):
                        if dc == 0 and im == owner(r, ct):
                            continue
                        rcopy(buf.at[sl, dc, im], buf.at[sl, dc, im], rs_ss.at[r, ct, dc], rs_rs.at[r, sl, dc, im],
                              partner).wait_recv()
                        tot += buf[sl, dc, im]
                gbuf[ct] = tot
                for di in range(1, n_img):
                    ag_copy(r, gbuf, ct, di).start()

    def rs_end(r, acc, buf, gbuf, ref, col):
        each_send(r, lambda ct, dc: rs_copy(r, acc, buf, ct, dc).wait_send())
        for ct in range(n_ct):
            @pl.when(img_i == owner(r, ct))
            def _(ct=ct):
                for di in range(1, n_img):
                    ag_copy(r, gbuf, ct, di).wait_send()

            @pl.when(img_i != owner(r, ct))
            def _(ct=ct):
                ag_copy(r, gbuf, ct, 1).wait_recv()
            ref[:, col + ct * LANES:col + (ct + 1) * LANES] = gbuf[ct]

    pair_copy(0, acc_e, d2d_e).start()
    ex_swap(ex2_fin, ex2_ss, ex2_rs).wait()

    dacat = jnp.concatenate([ex2_fin[0], ex2_fin[1]], axis=0)
    sq_c = rqcol[0]
    rq_c = rqcol[1]
    tau_c = rqcol[2]
    sk = srow[0:1]
    rk = srow[1:2]
    row_sums = []
    col_sums = []
    for w, (row0, rows, col0, heads) in enumerate(windows):
        da = jnp.concatenate([dacat[:, col0:col0 + WIN]] * heads, axis=0)
        a = a_f32[row0:row0 + rows]
        ds = a * (da - jnp.sum(a * da, axis=1, keepdims=True))
        dg = ds * scale_f32[row0:row0 + rows]
        dscale = ds * g_f32[row0:row0 + rows]
        row_sums.append(jnp.broadcast_to(jnp.sum(dscale * rk[:, col0:col0 + WIN], axis=1, keepdims=True),
                                         (rows, LANES)))
        col_sums.append(jnp.sum(dscale * _twice((tau_c * rq_c)[row0:row0 + rows]), axis=0, keepdims=True))
        if w == 0:
            full = jnp.concatenate([dg, jnp.zeros((WIN - rows, WIN), F32)], axis=0)
            dg_lo[...] = full.astype(BF)
            dgt_lo[...] = jnp.transpose(full).astype(BF)
        else:
            full = jnp.concatenate([jnp.zeros((WIN - rows, WIN), F32), dg], axis=0)
            dg_hi[...] = full.astype(BF)
            dgt_hi[...] = jnp.transpose(full).astype(BF)
    t_row = jnp.concatenate(row_sums, axis=0)
    cl, ch = col_sums
    w_col = jnp.concatenate([cl[:, :hi0], cl[:, hi0:] + ch[:, :WIN - hi0], ch[:, WIN - hi0:]], axis=1)
    cq_c[...] = 2.0 * (-0.5 * rq_c / sq_c * (tau_c * t_row))
    ck_c[...] = _column(2.0 * (-0.5 * rk / sk * w_col))
    lane = lax.broadcasted_iota(jnp.int32, (1, LANES), 1)
    dtau_row = jnp.zeros((1, LANES), F32)
    for h in range(n_head):
        part = jnp.sum((rq_c * t_row)[h * hd:(h + 1) * hd], axis=0, keepdims=True)
        dtau_row += jnp.where(lane == h, part, 0.0)
    gb_src[6:7] = jnp.where(seq_i == 0, dtau_row, 0.0)
    gb_src[7:8] = jnp.zeros((1, LANES), F32)

    def back(i, part):
        lo, hi, a_t, b_t, c = ((dg_lo, dg_hi, k_t, q_t, cq_c), (dgt_lo, dgt_hi, q_t, k_t, ck_c))[part]
        base = part * dim
        for n in range(n_sub):
            a_n = a_t[i, :, sub(n)]
            d = jnp.concatenate([_dot(lo[:r_lo], a_n[:WIN]), _dot(hi[off_hi:], a_n[hi0:])], axis=0)
            dqkv_t[i, base:base + dim, sub(n)] = (d + _twice(c[...]) * b_t[i, :, sub(n)].astype(F32)).astype(BF)
        add_cols((acc_q, acc_k)[part], _dot_nt(u_t[i], dqkv_t[i, base:base + dim, :]), i == 0)

    e_step1()
    for i in range(n_blk):
        back(i, 0)
    pair_copy(1, acc_q, d2d_q).start()
    e_step2()
    for i in range(n_blk):
        back(i, 1)
        if i == min(1, n_blk - 1):
            rs_start(0, acc_q, d2d_q, rs_q)
    pair_copy(2, acc_k, d2d_k).start()

    def body_du(i, _):
        for n in range(n_sub):
            du = _dot(w_v[...], dqkv_t[i, :, sub(n)]).astype(BF)
            do_t[i, :, sub(n)] = du
            for c in range(SUB // LANES):
                cols = slice(n * SUB + c * LANES, n * SUB + (c + 1) * LANES)
                du_c = du[:, c * LANES:(c + 1) * LANES].astype(F32)
                rstd = rstd_v[i, :, cols]
                xh = (x_t[i, :, cols].astype(F32) - mean_v[i, :, cols]) * rstd
                p = du_c * xh
                dgam_acc[...] += p
                dbet_acc[...] += du_c
                c1 = jnp.sum(du_c * gam_c[...], axis=0, keepdims=True) * inv_d
                c2 = jnp.sum(p * gam_c[...], axis=0, keepdims=True) * inv_d
                k1_v[i, :, cols] = rstd * c1
                k2_v[i, :, cols] = rstd * rstd * c2

        @pl.when(i == 0)
        def _():
            rs_start(1, acc_k, d2d_k, rs_k)

        @pl.when(i == min(1, n_blk - 1))
        def _():
            e_step3()
        return 0

    lax.fori_loop(0, n_blk, body_du, 0)

    for b, acc in ((0, dgam_acc), (dim // LANES, dbet_acc)):
        row = jnp.sum(jnp.transpose(acc[...]), axis=0, keepdims=True)
        for c in range(dim // LANES):
            gb_src[b + c:b + c + 1] = row[:, c * LANES:(c + 1) * LANES]
    gb_pair = rcopy(gb_src, gb_rc, gb_ss.at[0], gb_rs.at[0], partner)
    gb_pair.start()

    def gb_copy(n):
        pc, pi = peer(*offsets[n])
        return rcopy(gb_all.at[chip, img_i], gb_all.at[chip, img_i], gb_ss.at[1 + n], gb_rs.at[1 + n],
                     dev(pc, core, pi))


    def body_x(i, _):
        for n in range(n_sub):
            proj = _dot(wo_t[...], o_t[i, :, sub(n)])
            x_v[i, sub(n), :] = jnp.transpose((x_t[i, :, sub(n)].astype(F32) + proj).astype(BF))
            for c in range(SUB // LANES):
                cols = slice(n * SUB + c * LANES, n * SUB + (c + 1) * LANES)
                g = do_t[i, :, cols].astype(F32) * gam_c[...] * rstd_v[i, :, cols]
                cen = x_t[i, :, cols].astype(F32) - mean_v[i, :, cols]
                gx = gy_t[i, :, cols].astype(F32) + (g - k1_v[i, :, cols] - cen * k2_v[i, :, cols])
                gy_v[i, cols, :] = jnp.transpose(gx.astype(BF))

        @pl.when(i == 0)
        def _():
            gb_pair.wait()
            gb_all[chip, img_i] = gb_src[...] + gb_rc[...]
            for n in range(len(offsets)):
                gb_copy(n).start()
            rs_finish(0, acc_q, rs_q, ag_q)

        @pl.when(i == min(1, n_blk - 1))
        def _():
            e_step4()
        return 0

    lax.fori_loop(0, n_blk, body_x, 0)
    rs_finish(1, acc_k, rs_k, ag_k)
    for n in range(len(offsets)):
        gb_copy(n).wait()
    tot = jnp.zeros(gb_src.shape, F32)
    for j in range(n_chip):
        for m in range(n_img):
            tot += gb_all[j, m]
    n_row = dim // LANES
    for b, ref in ((0, dgam_ref), (n_row, dbet_ref)):
        ref[...] = jnp.concatenate([tot[b + c:b + c + 1] for c in range(n_row)], axis=1).reshape(dim)
    dtau_ref[...] = tot[6:7, :n_head].reshape(n_head)
    rs_end(0, acc_q, rs_q, ag_q, dwqkv_ref, 0)
    for di in range(1, n_img):
        age_copy(di).wait()
    rc = ag_e.shape[1]
    for a in range(hn):
        for g, (ref, col) in enumerate(((dwout_ref, 0), (dwqkv_ref, 2 * dim))):
            ref[a * rc:(a + 1) * rc, col:col + dim] = ag_e[2 * a + g]
    rs_end(1, acc_k, rs_k, ag_k, dwqkv_ref, dim)


def _write(n_blk, blk, *refs):
    srcs, dsts, act_sem, sem = refs[:7], refs[7:14], refs[14], refs[15]
    copies = []
    for a in range(2):
        for i in range(n_blk):
            copies.append(pltpu.make_async_copy(srcs[a].at[i], dsts[a].at[0, pl.ds(i * blk, blk), :],
                                                act_sem.at[a, i]))
    for n in range(5):
        copies.append(pltpu.make_async_copy(srcs[2 + n], dsts[2 + n], sem.at[n]))
    for c in copies:
        c.start()
    for c in copies:
        c.wait()


def solution(mesh):
    act_spec = P(('data', 'img'), 'seq', None)
    row_spec = P(('data', 'seq'), None)
    in_specs = (act_spec, act_spec, P(), P(), P(), P(), P())
    out_specs = (act_spec, act_spec, row_spec, row_spec, P('data'), P('data'), P('data'))
    n_img = mesh.shape['img']
    n_seq = mesh.shape['seq']
    n_chip = n_seq // 2

    def local_block(x_in, grad_y, ln_gamma, ln_beta, w_qkv, w_out, head_temp):
        _, n_tok, dim = x_in.shape
        n_head = head_temp.shape[0]
        hd = dim // n_head
        blk = min(1024, n_tok)
        n_blk = n_tok // blk
        rb = dim // n_seq
        rc = rb // (n_img // 2)
        h1 = (hd + 16) // 2
        hbm = pl.BlockSpec(memory_space=pltpu.HBM)
        vmem = pl.BlockSpec(memory_space=pltpu.VMEM)
        smem = pl.BlockSpec(memory_space=pltpu.SMEM)
        V = pltpu.VMEM
        n_off = n_chip * n_img - 1
        n_hi = n_head - WIN // hd
        r_hi = n_hi * hd
        r_lo = dim - r_hi
        feat = V((n_blk, dim, blk), BF)
        stat = V((n_blk, 1, blk), F32)
        col = V((dim, LANES), F32)
        sqr = V((WIN, WIN), BF)
        acc = V((2, n_chip, n_img, rc, dim), F32)
        n_ct = dim // LANES
        n_sl = -(-n_ct // n_img)
        accc = V((2, n_chip, n_ct, rb, LANES), F32)
        dma = pltpu.SemaphoreType.DMA
        scratch = [
            feat, feat, feat, feat, feat, feat, feat, feat, V((n_blk, 3 * dim, blk), BF),
            stat, stat, stat, stat, V((dim, 3 * dim), BF), V((3 * dim, dim), BF), V((dim, dim), BF), V((dim, dim), BF),
            V((dim,), F32), V((dim,), F32), col, col,
            V((r_lo, WIN), F32), V((r_hi, WIN), F32), V((r_lo, WIN), F32), V((r_hi, WIN), F32),
            col, col, col, col,
            V((dim, WIN), F32), V((dim, WIN), F32), V((dim, WIN), F32),
            sqr, sqr, sqr, sqr, sqr, sqr, sqr, sqr,
            col, col, V((8, dim), F32), V((3, dim, LANES), F32),
            V((2, h1, dim), F32), V((h1, dim), F32), V((n_chip, h1, dim), F32), V((2, h1, dim), F32),
            V((2, hd // 2, dim), F32), V((hd // 2, dim), F32), V((n_chip, hd // 2, dim), F32),
            V((2, hd // 2, dim), F32),
            acc, accc, accc, V((n_chip, n_img, rc, dim), F32), V((n_chip, n_ct, rb, LANES), F32),
            V((n_chip, n_ct, rb, LANES), F32), V((2, n_img // 2, rc, dim), F32), V((2, n_img, rc, dim), F32),
            V((n_img - 1, rc, dim), F32), V((n_img, rc, dim), F32), V((n_sl, n_chip, n_img, rb, LANES), F32),
            V((n_sl, n_chip, n_img, rb, LANES), F32), V((n_ct, rb, LANES), F32), V((n_ct, rb, LANES), F32),
            V((8, LANES), F32), V((8, LANES), F32), V((n_chip, n_img, 8, LANES), F32),
            dma((n_blk,)), dma((n_blk,)), dma((4,)),
            dma((n_chip + 1,)), dma((n_chip + 1,)), dma((n_chip + 1,)), dma((n_chip + 1,)),
            dma((3,)), dma((3,)), dma((4,)), dma((4,)), dma((n_img - 1,)), dma((n_img - 1,)),
            dma((n_img - 1,)), dma((n_img - 1,)),
            dma((2, n_ct, n_chip)), dma((2, n_sl, n_chip, n_img)), dma((2, n_ct, n_img - 1)), dma((2, n_ct)),
            dma((1 + n_off,)), dma((1 + n_off,)),
        ]
        out_shape = (
            V((n_blk, blk, dim), BF), V((n_blk, blk, dim), BF), V((rb, 3 * dim), F32), V((rb, dim), F32),
            V((dim,), F32), V((dim,), F32), V((n_head,), F32),
        )
        cfg = (n_chip, n_img, n_blk, blk, dim, n_head)
        outs = pl.pallas_call(
            functools.partial(_kernel, cfg),
            out_shape=out_shape,
            in_specs=[hbm, hbm, hbm, hbm, hbm, hbm, smem],
            out_specs=(vmem,) * 7,
            scratch_shapes=scratch,
            compiler_params=pltpu.CompilerParams(collective_id=0, has_side_effects=True,
                                                 vmem_limit_bytes=VMEM_MAIN),
        )(x_in, grad_y, ln_gamma, ln_beta, w_qkv, w_out, head_temp)
        finals = (
            jax.ShapeDtypeStruct(x_in.shape, BF), jax.ShapeDtypeStruct(x_in.shape, BF),
            jax.ShapeDtypeStruct((rb, 3 * dim), F32), jax.ShapeDtypeStruct((rb, dim), F32),
            jax.ShapeDtypeStruct((dim,), F32), jax.ShapeDtypeStruct((dim,), F32),
            jax.ShapeDtypeStruct((n_head,), F32),
        )
        return pl.pallas_call(
            functools.partial(_write, n_blk, blk),
            out_shape=finals,
            in_specs=[vmem] * 7,
            out_specs=(hbm,) * 7,
            scratch_shapes=[dma((2, n_blk)), dma((5,))],
            compiler_params=pltpu.CompilerParams(vmem_limit_bytes=1 << 20),
        )(*outs)

    return jax.shard_map(local_block, mesh=mesh, in_specs=in_specs, out_specs=out_specs, check_vma=False)
```

```python
import functools

import jax
import jax.numpy as jnp
from jax import lax
from jax.experimental import pallas as pl
from jax.experimental.pallas import tpu as pltpu
from jax.sharding import PartitionSpec as P

LN_EPS = 1e-6
BF = jnp.bfloat16
F32 = jnp.float32
MESH = pl.DeviceIdType.MESH
WIN = 256
LANES = 128
SUB = 256
VMEM_MAIN = 56 * 1024 * 1024


def _dot(a, b):
    return lax.dot_general(a, b, (((1,), (0,)), ((), ())), preferred_element_type=F32)


def _dot_nt(a, b):
    return lax.dot_general(a, b, (((1,), (1,)), ((), ())), preferred_element_type=F32)


def _column(row):
    return jnp.transpose(jnp.broadcast_to(row, (LANES, row.shape[1])))


def _twice(x):
    return jnp.concatenate([x, x], axis=1)


def _kernel(cfg, x_hbm, gy_hbm, gam_hbm, bet_hbm, wqkv_hbm, wout_hbm, tau_ref,
            x_v, gy_v, dwqkv_ref, dwout_ref, dgam_ref, dbet_ref, dtau_ref,
            x_t, gy_t, u_t, q_t, k_t, v_t, do_t, o_t, dqkv_t,
            mean_v, rstd_v, k1_v, k2_v, w_v, w_t, wo_v, wo_t, gam_v, bet_v, gam_c, bet_c,
            g_lo, g_hi, da_lo, da_hi, sq_acc, sk_acc, dgam_acc, dbet_acc,
            a_f32, scale_f32, g_f32, a_lo, a_hi, at_lo, at_hi, dg_lo, dg_hi, dgt_lo, dgt_hi,
            cq_c, ck_c, srow, rqcol,
            ex1_src, ex1_rc, ex1_x, ex1_fin, ex2_src, ex2_rc, ex2_x, ex2_fin,
            acc_e, acc_q, acc_k, d2d_e, d2d_q, d2d_k, ring1, ring2, yrs_e, ag_e, rs_q, rs_k, ag_q, ag_k,
            gb_src, gb_rc, gb_all,
            x_sem, gy_sem, w_sem,
            ex1_ss, ex1_rs, ex2_ss, ex2_rs,
            d2d_ss, d2d_rs, ring_ss, ring_rs, yrs_ss, yrs_rs, age_ss, age_rs,
            rs_ss, rs_rs, ag_ss, ag_rs, gb_ss, gb_rs):
    n_chip, n_img, n_blk, blk, dim, n_head = cfg
    hd = dim // n_head
    n_lo = WIN // hd
    r_lo = n_lo * hd
    hi0 = dim - WIN
    off_hi = r_lo - hi0
    r_hi = dim - r_lo
    n_sub = blk // SUB
    inv_d = 1.0 / dim
    data_i = lax.axis_index('data')
    img_i = lax.axis_index('img')
    seq_i = lax.axis_index('seq')
    core = lax.rem(seq_i, 2)
    chip = seq_i // 2

    def dev(chip_to, core_to, img_to):
        return (data_i, img_to, chip_to * 2 + core_to)

    partner = dev(chip, 1 - core, img_i)

    def rcopy(src, dst, ssem, rsem, to):
        return pltpu.make_async_remote_copy(src_ref=src, dst_ref=dst, send_sem=ssem, recv_sem=rsem,
                                            device_id=to, device_id_type=MESH)

    offsets = [(dc, di) for dc in range(n_chip) for di in range(n_img) if (dc, di) != (0, 0)]

    def peer(dc, di):
        return lax.rem(chip + dc, n_chip), lax.rem(img_i + di, n_img)

    def x_copy(i):
        return pltpu.make_async_copy(x_hbm.at[0, pl.ds(i * blk, blk), :], x_v.at[i], x_sem.at[i])

    def gy_copy(i):
        return pltpu.make_async_copy(gy_hbm.at[0, pl.ds(i * blk, blk), :], gy_v.at[i], gy_sem.at[i])

    small = [(gam_hbm, gam_v), (bet_hbm, bet_v), (wqkv_hbm, w_v), (wout_hbm, wo_v)]
    loads = [pltpu.make_async_copy(s, d, w_sem.at[n]) for n, (s, d) in enumerate(small)]
    loads[0].start()
    loads[1].start()
    x_copy(0).start()
    loads[2].start()
    loads[3].start()

    barrier = pltpu.get_barrier_semaphore()
    pl.semaphore_signal(barrier, inc=1, device_id=partner, device_id_type=MESH)
    for dc, di in offsets:
        pc, pi = peer(dc, di)
        pl.semaphore_signal(barrier, inc=1, device_id=dev(pc, core, pi), device_id_type=MESH)

    for i in range(1, n_blk):
        x_copy(i).start()

    zero = (dgam_acc, dbet_acc)
    for ref in zero:
        ref[...] = jnp.zeros_like(ref)

    def sub(n):
        return slice(n * SUB, (n + 1) * SUB)

    def norm(i, cols):
        rows = 48
        cuts = [slice(r, r + rows) for r in range(0, dim, rows)]

        def fold(v):
            t = v[0:8]
            for r in range(8, rows, 8):
                t += v[r:r + 8]
            return t

        s = jnp.zeros((8, LANES), F32)
        for cut in cuts:
            s += fold(x_t[i, cut, cols].astype(F32))
        mean = jnp.sum(s, axis=0, keepdims=True) * inv_d
        s = jnp.zeros((8, LANES), F32)
        for cut in cuts:
            cen = x_t[i, cut, cols].astype(F32) - mean
            s += fold(cen * cen)
        var = jnp.sum(s, axis=0, keepdims=True) * inv_d
        rstd = lax.rsqrt(var + LN_EPS)
        mean_v[i, :, cols] = mean
        rstd_v[i, :, cols] = rstd
        for cut in cuts:
            cen = x_t[i, cut, cols].astype(F32) - mean
            u_t[i, cut, cols] = (cen * rstd * gam_c[cut] + bet_c[cut]).astype(BF)

    def norm_sub(i, n):
        x_t[i, :, sub(n)] = jnp.transpose(x_v[i, sub(n), :])
        for c in range(SUB // LANES):
            norm(i, slice(n * SUB + c * LANES, n * SUB + (c + 1) * LANES))

    for ld in loads:
        ld.wait()
    x_copy(0).wait()
    gam_c[...] = _column(gam_v[...].reshape(1, dim))
    bet_c[...] = _column(bet_v[...].reshape(1, dim))
    for n in range(n_sub):
        norm_sub(0, n)
    for c in range(3):
        w_t[c * dim:(c + 1) * dim, :] = jnp.transpose(w_v[:, c * dim:(c + 1) * dim])
    wo_t[...] = jnp.transpose(wo_v[...])
    for i in range(1, n_blk):
        x_copy(i).wait()
    for i in range(n_blk):
        gy_copy(i).start()
    for i in range(n_blk):
        for n in range(n_sub):
            u_n = u_t[i, :, sub(n)]
            for part, ref in ((0, q_t), (1, k_t)):
                r = _dot(w_t[part * dim:(part + 1) * dim, :], u_n).astype(BF)
                ref[i, :, sub(n)] = r
                rf = r.astype(F32)
                rf = rf * rf
                acc = (sq_acc, sk_acc)[part]
                val = rf[:, :LANES] + rf[:, LANES:]
                if i == 0 and n == 0:
                    acc[...] = val
                else:
                    acc[...] += val
            if i + 1 < n_blk:
                norm_sub(i + 1, n)
        lo = _dot_nt(q_t[i, :r_lo, :], k_t[i, :WIN, :])
        hi = _dot_nt(q_t[i, r_lo:, :], k_t[i, hi0:, :])
        if i == 0:
            g_lo[...] = lo
            g_hi[...] = hi
        else:
            g_lo[...] += lo
            g_hi[...] += hi

    def pack(lo, hi, put):
        col = lax.broadcasted_iota(jnp.int32, (hd, WIN), 1)
        t_lo = jnp.zeros((hd, WIN), F32)
        for h in range(n_lo):
            t_lo += jnp.where((col >= h * hd) & (col < (h + 1) * hd), lo[h * hd:(h + 1) * hd, :], 0.0)
        t_hi = jnp.zeros((hd, WIN), F32)
        for h in range(n_lo, n_head):
            b = h * hd - hi0
            r = h * hd - r_lo
            t_hi += jnp.where((col >= b) & (col < b + hd), hi[r:r + hd, :], 0.0)
        put(jnp.concatenate([t_lo[:, :hi0], t_lo[:, hi0:] + t_hi[:, :WIN - hi0], t_hi[:, WIN - hi0:]], axis=1))

    def ex_pair(src, rc, ss, rs):
        return rcopy(src.at[1 - core], rc, ss.at[0], rs.at[0], partner)

    def ex_chip(buf, ss, rs, dc):
        return rcopy(buf.at[chip], buf.at[chip], ss.at[dc], rs.at[dc], dev(lax.rem(chip + dc, n_chip), core, img_i))

    def ex_swap(fin, ss, rs):
        return rcopy(fin.at[core], fin.at[core], ss.at[n_chip], rs.at[n_chip], partner)

    def ex_step2(src, rc, buf, ss, rs):
        ex_pair(src, rc, ss, rs).wait()
        buf[chip] = src[core] + rc[...]
        for dc in sorted(range(1, n_chip), key=lambda d: -min(d, n_chip - d)):
            ex_chip(buf, ss, rs, dc).start()

    def ex_step3(buf, fin, ss, rs):
        for dc in range(1, n_chip):
            ex_chip(buf, ss, rs, dc).wait()
        tot = buf[0]
        for j in range(1, n_chip):
            tot += buf[j]
        fin[core] = tot
        ex_swap(fin, ss, rs).start()

    def put_g(t):
        h1 = ex1_src.shape[1]
        sq = jnp.sum(jnp.transpose(sq_acc[...]), axis=0, keepdims=True)
        sk = jnp.sum(jnp.transpose(sk_acc[...]), axis=0, keepdims=True)
        ex1_src[0] = t[:h1]
        ex1_src[1, :hd - h1] = t[h1:]
        ex1_src[1, hd - h1:hd - h1 + 8] = jnp.broadcast_to(sq, (8, dim))
        ex1_src[1, hd - h1 + 8:] = jnp.broadcast_to(sk, (8, dim))

    def put_da(t):
        ex2_src[0] = t[:hd // 2]
        ex2_src[1] = t[hd // 2:]

    pack(g_lo, g_hi, put_g)
    pl.semaphore_wait(barrier, 1 + len(offsets))
    ex_pair(ex1_src, ex1_rc, ex1_ss, ex1_rs).start()

    for i in range(n_blk):
        gy_copy(i).wait()
    for i in range(n_blk):
        for n in range(n_sub):
            gy_t[i, :, sub(n)] = jnp.transpose(gy_v[i, sub(n), :])
            v_t[i, :, sub(n)] = _dot(w_t[2 * dim:, :], u_t[i, :, sub(n)]).astype(BF)
            do_t[i, :, sub(n)] = _dot(wo_v[...], gy_t[i, :, sub(n)]).astype(BF)
        lo = _dot_nt(do_t[i, :r_lo, :], v_t[i, :WIN, :])
        hi = _dot_nt(do_t[i, r_lo:, :], v_t[i, hi0:, :])
        if i == 0:
            da_lo[...] = lo
            da_hi[...] = hi
            ex_step2(ex1_src, ex1_rc, ex1_x, ex1_ss, ex1_rs)
        else:
            da_lo[...] += lo
            da_hi[...] += hi

    pack(da_lo, da_hi, put_da)
    ex_pair(ex2_src, ex2_rc, ex2_ss, ex2_rs).start()
    ex_step3(ex1_x, ex1_fin, ex1_ss, ex1_rs)
    ex_step2(ex2_src, ex2_rc, ex2_x, ex2_ss, ex2_rs)
    ex_swap(ex1_fin, ex1_ss, ex1_rs).wait()

    def head_mask(rows, row0, col0):
        r = lax.broadcasted_iota(jnp.int32, (rows, WIN), 0) + row0
        c = lax.broadcasted_iota(jnp.int32, (rows, WIN), 1) + col0
        out = (r < 0)
        for h in range(n_head):
            out |= (r >= h * hd) & (r < (h + 1) * hd) & (c >= h * hd) & (c < (h + 1) * hd)
        return out

    windows = ((0, r_lo, 0, n_lo), (r_lo, r_hi, hi0, n_head - n_lo))
    h1 = ex1_fin.shape[1]
    gcat = jnp.concatenate([ex1_fin[0], ex1_fin[1, :hd - h1]], axis=0)
    sq = ex1_fin[1, hd - h1:hd - h1 + 1]
    sk = ex1_fin[1, hd - h1 + 8:hd - h1 + 9]
    rk = lax.rsqrt(sk)
    srow[0:1] = sk
    srow[1:2] = rk
    sq_c = _column(sq)
    rq_c = lax.rsqrt(sq_c)
    rqcol[0] = sq_c
    rqcol[1] = rq_c
    tau_c = jnp.concatenate([jnp.full((hd, LANES), tau_ref[h], F32) for h in range(n_head)], axis=0)
    rqcol[2] = tau_c
    for w, (row0, rows, col0, heads) in enumerate(windows):
        g = jnp.concatenate([gcat[:, col0:col0 + WIN]] * heads, axis=0)
        mask = head_mask(rows, row0, col0)
        scale = _twice((tau_c * rq_c)[row0:row0 + rows]) * rk[:, col0:col0 + WIN]
        s = g * scale
        top = jnp.max(jnp.where(mask, s, -jnp.inf), axis=1, keepdims=True)
        e = jnp.where(mask, jnp.exp(jnp.where(mask, s - top, 0.0)), 0.0)
        a = e / jnp.sum(e, axis=1, keepdims=True)
        a_f32[row0:row0 + rows] = a
        scale_f32[row0:row0 + rows] = scale
        g_f32[row0:row0 + rows] = g
        if w == 0:
            full = jnp.concatenate([a, jnp.zeros((WIN - rows, WIN), F32)], axis=0)
            a_lo[...] = full.astype(BF)
            at_lo[...] = jnp.transpose(full).astype(BF)
        else:
            full = jnp.concatenate([jnp.zeros((WIN - rows, WIN), F32), a], axis=0)
            a_hi[...] = full.astype(BF)
            at_hi[...] = jnp.transpose(full).astype(BF)

    def add_rows(acc, g, val, first):
        rb = dim // (2 * n_chip)
        n_a = n_img // 2
        rc = rb // n_a
        for s in range(2 * n_chip):
            for a in range(n_a):
                part = val[s * rb + a * rc:s * rb + (a + 1) * rc]
                if first:
                    acc[s % 2, s // 2, 2 * a + g] = part
                else:
                    acc[s % 2, s // 2, 2 * a + g] += part

    n_ct = dim // LANES

    def add_cols(acc, val, first):
        rb = dim // (2 * n_chip)
        for s in range(2 * n_chip):
            for ct in range(n_ct):
                part = val[s * rb:(s + 1) * rb, ct * LANES:(ct + 1) * LANES]
                if first:
                    acc[s % 2, s // 2, ct] = part
                else:
                    acc[s % 2, s // 2, ct] += part

    for i in range(n_blk):
        for n in range(n_sub):
            o_t[i, :r_lo, sub(n)] = _dot(a_lo[:r_lo], v_t[i, :WIN, sub(n)]).astype(BF)
            o_t[i, r_lo:, sub(n)] = _dot(a_hi[off_hi:], v_t[i, hi0:, sub(n)]).astype(BF)
            dqkv_t[i, 2 * dim:2 * dim + r_lo, sub(n)] = _dot(at_lo[:r_lo], do_t[i, :WIN, sub(n)]).astype(BF)
            dqkv_t[i, 2 * dim + r_lo:, sub(n)] = _dot(at_hi[off_hi:], do_t[i, hi0:, sub(n)]).astype(BF)
        add_rows(acc_e, 0, _dot(o_t[i], gy_v[i]), i == 0)
        add_rows(acc_e, 1, _dot_nt(u_t[i], dqkv_t[i, 2 * dim:, :]), i == 0)
        if i == max(n_blk - 2, 0):
            ex_step3(ex2_x, ex2_fin, ex2_ss, ex2_rs)

    def pair_copy(r, acc, buf):
        return rcopy(acc.at[1 - core], buf, d2d_ss.at[r], d2d_rs.at[r], partner)

    hn = n_img // 2
    far_first = sorted(range(1, n_img), key=lambda d: -min(d, n_img - d))
    right = lax.rem(chip + 1, n_chip)
    left = lax.rem(chip + n_chip - 1, n_chip)
    opp = lax.rem(chip + 2, n_chip)

    def ring_copy(n):
        to = dev((right, left)[n % 2], core, img_i)
        if n == 0:
            src, dst = acc_e.at[core, opp, pl.ds(0, hn)], ring1.at[0]
        elif n == 1:
            src, dst = acc_e.at[core, opp, pl.ds(hn, hn)], ring1.at[1]
        else:
            src, dst = acc_e.at[core, (right, left)[n % 2]], ring2.at[n % 2]
        return rcopy(src, dst, ring_ss.at[n], ring_rs.at[n], to)

    def yrs_copy(di):
        pi = lax.rem(img_i + di, n_img)
        return rcopy(acc_e.at[core, chip, pi], yrs_e.at[di - 1], yrs_ss.at[di - 1], yrs_rs.at[di - 1],
                     dev(chip, core, pi))

    def age_copy(di):
        return rcopy(ag_e.at[img_i], ag_e.at[img_i], age_ss.at[di - 1], age_rs.at[di - 1],
                     dev(chip, core, lax.rem(img_i + di, n_img)))

    def e_step1():
        pair_copy(0, acc_e, d2d_e).wait()
        for j in range(n_chip):
            acc_e[core, j] += d2d_e[j]
        ring_copy(0).start()
        ring_copy(1).start()

    def e_step2():
        ring_copy(0).wait()
        ring_copy(1).wait()
        acc_e[core, right, :hn] += ring1[0]
        acc_e[core, left, hn:] += ring1[1]
        ring_copy(2).start()
        ring_copy(3).start()

    def e_step3():
        ring_copy(2).wait()
        ring_copy(3).wait()
        acc_e[core, chip] += ring2[0] + ring2[1]
        for di in far_first:
            yrs_copy(di).start()

    def e_step4():
        tot = acc_e[core, chip, img_i]
        for di in range(1, n_img):
            yrs_copy(di).wait()
            tot += yrs_e[di - 1]
        ag_e[img_i] = tot
        for di in far_first:
            age_copy(di).start()

    def owner(r, ct):
        return (2 * r + ct) % n_img

    def rs_copy(r, acc, buf, ct, dc):
        pc = lax.rem(chip + dc, n_chip)
        sl = ct // n_img
        return rcopy(acc.at[core, pc, ct], buf.at[sl, dc, img_i], rs_ss.at[r, ct, dc], rs_rs.at[r, sl, dc, img_i],
                     dev(pc, core, owner(r, ct)))

    def each_send(r, do):
        for dc in sorted(range(n_chip), key=lambda d: -min(d, n_chip - d)):
            for ct in range(n_ct):
                if dc:
                    do(ct, dc)
                else:
                    pl.when(img_i != owner(r, ct))(functools.partial(do, ct, dc))

    def rs_start(r, acc, d2d, buf):
        pair_copy(1 + r, acc, d2d).wait()
        for j in range(n_chip):
            acc[core, j] += d2d[j]
        each_send(r, lambda ct, dc: rs_copy(r, acc, buf, ct, dc).start())

    def ag_copy(r, gbuf, ct, di):
        return rcopy(gbuf.at[ct], gbuf.at[ct], ag_ss.at[r, ct, di - 1], ag_rs.at[r, ct],
                     dev(chip, core, lax.rem(img_i + di, n_img)))

    def rs_finish(r, acc, buf, gbuf):
        for ct in range(n_ct):
            @pl.when(img_i == owner(r, ct))
            def _(ct=ct):
                sl = ct // n_img
                tot = acc[core, chip, ct]
                for dc in range(n_chip):
                    for im in range(n_img):
                        if dc == 0 and im == owner(r, ct):
                            continue
                        rcopy(buf.at[sl, dc, im], buf.at[sl, dc, im], rs_ss.at[r, ct, dc], rs_rs.at[r, sl, dc, im],
                              partner).wait_recv()
                        tot += buf[sl, dc, im]
                gbuf[ct] = tot
                for di in far_first:
                    ag_copy(r, gbuf, ct, di).start()

    def rs_end(r, acc, buf, gbuf, ref, col):
        each_send(r, lambda ct, dc: rs_copy(r, acc, buf, ct, dc).wait_send())
        for ct in range(n_ct):
            @pl.when(img_i == owner(r, ct))
            def _(ct=ct):
                for di in range(1, n_img):
                    ag_copy(r, gbuf, ct, di).wait_send()

            @pl.when(img_i != owner(r, ct))
            def _(ct=ct):
                ag_copy(r, gbuf, ct, 1).wait_recv()
            ref[:, col + ct * LANES:col + (ct + 1) * LANES] = gbuf[ct]

    pair_copy(0, acc_e, d2d_e).start()
    ex_swap(ex2_fin, ex2_ss, ex2_rs).wait()

    dacat = jnp.concatenate([ex2_fin[0], ex2_fin[1]], axis=0)
    sq_c = rqcol[0]
    rq_c = rqcol[1]
    tau_c = rqcol[2]
    sk = srow[0:1]
    rk = srow[1:2]
    row_sums = []
    col_sums = []
    for w, (row0, rows, col0, heads) in enumerate(windows):
        da = jnp.concatenate([dacat[:, col0:col0 + WIN]] * heads, axis=0)
        a = a_f32[row0:row0 + rows]
        ds = a * (da - jnp.sum(a * da, axis=1, keepdims=True))
        dg = ds * scale_f32[row0:row0 + rows]
        dscale = ds * g_f32[row0:row0 + rows]
        row_sums.append(jnp.broadcast_to(jnp.sum(dscale * rk[:, col0:col0 + WIN], axis=1, keepdims=True),
                                         (rows, LANES)))
        col_sums.append(jnp.sum(dscale * _twice((tau_c * rq_c)[row0:row0 + rows]), axis=0, keepdims=True))
        if w == 0:
            full = jnp.concatenate([dg, jnp.zeros((WIN - rows, WIN), F32)], axis=0)
            dg_lo[...] = full.astype(BF)
            dgt_lo[...] = jnp.transpose(full).astype(BF)
        else:
            full = jnp.concatenate([jnp.zeros((WIN - rows, WIN), F32), dg], axis=0)
            dg_hi[...] = full.astype(BF)
            dgt_hi[...] = jnp.transpose(full).astype(BF)
    t_row = jnp.concatenate(row_sums, axis=0)
    cl, ch = col_sums
    w_col = jnp.concatenate([cl[:, :hi0], cl[:, hi0:] + ch[:, :WIN - hi0], ch[:, WIN - hi0:]], axis=1)
    cq_c[...] = 2.0 * (-0.5 * rq_c / sq_c * (tau_c * t_row))
    ck_c[...] = _column(2.0 * (-0.5 * rk / sk * w_col))
    lane = lax.broadcasted_iota(jnp.int32, (1, LANES), 1)
    dtau_row = jnp.zeros((1, LANES), F32)
    for h in range(n_head):
        part = jnp.sum((rq_c * t_row)[h * hd:(h + 1) * hd], axis=0, keepdims=True)
        dtau_row += jnp.where(lane == h, part, 0.0)
    gb_src[6:7] = jnp.where(seq_i == 0, dtau_row, 0.0)
    gb_src[7:8] = jnp.zeros((1, LANES), F32)

    def back(i, part):
        lo, hi, a_t, b_t, c = ((dg_lo, dg_hi, k_t, q_t, cq_c), (dgt_lo, dgt_hi, q_t, k_t, ck_c))[part]
        base = part * dim
        for n in range(n_sub):
            a_n = a_t[i, :, sub(n)]
            d = jnp.concatenate([_dot(lo[:r_lo], a_n[:WIN]), _dot(hi[off_hi:], a_n[hi0:])], axis=0)
            dqkv_t[i, base:base + dim, sub(n)] = (d + _twice(c[...]) * b_t[i, :, sub(n)].astype(F32)).astype(BF)
        add_cols((acc_q, acc_k)[part], _dot_nt(u_t[i], dqkv_t[i, base:base + dim, :]), i == 0)

    e_step1()
    for i in range(n_blk):
        back(i, 0)
        if i == max(n_blk - 2, 0):
            e_step2()
    pair_copy(1, acc_q, d2d_q).start()
    for i in range(n_blk):
        back(i, 1)
        if i == 0:
            rs_start(0, acc_q, d2d_q, rs_q)
    pair_copy(2, acc_k, d2d_k).start()

    def body_du(i, _):
        for n in range(n_sub):
            du = _dot(w_v[...], dqkv_t[i, :, sub(n)]).astype(BF)
            do_t[i, :, sub(n)] = du
            for c in range(SUB // LANES):
                cols = slice(n * SUB + c * LANES, n * SUB + (c + 1) * LANES)
                du_c = du[:, c * LANES:(c + 1) * LANES].astype(F32)
                rstd = rstd_v[i, :, cols]
                xh = (x_t[i, :, cols].astype(F32) - mean_v[i, :, cols]) * rstd
                p = du_c * xh
                dgam_acc[...] += p
                dbet_acc[...] += du_c
                c1 = jnp.sum(du_c * gam_c[...], axis=0, keepdims=True) * inv_d
                c2 = jnp.sum(p * gam_c[...], axis=0, keepdims=True) * inv_d
                k1_v[i, :, cols] = rstd * c1
                k2_v[i, :, cols] = rstd * rstd * c2

        @pl.when(i == 0)
        def _():
            rs_start(1, acc_k, d2d_k, rs_k)

        @pl.when(i == min(1, n_blk - 1))
        def _():
            e_step3()
        return 0

    lax.fori_loop(0, n_blk, body_du, 0)

    for b, acc in ((0, dgam_acc), (dim // LANES, dbet_acc)):
        row = jnp.sum(jnp.transpose(acc[...]), axis=0, keepdims=True)
        for c in range(dim // LANES):
            gb_src[b + c:b + c + 1] = row[:, c * LANES:(c + 1) * LANES]
    gb_pair = rcopy(gb_src, gb_rc, gb_ss.at[0], gb_rs.at[0], partner)
    gb_pair.start()

    def gb_copy(n):
        pc, pi = peer(*offsets[n])
        return rcopy(gb_all.at[chip, img_i], gb_all.at[chip, img_i], gb_ss.at[1 + n], gb_rs.at[1 + n],
                     dev(pc, core, pi))


    def body_x(i, _):
        for n in range(n_sub):
            proj = _dot(wo_t[...], o_t[i, :, sub(n)])
            x_v[i, sub(n), :] = jnp.transpose((x_t[i, :, sub(n)].astype(F32) + proj).astype(BF))
            for c in range(SUB // LANES):
                cols = slice(n * SUB + c * LANES, n * SUB + (c + 1) * LANES)
                g = do_t[i, :, cols].astype(F32) * gam_c[...] * rstd_v[i, :, cols]
                cen = x_t[i, :, cols].astype(F32) - mean_v[i, :, cols]
                gx = gy_t[i, :, cols].astype(F32) + (g - k1_v[i, :, cols] - cen * k2_v[i, :, cols])
                gy_v[i, cols, :] = jnp.transpose(gx.astype(BF))

        @pl.when(i == 0)
        def _():
            gb_pair.wait()
            gb_all[chip, img_i] = gb_src[...] + gb_rc[...]
            for n in range(len(offsets)):
                gb_copy(n).start()
            rs_finish(0, acc_q, rs_q, ag_q)

        @pl.when(i == min(1, n_blk - 1))
        def _():
            e_step4()

        @pl.when(i == max(n_blk - 2, 0))
        def _():
            rs_finish(1, acc_k, rs_k, ag_k)
        return 0

    lax.fori_loop(0, n_blk, body_x, 0)
    for n in range(len(offsets)):
        gb_copy(n).wait()
    tot = jnp.zeros(gb_src.shape, F32)
    for j in range(n_chip):
        for m in range(n_img):
            tot += gb_all[j, m]
    n_row = dim // LANES
    for b, ref in ((0, dgam_ref), (n_row, dbet_ref)):
        ref[...] = jnp.concatenate([tot[b + c:b + c + 1] for c in range(n_row)], axis=1).reshape(dim)
    dtau_ref[...] = tot[6:7, :n_head].reshape(n_head)
    rs_end(0, acc_q, rs_q, ag_q, dwqkv_ref, 0)
    for di in range(1, n_img):
        age_copy(di).wait()
    rc = ag_e.shape[1]
    for a in range(hn):
        for g, (ref, col) in enumerate(((dwout_ref, 0), (dwqkv_ref, 2 * dim))):
            ref[a * rc:(a + 1) * rc, col:col + dim] = ag_e[2 * a + g]
    rs_end(1, acc_k, rs_k, ag_k, dwqkv_ref, dim)


def _write(n_blk, blk, *refs):
    srcs, dsts, act_sem, sem = refs[:7], refs[7:14], refs[14], refs[15]
    copies = []
    for a in range(2):
        for i in range(n_blk):
            copies.append(pltpu.make_async_copy(srcs[a].at[i], dsts[a].at[0, pl.ds(i * blk, blk), :],
                                                act_sem.at[a, i]))
    for n in range(5):
        copies.append(pltpu.make_async_copy(srcs[2 + n], dsts[2 + n], sem.at[n]))
    for c in copies:
        c.start()
    for c in copies:
        c.wait()


def solution(mesh):
    act_spec = P(('data', 'img'), 'seq', None)
    row_spec = P(('data', 'seq'), None)
    in_specs = (act_spec, act_spec, P(), P(), P(), P(), P())
    out_specs = (act_spec, act_spec, row_spec, row_spec, P('data'), P('data'), P('data'))
    n_img = mesh.shape['img']
    n_seq = mesh.shape['seq']
    n_chip = n_seq // 2

    def local_block(x_in, grad_y, ln_gamma, ln_beta, w_qkv, w_out, head_temp):
        _, n_tok, dim = x_in.shape
        n_head = head_temp.shape[0]
        hd = dim // n_head
        blk = min(1024, n_tok)
        n_blk = n_tok // blk
        rb = dim // n_seq
        rc = rb // (n_img // 2)
        h1 = (hd + 16) // 2
        hbm = pl.BlockSpec(memory_space=pltpu.HBM)
        vmem = pl.BlockSpec(memory_space=pltpu.VMEM)
        smem = pl.BlockSpec(memory_space=pltpu.SMEM)
        V = pltpu.VMEM
        n_off = n_chip * n_img - 1
        n_hi = n_head - WIN // hd
        r_hi = n_hi * hd
        r_lo = dim - r_hi
        feat = V((n_blk, dim, blk), BF)
        stat = V((n_blk, 1, blk), F32)
        col = V((dim, LANES), F32)
        sqr = V((WIN, WIN), BF)
        acc = V((2, n_chip, n_img, rc, dim), F32)
        n_ct = dim // LANES
        n_sl = -(-n_ct // n_img)
        accc = V((2, n_chip, n_ct, rb, LANES), F32)
        dma = pltpu.SemaphoreType.DMA
        scratch = [
            feat, feat, feat, feat, feat, feat, feat, feat, V((n_blk, 3 * dim, blk), BF),
            stat, stat, stat, stat, V((dim, 3 * dim), BF), V((3 * dim, dim), BF), V((dim, dim), BF), V((dim, dim), BF),
            V((dim,), F32), V((dim,), F32), col, col,
            V((r_lo, WIN), F32), V((r_hi, WIN), F32), V((r_lo, WIN), F32), V((r_hi, WIN), F32),
            col, col, col, col,
            V((dim, WIN), F32), V((dim, WIN), F32), V((dim, WIN), F32),
            sqr, sqr, sqr, sqr, sqr, sqr, sqr, sqr,
            col, col, V((8, dim), F32), V((3, dim, LANES), F32),
            V((2, h1, dim), F32), V((h1, dim), F32), V((n_chip, h1, dim), F32), V((2, h1, dim), F32),
            V((2, hd // 2, dim), F32), V((hd // 2, dim), F32), V((n_chip, hd // 2, dim), F32),
            V((2, hd // 2, dim), F32),
            acc, accc, accc, V((n_chip, n_img, rc, dim), F32), V((n_chip, n_ct, rb, LANES), F32),
            V((n_chip, n_ct, rb, LANES), F32), V((2, n_img // 2, rc, dim), F32), V((2, n_img, rc, dim), F32),
            V((n_img - 1, rc, dim), F32), V((n_img, rc, dim), F32), V((n_sl, n_chip, n_img, rb, LANES), F32),
            V((n_sl, n_chip, n_img, rb, LANES), F32), V((n_ct, rb, LANES), F32), V((n_ct, rb, LANES), F32),
            V((8, LANES), F32), V((8, LANES), F32), V((n_chip, n_img, 8, LANES), F32),
            dma((n_blk,)), dma((n_blk,)), dma((4,)),
            dma((n_chip + 1,)), dma((n_chip + 1,)), dma((n_chip + 1,)), dma((n_chip + 1,)),
            dma((3,)), dma((3,)), dma((4,)), dma((4,)), dma((n_img - 1,)), dma((n_img - 1,)),
            dma((n_img - 1,)), dma((n_img - 1,)),
            dma((2, n_ct, n_chip)), dma((2, n_sl, n_chip, n_img)), dma((2, n_ct, n_img - 1)), dma((2, n_ct)),
            dma((1 + n_off,)), dma((1 + n_off,)),
        ]
        out_shape = (
            V((n_blk, blk, dim), BF), V((n_blk, blk, dim), BF), V((rb, 3 * dim), F32), V((rb, dim), F32),
            V((dim,), F32), V((dim,), F32), V((n_head,), F32),
        )
        cfg = (n_chip, n_img, n_blk, blk, dim, n_head)
        outs = pl.pallas_call(
            functools.partial(_kernel, cfg),
            out_shape=out_shape,
            in_specs=[hbm, hbm, hbm, hbm, hbm, hbm, smem],
            out_specs=(vmem,) * 7,
            scratch_shapes=scratch,
            compiler_params=pltpu.CompilerParams(collective_id=0, has_side_effects=True,
                                                 vmem_limit_bytes=VMEM_MAIN),
        )(x_in, grad_y, ln_gamma, ln_beta, w_qkv, w_out, head_temp)
        finals = (
            jax.ShapeDtypeStruct(x_in.shape, BF), jax.ShapeDtypeStruct(x_in.shape, BF),
            jax.ShapeDtypeStruct((rb, 3 * dim), F32), jax.ShapeDtypeStruct((rb, dim), F32),
            jax.ShapeDtypeStruct((dim,), F32), jax.ShapeDtypeStruct((dim,), F32),
            jax.ShapeDtypeStruct((n_head,), F32),
        )
        return pl.pallas_call(
            functools.partial(_write, n_blk, blk),
            out_shape=finals,
            in_specs=[vmem] * 7,
            out_specs=(hbm,) * 7,
            scratch_shapes=[dma((2, n_blk)), dma((5,))],
            compiler_params=pltpu.CompilerParams(vmem_limit_bytes=1 << 20),
        )(*outs)

    return jax.shard_map(local_block, mesh=mesh, in_specs=in_specs, out_specs=out_specs, check_vma=False)
```

```python
import functools

import jax
import jax.numpy as jnp
from jax import lax
from jax.experimental import pallas as pl
from jax.experimental.pallas import tpu as pltpu
from jax.sharding import PartitionSpec as P

LN_EPS = 1e-6
BF = jnp.bfloat16
F32 = jnp.float32
MESH = pl.DeviceIdType.MESH
WIN = 256
LANES = 128
SUB = 256
VMEM_MAIN = 56 * 1024 * 1024


def _dot(a, b):
    return lax.dot_general(a, b, (((1,), (0,)), ((), ())), preferred_element_type=F32)


def _dot_nt(a, b):
    return lax.dot_general(a, b, (((1,), (1,)), ((), ())), preferred_element_type=F32)


def _column(row):
    return jnp.transpose(jnp.broadcast_to(row, (LANES, row.shape[1])))


def _twice(x):
    return jnp.concatenate([x, x], axis=1)


def _kernel(cfg, x_hbm, gy_hbm, gam_hbm, bet_hbm, wqkv_hbm, wout_hbm, tau_ref,
            x_v, gy_v, dwqkv_ref, dwout_ref, dgam_ref, dbet_ref, dtau_ref,
            x_t, gy_t, u_t, q_t, k_t, v_t, do_t, o_t, dqkv_t,
            mean_v, rstd_v, k1_v, k2_v, w_v, w_t, wo_v, wo_t, gam_v, bet_v, gam_c, bet_c,
            g_lo, g_hi, da_lo, da_hi, sq_acc, sk_acc, dgam_acc, dbet_acc,
            a_f32, scale_f32, g_f32, a_lo, a_hi, at_lo, at_hi, dg_lo, dg_hi, dgt_lo, dgt_hi,
            cq_c, ck_c, srow, rqcol,
            ex1_src, ex1_rc, ex1_x, ex1_fin, ex2_src, ex2_rc, ex2_x, ex2_fin,
            acc_e, acc_q, acc_k, d2d_e, d2d_q, d2d_k, ring1, ring2, yrs_e, ag_e, rs_q, rs_k, ag_q, ag_k,
            gb_src, gb_rc, gb_all,
            x_sem, gy_sem, w_sem,
            ex1_ss, ex1_rs, ex2_ss, ex2_rs,
            d2d_ss, d2d_rs, ring_ss, ring_rs, yrs_ss, yrs_rs, age_ss, age_rs,
            rs_ss, rs_rs, ag_ss, ag_rs, gb_ss, gb_rs):
    n_chip, n_img, n_blk, blk, dim, n_head = cfg
    hd = dim // n_head
    n_lo = WIN // hd
    r_lo = n_lo * hd
    hi0 = dim - WIN
    off_hi = r_lo - hi0
    r_hi = dim - r_lo
    n_sub = blk // SUB
    inv_d = 1.0 / dim
    data_i = lax.axis_index('data')
    img_i = lax.axis_index('img')
    seq_i = lax.axis_index('seq')
    core = lax.rem(seq_i, 2)
    chip = seq_i // 2

    def dev(chip_to, core_to, img_to):
        return (data_i, img_to, chip_to * 2 + core_to)

    partner = dev(chip, 1 - core, img_i)

    def rcopy(src, dst, ssem, rsem, to):
        return pltpu.make_async_remote_copy(src_ref=src, dst_ref=dst, send_sem=ssem, recv_sem=rsem,
                                            device_id=to, device_id_type=MESH)

    offsets = [(dc, di) for dc in range(n_chip) for di in range(n_img) if (dc, di) != (0, 0)]

    def peer(dc, di):
        return lax.rem(chip + dc, n_chip), lax.rem(img_i + di, n_img)

    def x_copy(i):
        return pltpu.make_async_copy(x_hbm.at[0, pl.ds(i * blk, blk), :], x_v.at[i], x_sem.at[i])

    def gy_copy(i):
        return pltpu.make_async_copy(gy_hbm.at[0, pl.ds(i * blk, blk), :], gy_v.at[i], gy_sem.at[i])

    small = [(gam_hbm, gam_v), (bet_hbm, bet_v), (wqkv_hbm, w_v), (wout_hbm, wo_v)]
    loads = [pltpu.make_async_copy(s, d, w_sem.at[n]) for n, (s, d) in enumerate(small)]
    loads[0].start()
    loads[1].start()
    x_copy(0).start()
    loads[2].start()
    loads[3].start()

    barrier = pltpu.get_barrier_semaphore()
    pl.semaphore_signal(barrier, inc=1, device_id=partner, device_id_type=MESH)
    for dc, di in offsets:
        pc, pi = peer(dc, di)
        pl.semaphore_signal(barrier, inc=1, device_id=dev(pc, core, pi), device_id_type=MESH)

    for i in range(1, n_blk):
        x_copy(i).start()

    zero = (dgam_acc, dbet_acc)
    for ref in zero:
        ref[...] = jnp.zeros_like(ref)

    def sub(n):
        return slice(n * SUB, (n + 1) * SUB)

    def norm(i, cols):
        rows = 48
        cuts = [slice(r, r + rows) for r in range(0, dim, rows)]

        def fold(v):
            t = v[0:8]
            for r in range(8, rows, 8):
                t += v[r:r + 8]
            return t

        s = jnp.zeros((8, LANES), F32)
        for cut in cuts:
            s += fold(x_t[i, cut, cols].astype(F32))
        mean = jnp.sum(s, axis=0, keepdims=True) * inv_d
        s = jnp.zeros((8, LANES), F32)
        for cut in cuts:
            cen = x_t[i, cut, cols].astype(F32) - mean
            s += fold(cen * cen)
        var = jnp.sum(s, axis=0, keepdims=True) * inv_d
        rstd = lax.rsqrt(var + LN_EPS)
        mean_v[i, :, cols] = mean
        rstd_v[i, :, cols] = rstd
        for cut in cuts:
            cen = x_t[i, cut, cols].astype(F32) - mean
            u_t[i, cut, cols] = (cen * rstd * gam_c[cut] + bet_c[cut]).astype(BF)

    def norm_sub(i, n):
        x_t[i, :, sub(n)] = jnp.transpose(x_v[i, sub(n), :])
        for c in range(SUB // LANES):
            norm(i, slice(n * SUB + c * LANES, n * SUB + (c + 1) * LANES))

    for ld in loads:
        ld.wait()
    x_copy(0).wait()
    gam_c[...] = _column(gam_v[...].reshape(1, dim))
    bet_c[...] = _column(bet_v[...].reshape(1, dim))
    for n in range(n_sub):
        norm_sub(0, n)
    for c in range(3):
        w_t[c * dim:(c + 1) * dim, :] = jnp.transpose(w_v[:, c * dim:(c + 1) * dim])
    wo_t[...] = jnp.transpose(wo_v[...])
    for i in range(1, n_blk):
        x_copy(i).wait()
    for i in range(n_blk):
        gy_copy(i).start()
    for i in range(n_blk):
        for n in range(n_sub):
            u_n = u_t[i, :, sub(n)]
            for part, ref in ((0, q_t), (1, k_t)):
                r = _dot(w_t[part * dim:(part + 1) * dim, :], u_n).astype(BF)
                ref[i, :, sub(n)] = r
                rf = r.astype(F32)
                rf = rf * rf
                acc = (sq_acc, sk_acc)[part]
                val = rf[:, :LANES] + rf[:, LANES:]
                if i == 0 and n == 0:
                    acc[...] = val
                else:
                    acc[...] += val
            if i + 1 < n_blk:
                norm_sub(i + 1, n)
        lo = _dot_nt(q_t[i, :r_lo, :], k_t[i, :WIN, :])
        hi = _dot_nt(q_t[i, r_lo:, :], k_t[i, hi0:, :])
        if i == 0:
            g_lo[...] = lo
            g_hi[...] = hi
        else:
            g_lo[...] += lo
            g_hi[...] += hi

    def pack(lo, hi, put):
        col = lax.broadcasted_iota(jnp.int32, (hd, WIN), 1)
        t_lo = jnp.zeros((hd, WIN), F32)
        for h in range(n_lo):
            t_lo += jnp.where((col >= h * hd) & (col < (h + 1) * hd), lo[h * hd:(h + 1) * hd, :], 0.0)
        t_hi = jnp.zeros((hd, WIN), F32)
        for h in range(n_lo, n_head):
            b = h * hd - hi0
            r = h * hd - r_lo
            t_hi += jnp.where((col >= b) & (col < b + hd), hi[r:r + hd, :], 0.0)
        put(jnp.concatenate([t_lo[:, :hi0], t_lo[:, hi0:] + t_hi[:, :WIN - hi0], t_hi[:, WIN - hi0:]], axis=1))

    def ex_pair(src, rc, ss, rs):
        return rcopy(src.at[1 - core], rc, ss.at[0], rs.at[0], partner)

    def ex_chip(buf, ss, rs, dc):
        return rcopy(buf.at[chip], buf.at[chip], ss.at[dc], rs.at[dc], dev(lax.rem(chip + dc, n_chip), core, img_i))

    def ex_swap(fin, ss, rs):
        return rcopy(fin.at[core], fin.at[core], ss.at[n_chip], rs.at[n_chip], partner)

    def ex_step2(src, rc, buf, ss, rs):
        ex_pair(src, rc, ss, rs).wait()
        buf[chip] = src[core] + rc[...]
        for dc in sorted(range(1, n_chip), key=lambda d: -min(d, n_chip - d)):
            ex_chip(buf, ss, rs, dc).start()

    def ex_step3(buf, fin, ss, rs):
        for dc in range(1, n_chip):
            ex_chip(buf, ss, rs, dc).wait()
        tot = buf[0]
        for j in range(1, n_chip):
            tot += buf[j]
        fin[core] = tot
        ex_swap(fin, ss, rs).start()

    def put_g(t):
        h1 = ex1_src.shape[1]
        sq = jnp.sum(jnp.transpose(sq_acc[...]), axis=0, keepdims=True)
        sk = jnp.sum(jnp.transpose(sk_acc[...]), axis=0, keepdims=True)
        ex1_src[0] = t[:h1]
        ex1_src[1, :hd - h1] = t[h1:]
        ex1_src[1, hd - h1:hd - h1 + 8] = jnp.broadcast_to(sq, (8, dim))
        ex1_src[1, hd - h1 + 8:] = jnp.broadcast_to(sk, (8, dim))

    def put_da(t):
        ex2_src[0] = t[:hd // 2]
        ex2_src[1] = t[hd // 2:]

    pack(g_lo, g_hi, put_g)
    pl.semaphore_wait(barrier, 1 + len(offsets))
    ex_pair(ex1_src, ex1_rc, ex1_ss, ex1_rs).start()

    for i in range(n_blk):
        gy_copy(i).wait()
    for i in range(n_blk):
        for n in range(n_sub):
            gy_t[i, :, sub(n)] = jnp.transpose(gy_v[i, sub(n), :])
            v_t[i, :, sub(n)] = _dot(w_t[2 * dim:, :], u_t[i, :, sub(n)]).astype(BF)
            do_t[i, :, sub(n)] = _dot(wo_v[...], gy_t[i, :, sub(n)]).astype(BF)
        lo = _dot_nt(do_t[i, :r_lo, :], v_t[i, :WIN, :])
        hi = _dot_nt(do_t[i, r_lo:, :], v_t[i, hi0:, :])
        if i == 0:
            da_lo[...] = lo
            da_hi[...] = hi
            ex_step2(ex1_src, ex1_rc, ex1_x, ex1_ss, ex1_rs)
        else:
            da_lo[...] += lo
            da_hi[...] += hi

    pack(da_lo, da_hi, put_da)
    ex_pair(ex2_src, ex2_rc, ex2_ss, ex2_rs).start()
    ex_step3(ex1_x, ex1_fin, ex1_ss, ex1_rs)
    ex_step2(ex2_src, ex2_rc, ex2_x, ex2_ss, ex2_rs)
    ex_swap(ex1_fin, ex1_ss, ex1_rs).wait()

    def head_mask(rows, row0, col0):
        r = lax.broadcasted_iota(jnp.int32, (rows, WIN), 0) + row0
        c = lax.broadcasted_iota(jnp.int32, (rows, WIN), 1) + col0
        out = (r < 0)
        for h in range(n_head):
            out |= (r >= h * hd) & (r < (h + 1) * hd) & (c >= h * hd) & (c < (h + 1) * hd)
        return out

    windows = ((0, r_lo, 0, n_lo), (r_lo, r_hi, hi0, n_head - n_lo))
    h1 = ex1_fin.shape[1]
    gcat = jnp.concatenate([ex1_fin[0], ex1_fin[1, :hd - h1]], axis=0)
    sq = ex1_fin[1, hd - h1:hd - h1 + 1]
    sk = ex1_fin[1, hd - h1 + 8:hd - h1 + 9]
    rk = lax.rsqrt(sk)
    srow[0:1] = sk
    srow[1:2] = rk
    sq_c = _column(sq)
    rq_c = lax.rsqrt(sq_c)
    rqcol[0] = sq_c
    rqcol[1] = rq_c
    tau_c = jnp.concatenate([jnp.full((hd, LANES), tau_ref[h], F32) for h in range(n_head)], axis=0)
    rqcol[2] = tau_c
    for w, (row0, rows, col0, heads) in enumerate(windows):
        g = jnp.concatenate([gcat[:, col0:col0 + WIN]] * heads, axis=0)
        mask = head_mask(rows, row0, col0)
        scale = _twice((tau_c * rq_c)[row0:row0 + rows]) * rk[:, col0:col0 + WIN]
        s = g * scale
        top = jnp.max(jnp.where(mask, s, -jnp.inf), axis=1, keepdims=True)
        e = jnp.where(mask, jnp.exp(jnp.where(mask, s - top, 0.0)), 0.0)
        a = e / jnp.sum(e, axis=1, keepdims=True)
        a_f32[row0:row0 + rows] = a
        scale_f32[row0:row0 + rows] = scale
        g_f32[row0:row0 + rows] = g
        if w == 0:
            full = jnp.concatenate([a, jnp.zeros((WIN - rows, WIN), F32)], axis=0)
            a_lo[...] = full.astype(BF)
            at_lo[...] = jnp.transpose(full).astype(BF)
        else:
            full = jnp.concatenate([jnp.zeros((WIN - rows, WIN), F32), a], axis=0)
            a_hi[...] = full.astype(BF)
            at_hi[...] = jnp.transpose(full).astype(BF)

    def add_rows(acc, g, val, first):
        rb = dim // (2 * n_chip)
        n_a = n_img // 2
        rc = rb // n_a
        for s in range(2 * n_chip):
            for a in range(n_a):
                part = val[s * rb + a * rc:s * rb + (a + 1) * rc]
                if first:
                    acc[s % 2, s // 2, 2 * a + g] = part
                else:
                    acc[s % 2, s // 2, 2 * a + g] += part

    n_ct = dim // LANES

    def add_cols(acc, val, first):
        rb = dim // (2 * n_chip)
        for s in range(2 * n_chip):
            for ct in range(n_ct):
                part = val[s * rb:(s + 1) * rb, ct * LANES:(ct + 1) * LANES]
                if first:
                    acc[s % 2, s // 2, ct] = part
                else:
                    acc[s % 2, s // 2, ct] += part

    for i in range(n_blk):
        for n in range(n_sub):
            o_t[i, :r_lo, sub(n)] = _dot(a_lo[:r_lo], v_t[i, :WIN, sub(n)]).astype(BF)
            o_t[i, r_lo:, sub(n)] = _dot(a_hi[off_hi:], v_t[i, hi0:, sub(n)]).astype(BF)
            dqkv_t[i, 2 * dim:2 * dim + r_lo, sub(n)] = _dot(at_lo[:r_lo], do_t[i, :WIN, sub(n)]).astype(BF)
            dqkv_t[i, 2 * dim + r_lo:, sub(n)] = _dot(at_hi[off_hi:], do_t[i, hi0:, sub(n)]).astype(BF)
        add_rows(acc_e, 0, _dot(o_t[i], gy_v[i]), i == 0)
        add_rows(acc_e, 1, _dot_nt(u_t[i], dqkv_t[i, 2 * dim:, :]), i == 0)
        if i == max(n_blk - 2, 0):
            ex_step3(ex2_x, ex2_fin, ex2_ss, ex2_rs)

    def pair_copy(r, acc, buf):
        return rcopy(acc.at[1 - core], buf, d2d_ss.at[r], d2d_rs.at[r], partner)

    hn = n_img // 2
    right = lax.rem(chip + 1, n_chip)
    left = lax.rem(chip + n_chip - 1, n_chip)
    opp = lax.rem(chip + 2, n_chip)

    def ring_copy(n):
        to = dev((right, left)[n % 2], core, img_i)
        if n == 0:
            src, dst = acc_e.at[core, opp, pl.ds(0, hn)], ring1.at[0]
        elif n == 1:
            src, dst = acc_e.at[core, opp, pl.ds(hn, hn)], ring1.at[1]
        else:
            src, dst = acc_e.at[core, (right, left)[n % 2]], ring2.at[n % 2]
        return rcopy(src, dst, ring_ss.at[n], ring_rs.at[n], to)

    def yrs_copy(di):
        pi = lax.rem(img_i + di, n_img)
        return rcopy(acc_e.at[core, chip, pi], yrs_e.at[di - 1], yrs_ss.at[di - 1], yrs_rs.at[di - 1],
                     dev(chip, core, pi))

    def age_copy(di):
        return rcopy(ag_e.at[img_i], ag_e.at[img_i], age_ss.at[di - 1], age_rs.at[di - 1],
                     dev(chip, core, lax.rem(img_i + di, n_img)))

    def e_step1():
        pair_copy(0, acc_e, d2d_e).wait()
        for j in range(n_chip):
            acc_e[core, j] += d2d_e[j]
        ring_copy(0).start()
        ring_copy(1).start()

    def e_step2():
        ring_copy(0).wait()
        ring_copy(1).wait()
        acc_e[core, right, :hn] += ring1[0]
        acc_e[core, left, hn:] += ring1[1]
        ring_copy(2).start()
        ring_copy(3).start()

    def e_step3():
        ring_copy(2).wait()
        ring_copy(3).wait()
        acc_e[core, chip] += ring2[0] + ring2[1]
        for di in range(1, n_img):
            yrs_copy(di).start()

    def e_step4():
        tot = acc_e[core, chip, img_i]
        for di in range(1, n_img):
            yrs_copy(di).wait()
            tot += yrs_e[di - 1]
        ag_e[img_i] = tot
        for di in range(1, n_img):
            age_copy(di).start()

    def owner(r, ct):
        return (2 * r + ct) % n_img

    def rs_copy(r, acc, buf, ct, dc):
        pc = lax.rem(chip + dc, n_chip)
        sl = ct // n_img
        return rcopy(acc.at[core, pc, ct], buf.at[sl, dc, img_i], rs_ss.at[r, ct, dc], rs_rs.at[r, sl, dc, img_i],
                     dev(pc, core, owner(r, ct)))

    def each_send(r, do):
        for dc in range(n_chip):
            for ct in range(n_ct):
                if dc:
                    do(ct, dc)
                else:
                    pl.when(img_i != owner(r, ct))(functools.partial(do, ct, dc))

    def rs_start(r, acc, d2d, buf):
        pair_copy(1 + r, acc, d2d).wait()
        for j in range(n_chip):
            acc[core, j] += d2d[j]
        each_send(r, lambda ct, dc: rs_copy(r, acc, buf, ct, dc).start())

    def ag_copy(r, gbuf, ct, di):
        return rcopy(gbuf.at[ct], gbuf.at[ct], ag_ss.at[r, ct, di - 1], ag_rs.at[r, ct],
                     dev(chip, core, lax.rem(img_i + di, n_img)))

    def rs_finish(r, acc, buf, gbuf):
        for ct in range(n_ct):
            @pl.when(img_i == owner(r, ct))
            def _(ct=ct):
                sl = ct // n_img
                tot = acc[core, chip, ct]
                for dc in range(n_chip):
                    for im in range(n_img):
                        if dc == 0 and im == owner(r, ct):
                            continue
                        rcopy(buf.at[sl, dc, im], buf.at[sl, dc, im], rs_ss.at[r, ct, dc], rs_rs.at[r, sl, dc, im],
                              partner).wait_recv()
                        tot += buf[sl, dc, im]
                gbuf[ct] = tot
                for di in range(1, n_img):
                    ag_copy(r, gbuf, ct, di).start()

    def rs_end(r, acc, buf, gbuf, ref, col):
        each_send(r, lambda ct, dc: rs_copy(r, acc, buf, ct, dc).wait_send())
        for ct in range(n_ct):
            @pl.when(img_i == owner(r, ct))
            def _(ct=ct):
                for di in range(1, n_img):
                    ag_copy(r, gbuf, ct, di).wait_send()

            @pl.when(img_i != owner(r, ct))
            def _(ct=ct):
                ag_copy(r, gbuf, ct, 1).wait_recv()
            ref[:, col + ct * LANES:col + (ct + 1) * LANES] = gbuf[ct]

    pair_copy(0, acc_e, d2d_e).start()
    ex_swap(ex2_fin, ex2_ss, ex2_rs).wait()

    dacat = jnp.concatenate([ex2_fin[0], ex2_fin[1]], axis=0)
    sq_c = rqcol[0]
    rq_c = rqcol[1]
    tau_c = rqcol[2]
    sk = srow[0:1]
    rk = srow[1:2]
    row_sums = []
    col_sums = []
    for w, (row0, rows, col0, heads) in enumerate(windows):
        da = jnp.concatenate([dacat[:, col0:col0 + WIN]] * heads, axis=0)
        a = a_f32[row0:row0 + rows]
        ds = a * (da - jnp.sum(a * da, axis=1, keepdims=True))
        dg = ds * scale_f32[row0:row0 + rows]
        dscale = ds * g_f32[row0:row0 + rows]
        row_sums.append(jnp.broadcast_to(jnp.sum(dscale * rk[:, col0:col0 + WIN], axis=1, keepdims=True),
                                         (rows, LANES)))
        col_sums.append(jnp.sum(dscale * _twice((tau_c * rq_c)[row0:row0 + rows]), axis=0, keepdims=True))
        if w == 0:
            full = jnp.concatenate([dg, jnp.zeros((WIN - rows, WIN), F32)], axis=0)
            dg_lo[...] = full.astype(BF)
            dgt_lo[...] = jnp.transpose(full).astype(BF)
        else:
            full = jnp.concatenate([jnp.zeros((WIN - rows, WIN), F32), dg], axis=0)
            dg_hi[...] = full.astype(BF)
            dgt_hi[...] = jnp.transpose(full).astype(BF)
    t_row = jnp.concatenate(row_sums, axis=0)
    cl, ch = col_sums
    w_col = jnp.concatenate([cl[:, :hi0], cl[:, hi0:] + ch[:, :WIN - hi0], ch[:, WIN - hi0:]], axis=1)
    cq_c[...] = 2.0 * (-0.5 * rq_c / sq_c * (tau_c * t_row))
    ck_c[...] = _column(2.0 * (-0.5 * rk / sk * w_col))
    lane = lax.broadcasted_iota(jnp.int32, (1, LANES), 1)
    dtau_row = jnp.zeros((1, LANES), F32)
    for h in range(n_head):
        part = jnp.sum((rq_c * t_row)[h * hd:(h + 1) * hd], axis=0, keepdims=True)
        dtau_row += jnp.where(lane == h, part, 0.0)
    gb_src[6:7] = jnp.where(seq_i == 0, dtau_row, 0.0)
    gb_src[7:8] = jnp.zeros((1, LANES), F32)

    def back(i, part):
        lo, hi, a_t, b_t, c = ((dg_lo, dg_hi, k_t, q_t, cq_c), (dgt_lo, dgt_hi, q_t, k_t, ck_c))[part]
        base = part * dim
        for n in range(n_sub):
            a_n = a_t[i, :, sub(n)]
            d = jnp.concatenate([_dot(lo[:r_lo], a_n[:WIN]), _dot(hi[off_hi:], a_n[hi0:])], axis=0)
            dqkv_t[i, base:base + dim, sub(n)] = (d + _twice(c[...]) * b_t[i, :, sub(n)].astype(F32)).astype(BF)
        add_cols((acc_q, acc_k)[part], _dot_nt(u_t[i], dqkv_t[i, base:base + dim, :]), i == 0)

    e_step1()
    for i in range(n_blk):
        back(i, 0)
    pair_copy(1, acc_q, d2d_q).start()
    e_step2()
    for i in range(n_blk):
        back(i, 1)
        if i == min(1, n_blk - 1):
            rs_start(0, acc_q, d2d_q, rs_q)
    pair_copy(2, acc_k, d2d_k).start()

    for i in range(n_blk):
        for n in range(n_sub):
            du = _dot(w_v[...], dqkv_t[i, :, sub(n)]).astype(BF)
            do_t[i, :, sub(n)] = du
            for c in range(SUB // LANES):
                cols = slice(n * SUB + c * LANES, n * SUB + (c + 1) * LANES)
                du_c = du[:, c * LANES:(c + 1) * LANES].astype(F32)
                rstd = rstd_v[i, :, cols]
                xh = (x_t[i, :, cols].astype(F32) - mean_v[i, :, cols]) * rstd
                p = du_c * xh
                dgam_acc[...] += p
                dbet_acc[...] += du_c
                c1 = jnp.sum(du_c * gam_c[...], axis=0, keepdims=True) * inv_d
                c2 = jnp.sum(p * gam_c[...], axis=0, keepdims=True) * inv_d
                k1_v[i, :, cols] = rstd * c1
                k2_v[i, :, cols] = rstd * rstd * c2

        if i == 0:
            rs_start(1, acc_k, d2d_k, rs_k)
        if i == min(1, n_blk - 1):
            e_step3()

    for b, acc in ((0, dgam_acc), (dim // LANES, dbet_acc)):
        row = jnp.sum(jnp.transpose(acc[...]), axis=0, keepdims=True)
        for c in range(dim // LANES):
            gb_src[b + c:b + c + 1] = row[:, c * LANES:(c + 1) * LANES]
    gb_pair = rcopy(gb_src, gb_rc, gb_ss.at[0], gb_rs.at[0], partner)
    gb_pair.start()

    def gb_copy(n):
        pc, pi = peer(*offsets[n])
        return rcopy(gb_all.at[chip, img_i], gb_all.at[chip, img_i], gb_ss.at[1 + n], gb_rs.at[1 + n],
                     dev(pc, core, pi))


    def body_x(i, _):
        for n in range(n_sub):
            proj = _dot(wo_t[...], o_t[i, :, sub(n)])
            x_v[i, sub(n), :] = jnp.transpose((x_t[i, :, sub(n)].astype(F32) + proj).astype(BF))
            for c in range(SUB // LANES):
                cols = slice(n * SUB + c * LANES, n * SUB + (c + 1) * LANES)
                g = do_t[i, :, cols].astype(F32) * gam_c[...] * rstd_v[i, :, cols]
                cen = x_t[i, :, cols].astype(F32) - mean_v[i, :, cols]
                gx = gy_t[i, :, cols].astype(F32) + (g - k1_v[i, :, cols] - cen * k2_v[i, :, cols])
                gy_v[i, cols, :] = jnp.transpose(gx.astype(BF))

        @pl.when(i == 0)
        def _():
            gb_pair.wait()
            gb_all[chip, img_i] = gb_src[...] + gb_rc[...]
            for n in range(len(offsets)):
                gb_copy(n).start()
            rs_finish(0, acc_q, rs_q, ag_q)

        @pl.when(i == min(1, n_blk - 1))
        def _():
            e_step4()
        return 0

    lax.fori_loop(0, n_blk, body_x, 0)
    rs_finish(1, acc_k, rs_k, ag_k)
    for n in range(len(offsets)):
        gb_copy(n).wait()
    tot = jnp.zeros(gb_src.shape, F32)
    for j in range(n_chip):
        for m in range(n_img):
            tot += gb_all[j, m]
    n_row = dim // LANES
    for b, ref in ((0, dgam_ref), (n_row, dbet_ref)):
        ref[...] = jnp.concatenate([tot[b + c:b + c + 1] for c in range(n_row)], axis=1).reshape(dim)
    dtau_ref[...] = tot[6:7, :n_head].reshape(n_head)
    rs_end(0, acc_q, rs_q, ag_q, dwqkv_ref, 0)
    for di in range(1, n_img):
        age_copy(di).wait()
    rc = ag_e.shape[1]
    for a in range(hn):
        for g, (ref, col) in enumerate(((dwout_ref, 0), (dwqkv_ref, 2 * dim))):
            ref[a * rc:(a + 1) * rc, col:col + dim] = ag_e[2 * a + g]
    rs_end(1, acc_k, rs_k, ag_k, dwqkv_ref, dim)


def _write(n_blk, blk, *refs):
    srcs, dsts, act_sem, sem = refs[:7], refs[7:14], refs[14], refs[15]
    copies = []
    for a in range(2):
        for i in range(n_blk):
            copies.append(pltpu.make_async_copy(srcs[a].at[i], dsts[a].at[0, pl.ds(i * blk, blk), :],
                                                act_sem.at[a, i]))
    for n in range(5):
        copies.append(pltpu.make_async_copy(srcs[2 + n], dsts[2 + n], sem.at[n]))
    for c in copies:
        c.start()
    for c in copies:
        c.wait()


def solution(mesh):
    act_spec = P(('data', 'img'), 'seq', None)
    row_spec = P(('data', 'seq'), None)
    in_specs = (act_spec, act_spec, P(), P(), P(), P(), P())
    out_specs = (act_spec, act_spec, row_spec, row_spec, P('data'), P('data'), P('data'))
    n_img = mesh.shape['img']
    n_seq = mesh.shape['seq']
    n_chip = n_seq // 2

    def local_block(x_in, grad_y, ln_gamma, ln_beta, w_qkv, w_out, head_temp):
        _, n_tok, dim = x_in.shape
        n_head = head_temp.shape[0]
        hd = dim // n_head
        blk = min(1024, n_tok)
        n_blk = n_tok // blk
        rb = dim // n_seq
        rc = rb // (n_img // 2)
        h1 = (hd + 16) // 2
        hbm = pl.BlockSpec(memory_space=pltpu.HBM)
        vmem = pl.BlockSpec(memory_space=pltpu.VMEM)
        smem = pl.BlockSpec(memory_space=pltpu.SMEM)
        V = pltpu.VMEM
        n_off = n_chip * n_img - 1
        n_hi = n_head - WIN // hd
        r_hi = n_hi * hd
        r_lo = dim - r_hi
        feat = V((n_blk, dim, blk), BF)
        stat = V((n_blk, 1, blk), F32)
        col = V((dim, LANES), F32)
        sqr = V((WIN, WIN), BF)
        acc = V((2, n_chip, n_img, rc, dim), F32)
        n_ct = dim // LANES
        n_sl = -(-n_ct // n_img)
        accc = V((2, n_chip, n_ct, rb, LANES), F32)
        dma = pltpu.SemaphoreType.DMA
        scratch = [
            feat, feat, feat, feat, feat, feat, feat, feat, V((n_blk, 3 * dim, blk), BF),
            stat, stat, stat, stat, V((dim, 3 * dim), BF), V((3 * dim, dim), BF), V((dim, dim), BF), V((dim, dim), BF),
            V((dim,), F32), V((dim,), F32), col, col,
            V((r_lo, WIN), F32), V((r_hi, WIN), F32), V((r_lo, WIN), F32), V((r_hi, WIN), F32),
            col, col, col, col,
            V((dim, WIN), F32), V((dim, WIN), F32), V((dim, WIN), F32),
            sqr, sqr, sqr, sqr, sqr, sqr, sqr, sqr,
            col, col, V((8, dim), F32), V((3, dim, LANES), F32),
            V((2, h1, dim), F32), V((h1, dim), F32), V((n_chip, h1, dim), F32), V((2, h1, dim), F32),
            V((2, hd // 2, dim), F32), V((hd // 2, dim), F32), V((n_chip, hd // 2, dim), F32),
            V((2, hd // 2, dim), F32),
            acc, accc, accc, V((n_chip, n_img, rc, dim), F32), V((n_chip, n_ct, rb, LANES), F32),
            V((n_chip, n_ct, rb, LANES), F32), V((2, n_img // 2, rc, dim), F32), V((2, n_img, rc, dim), F32),
            V((n_img - 1, rc, dim), F32), V((n_img, rc, dim), F32), V((n_sl, n_chip, n_img, rb, LANES), F32),
            V((n_sl, n_chip, n_img, rb, LANES), F32), V((n_ct, rb, LANES), F32), V((n_ct, rb, LANES), F32),
            V((8, LANES), F32), V((8, LANES), F32), V((n_chip, n_img, 8, LANES), F32),
            dma((n_blk,)), dma((n_blk,)), dma((4,)),
            dma((n_chip + 1,)), dma((n_chip + 1,)), dma((n_chip + 1,)), dma((n_chip + 1,)),
            dma((3,)), dma((3,)), dma((4,)), dma((4,)), dma((n_img - 1,)), dma((n_img - 1,)),
            dma((n_img - 1,)), dma((n_img - 1,)),
            dma((2, n_ct, n_chip)), dma((2, n_sl, n_chip, n_img)), dma((2, n_ct, n_img - 1)), dma((2, n_ct)),
            dma((1 + n_off,)), dma((1 + n_off,)),
        ]
        out_shape = (
            V((n_blk, blk, dim), BF), V((n_blk, blk, dim), BF), V((rb, 3 * dim), F32), V((rb, dim), F32),
            V((dim,), F32), V((dim,), F32), V((n_head,), F32),
        )
        cfg = (n_chip, n_img, n_blk, blk, dim, n_head)
        outs = pl.pallas_call(
            functools.partial(_kernel, cfg),
            out_shape=out_shape,
            in_specs=[hbm, hbm, hbm, hbm, hbm, hbm, smem],
            out_specs=(vmem,) * 7,
            scratch_shapes=scratch,
            compiler_params=pltpu.CompilerParams(collective_id=0, has_side_effects=True,
                                                 vmem_limit_bytes=VMEM_MAIN),
        )(x_in, grad_y, ln_gamma, ln_beta, w_qkv, w_out, head_temp)
        finals = (
            jax.ShapeDtypeStruct(x_in.shape, BF), jax.ShapeDtypeStruct(x_in.shape, BF),
            jax.ShapeDtypeStruct((rb, 3 * dim), F32), jax.ShapeDtypeStruct((rb, dim), F32),
            jax.ShapeDtypeStruct((dim,), F32), jax.ShapeDtypeStruct((dim,), F32),
            jax.ShapeDtypeStruct((n_head,), F32),
        )
        return pl.pallas_call(
            functools.partial(_write, n_blk, blk),
            out_shape=finals,
            in_specs=[vmem] * 7,
            out_specs=(hbm,) * 7,
            scratch_shapes=[dma((2, n_blk)), dma((5,))],
            compiler_params=pltpu.CompilerParams(vmem_limit_bytes=1 << 20),
        )(*outs)

    return jax.shard_map(local_block, mesh=mesh, in_specs=in_specs, out_specs=out_specs, check_vma=False)
```
